32 devices in a mesh: freq: 2 (over x), base: 4 (over y, core), pix: 4 (over z).
Axes of the slice: x: 2, y: 2, z: 4, core: 2. Of those that a mesh axis runs over, the one named last changes fastest.
Arguments:
- sensing_operator_parts: bfloat16 [2, 4096, 2048], P('freq', 'base', 'pix'), may hold values from -1 to 1
- sampled_correlations: float32 [64, 4096], P('freq', 'base'), may hold values from -40 to 40
- first_sky_estimate: float32 [64, 4, 4, 128], P('freq', 'pix', 'base'), may hold values from -2.5 to 2.5
- patch_order_record: int32 [6, 16], P(None, 'pix'), may hold values from 0 to 15, as said below
Outputs:
- image: float32 [64, 4, 4, 128], P('freq', 'pix', 'base')
The draws below stay inside these ranges and needn't reach their ends.
Inputs may be any that keep to these rules, and one draw needn't show every extreme that they name: `patch_order_record`: each row holds every tile number once; the tiles of rank under 4 are the same in every row.
All inputs are finite; a program needn't handle non-finite values.
Results may differ from the reference program's by a relative error of at most 0.0014.
Values may be sent and summed in bfloat16 or wider, within the bound.
No kernel may reach another device: no remote copies, remote signals or barrier semaphores. Data moves between devices by JAX's collectives and lax.ppermute only.
A program may use at most 64 MiB of HBM per device.

```python
import math
import jax
import jax.numpy as jnp
from jax import lax

CH = 64
TILE = 128
ITERS = 6
TILES_DEV = 1
GROUPS = 2
TSH = 128
NP = 2048
NM = 4096
NT = 16
KEEP = 4
N_BASE = 4
N_PIX = 4


def draw_sensing_operator_parts(key, part):
    key_base, key_tile, key_col = jax.random.split(jax.random.fold_in(key, 11), 3)
    tile_scaling = jnp.exp(jax.random.uniform(key_tile, (GROUPS, 1, NT, 1), jnp.float32, math.log(0.3), math.log(1.5)))
    col_scale = jax.random.uniform(key_col, (GROUPS, 1, NT, TILE), jnp.float32, 0.7, 1.3)
    scales = (tile_scaling * col_scale).reshape(GROUPS, 1, NP)
    values = jnp.clip(jax.random.normal(key_base, (GROUPS, NM, NP), jnp.float32), -4.0, 4.0)
    denom = math.sqrt(NM) + math.sqrt(NP)
    return jnp.clip(values * scales / denom, -1.0, 1.0).astype(jnp.bfloat16)


def draw_sampled_correlations(key, part):
    key_main = jax.random.fold_in(jax.random.fold_in(key, 23), 0)
    chan_scale = jnp.exp(math.log(3.0) * jnp.arange(CH, dtype=jnp.float32) / max(CH - 1, 1))
    values = jnp.clip(jax.random.normal(key_main, (CH, NM), jnp.float32), -5.0, 5.0)
    return jnp.clip(values * chan_scale[:, None], -40.0, 40.0)


def draw_patch_order_record(key, part):
    key_set, key_rows = jax.random.split(jax.random.fold_in(key, 37))
    tile_order = jax.random.permutation(key_set, NT).astype(jnp.int32)
    all_rows = []
    for iteration in range(ITERS):
        key_kept, key_rest = jax.random.split(jax.random.fold_in(key_rows, iteration))
        kept_rank = jax.random.permutation(key_kept, KEEP).astype(jnp.int32)
        rest_rank = (KEEP + jax.random.permutation(key_rest, NT - KEEP)).astype(jnp.int32)
        rank_values = jnp.concatenate([kept_rank, rest_rank])
        rank_row = jnp.zeros((NT,), jnp.int32).at[tile_order].set(rank_values)
        all_rows.append(rank_row)
    return jnp.stack(all_rows)


def steps_of(key, shape, pieces, least, largest):
    gain = 1.0
    for axis_at, shards_of in pieces:
        heights = jax.random.uniform(jax.random.fold_in(jax.random.fold_in(key, 6), axis_at), (shards_of,), jnp.float32, least / len(pieces), largest / len(pieces))
        gain = gain * jnp.repeat(jnp.exp(heights), shape[axis_at] // shards_of).reshape((-1,) + (1,) * (len(shape) - 1 - axis_at))
    return gain


def noise(own_key, extent, width, limit, cuts=(), kind=jnp.bfloat16):
    result = width * jax.random.normal(own_key, extent, jnp.float32)
    if cuts:
        result = result * steps_of(own_key, extent, cuts, -0.22, 0.18)
    return jnp.clip(result, -limit, limit).astype(kind)


def setup_inputs(seed: int = 0) -> dict:
    key_of = jax.random.split(jax.random.key(seed), 5)
    return {
        "sensing_operator_parts": draw_sensing_operator_parts(jax.random.fold_in(key_of[4], 71), 0),
        "sampled_correlations": draw_sampled_correlations(jax.random.fold_in(key_of[4], 71), 0),
        "first_sky_estimate": noise(key_of[2], (CH, N_PIX, N_BASE, TSH), 1.0, 2.5, ((0, 2), (1, 4), (2, 4)), jnp.float32),
        "patch_order_record": draw_patch_order_record(jax.random.fold_in(key_of[4], 71), 0),
    }


descent_stride = 0.6
lam_shrink = 0.3
eps_norm = 1e-06

def reference(sensing_operator_parts, sampled_correlations, first_sky_estimate, patch_order_record):
    chan_grp = CH // GROUPS
    current = first_sky_estimate.reshape(CH, NP)
    for step in range(ITERS):
        rounded_amount = current.astype(jnp.bfloat16)
        grads = []
        for spectral_band_set in range(GROUPS):
            sensing_operator = sensing_operator_parts[spectral_band_set]
            part = rounded_amount[spectral_band_set * chan_grp:(spectral_band_set + 1) * chan_grp]
            pred = lax.dot_general(part, sensing_operator, (((1,), (1,)), ((), ())), preferred_element_type=jnp.float32)
            resid = (sampled_correlations[spectral_band_set * chan_grp:(spectral_band_set + 1) * chan_grp] - pred).astype(jnp.bfloat16)
            grads.append(jnp.dot(resid, sensing_operator, preferred_element_type=jnp.float32))
        moved = current + descent_stride * jnp.concatenate(grads, axis=0)
        tiles = moved.reshape(CH, NT, TILE)
        tnorm = lax.optimization_barrier(jnp.sum(tiles * tiles, axis=(0, 2)))
        rms_tile = jnp.sqrt(tnorm / (CH * TILE) + eps_norm)
        keeping = (patch_order_record[step] < KEEP).astype(jnp.float32)
        factor = keeping * rms_tile / (rms_tile + lam_shrink)
        current = (tiles * factor[None, :, None]).reshape(CH, NP)
    return current.reshape(CH, N_PIX, N_BASE, TILES_DEV * TILE)
```

```python
import functools

import jax
import jax.numpy as jnp
from jax import lax
from jax.experimental import pallas as pl
from jax.experimental.pallas import tpu as pltpu
from jax.sharding import PartitionSpec as P

CH = 64
TILE = 128
ITERS = 6


descent_stride = 0.6
lam_shrink = 0.3
eps_norm = 1e-06

GRAM_LIMIT = 1 << 20
PAD = 16


def project_rows(rounded_amount, columns):
    return lax.dot_general(
        rounded_amount, columns, (((1,), (1,)), ((), ())), preferred_element_type=jnp.float32
    )


def residual_of(sampled_correlations, partial_value):
    shares = lax.psum_scatter(partial_value, "pix", scatter_dimension=1, tiled=True)
    width = shares.shape[1]
    own_rows = lax.dynamic_slice_in_dim(
        sampled_correlations, lax.axis_index("pix") * width, width, 1
    )
    return lax.all_gather((own_rows - shares).astype(jnp.bfloat16), "pix", axis=1, tiled=True)


def streaming(sensing_operator_parts, sampled_correlations, first_sky_estimate, patch_order_record):
    sensing_operator = sensing_operator_parts[0]
    chans, m_dev = sampled_correlations.shape
    share_width = first_sky_estimate.shape[3]
    tiles_share = share_width // TILE
    keep_count = tiles_share * lax.axis_size("base") * lax.axis_size("pix") // 4
    base_index = lax.axis_index("base")
    own_share = first_sky_estimate[:, 0, 0, :]
    current = own_share
    for step in range(ITERS):
        rounded_amount = current.astype(jnp.bfloat16)
        partial_value = project_rows(
            lax.all_gather(rounded_amount, "base", axis=1, tiled=True), sensing_operator
        )
        resid = residual_of(sampled_correlations, partial_value)
        gradient_portion = jnp.dot(resid, sensing_operator, preferred_element_type=jnp.float32)
        grad_share = lax.psum_scatter(gradient_portion, "base", scatter_dimension=1, tiled=True)
        moved = current + descent_stride * grad_share
        tiles = moved.reshape(chans, tiles_share, TILE)
        local_sum = jnp.sum(tiles * tiles, axis=(0, 2))
        total = lax.psum(local_sum, "freq")
        ranks = lax.dynamic_slice_in_dim(
            patch_order_record[step], base_index * tiles_share, tiles_share, 0
        )
        rms_tile = jnp.sqrt(total / (CH * TILE) + eps_norm)
        keeping = (ranks < keep_count).astype(jnp.float32)
        factor = keeping * rms_tile / (rms_tile + lam_shrink)
        current = (tiles * factor[None, :, None]).reshape(chans, share_width)
    return current.reshape(chans, 1, 1, share_width)


def swap(value, axis, offset):
    size = lax.axis_size(axis)
    return lax.ppermute(value, axis, [(i, i ^ offset) for i in range(size)])


def call(body, out_shape, args, scratch=(), smem=(), name=None):
    specs = [
        pl.BlockSpec(memory_space=pltpu.SMEM if i in smem else pltpu.VMEM) for i in range(len(args))
    ]
    out_specs = jax.tree.map(lambda _: pl.BlockSpec(memory_space=pltpu.VMEM), out_shape)
    return pl.pallas_call(
        body,
        out_shape=out_shape,
        in_specs=specs,
        out_specs=out_specs,
        scratch_shapes=list(scratch),
        name=name,
    )(*args)


def split(value):
    high = value.astype(jnp.bfloat16)
    return high, (value - high.astype(jnp.float32)).astype(jnp.bfloat16)


def pack_body(slots, where_ref, ranks_ref, a_ref, *outs):
    pix = where_ref[0]
    tiles = a_ref.shape[1] // TILE
    quarter = outs[0].shape[0]
    for d, out in enumerate(outs):
        rows = pl.ds(pl.multiple_of((pix ^ d) * quarter, quarter), quarter)
        for r in range(slots):
            tile = jnp.int32(0)
            owned = jnp.int32(0)
            for j in range(tiles):
                hit = ranks_ref[0, j] == r
                tile = jnp.where(hit, j, tile)
                owned = jnp.where(hit, 1, owned)
            block = a_ref[rows, pl.ds(pl.multiple_of(tile * TILE, TILE), TILE)]
            out[:, r * TILE : (r + 1) * TILE] = jnp.where(owned == 1, block, jnp.zeros_like(block))


def first_body(where_ref, a_ref, *refs):
    pix, base = where_ref[0], where_ref[1]
    n_base = a_ref.shape[1] // TILE
    shares, rest = refs[:n_base], refs[n_base:]
    outs, x_ref = rest[:-1], rest[-1]
    quarter = outs[0].shape[1]
    for d, share in enumerate(shares):
        x_ref[:, pl.ds(pl.multiple_of((base ^ d) * TILE, TILE), TILE)] = share[...]
    for d, out in enumerate(outs):
        rows = pl.ds(pl.multiple_of((pix ^ d) * quarter, quarter), quarter)
        out[...] = lax.dot_general(
            x_ref[...], a_ref[rows, :], (((1,), (1,)), ((), ())), preferred_element_type=jnp.float32
        )


def in_order(values, index):
    bit = 1
    while bit < len(values):
        odd = (index & bit) != 0
        values = [jnp.where(odd, values[d ^ bit], values[d]) for d in range(len(values))]
        bit *= 2
    return values


def pairs(slots):
    return [(r, s) for r in range(slots) for s in range(r, slots)]


def gram_body(slots, n_pix, where_ref, ranks_ref, y_ref, x0_ref, *refs):
    pix, base = where_ref[0], where_ref[1]
    parts, preds = refs[:n_pix], refs[n_pix : 2 * n_pix]
    *outs, all_ref = refs[2 * n_pix :]
    n_base = len(outs)
    chans, quarter = preds[0].shape
    a = parts[0][...]
    for part in parts[1:]:
        a = a + part[...]
    pred = preds[0][...]
    for piece in preds[1:]:
        pred = pred + piece[...]
    y = y_ref[:, pl.ds(pl.multiple_of(pix * quarter, quarter), quarter)]
    resid = (y - pred).astype(jnp.bfloat16)
    y_hi, y_lo = split(y)
    left = jnp.concatenate([y_hi, y_lo, resid], axis=0)
    sides = jnp.dot(left, a, preferred_element_type=jnp.float32)
    data = sides[:chans] + sides[chans : 2 * chans]
    moved = descent_stride * sides[2 * chans :]
    rank = ranks_ref[0, base]
    gram = lax.dot_general(a, a, (((0,), (0,)), ((), ())), preferred_element_type=jnp.float32)
    rows = lax.broadcasted_iota(jnp.int32, (TILE, TILE), 0)
    cols = lax.broadcasted_iota(jnp.int32, (TILE, TILE), 1)
    here = rows == cols
    n_pairs = len(pairs(slots))
    g_rows = n_pairs * TILE // n_base
    per = slots // n_base
    side_rows = 4 * chans + PAD
    half = min(TILE, g_rows & -g_rows)
    diags = {}
    for i, (r, s) in enumerate(pairs(slots)):
        block = gram[r * TILE : (r + 1) * TILE, s * TILE : (s + 1) * TILE]
        if r == s:
            diags[r] = jnp.sum(jnp.where(here, block, 0.0), axis=0, keepdims=True)
            block = jnp.where(here, 0.0, block)
        block = block.astype(jnp.bfloat16)
        for q in range(TILE // half):
            at = i * TILE + q * half
            all_ref[at // g_rows, at % g_rows : at % g_rows + half, :] = block[q * half : (q + 1) * half]
    for r in range(slots):
        lanes = slice(r * TILE, (r + 1) * TILE)
        start = jnp.where(rank == r, x0_ref[...], 0.0)
        d_hi, d_lo = split(diags[r])
        stack = [
            *split(data[:, lanes]),
            *split(moved[:, lanes] + start),
            d_hi,
            d_lo,
            jnp.zeros((PAD - 2, TILE), jnp.bfloat16),
        ]
        at = g_rows + (r % per) * side_rows
        for piece in stack[:4]:
            all_ref[r // per, at : at + chans, :] = piece
            at += chans
        all_ref[r // per, at : at + PAD, :] = jnp.concatenate(stack[4:], axis=0)
    for d, out in enumerate(outs):
        out[...] = all_ref[base ^ d]


def sum_body(g_rows, chans, per, *refs):
    *parts, out = refs

    def total(at, size):
        value = parts[0][at : at + size].astype(jnp.float32)
        for part in parts[1:]:
            value = value + part[at : at + size].astype(jnp.float32)
        return value

    out[:g_rows] = total(0, g_rows).astype(jnp.bfloat16)
    at = g_rows
    for _ in range(per):
        for _ in range(2):
            high, low = split(total(at, chans) + total(at + chans, chans))
            out[at : at + chans] = high
            out[at + chans : at + 2 * chans] = low
            at += 2 * chans
        tail = total(at, PAD)
        high, low = split(tail[0:1] + tail[1:2])
        rest = jnp.zeros((PAD - 2, TILE), jnp.bfloat16)
        out[at : at + PAD] = jnp.concatenate([high, low, rest], axis=0)
        at += PAD


def iterate_body(slots, n_base, g_rows, chans, where_ref, ranks_ref, *refs):
    base = where_ref[1]
    per = slots // n_base
    side_rows = 4 * chans + PAD
    chunks = [refs[:n_base], refs[n_base : 2 * n_base]]
    out_ref, gram_ref, last_ref = refs[2 * n_base :]
    states, datas, diags = [], [], []
    for g in range(2):
        full = in_order([ref[...] for ref in chunks[g]], base)
        half = min(TILE, g_rows & -g_rows)
        for i, (r, s) in enumerate(pairs(slots)):
            pieces = []
            for q in range(TILE // half):
                at = i * TILE + q * half
                pieces.append(full[at // g_rows][at % g_rows : at % g_rows + half])
            block = jnp.concatenate(pieces, axis=0)
            gram_ref[g, r * TILE : (r + 1) * TILE, s * TILE : (s + 1) * TILE] = block
            if r != s:
                gram_ref[g, s * TILE : (s + 1) * TILE, r * TILE : (r + 1) * TILE] = block.T
        sides = [full[r // per][g_rows + (r % per) * side_rows :][:side_rows].astype(jnp.float32) for r in range(slots)]
        wide = lambda at: jnp.concatenate([v[at : at + chans] + v[at + chans : at + 2 * chans] for v in sides], axis=1)
        datas.append(wide(0))
        states.append(wide(2 * chans))
        tails = [v[4 * chans :] for v in sides]
        diags.append(jnp.concatenate([t[0:1] + t[1:2] for t in tails], axis=1))
    for step in range(ITERS):
        factors = []
        for r in range(slots):
            lanes = slice(r * TILE, (r + 1) * TILE)
            square = states[0][:, lanes] * states[0][:, lanes] + states[1][:, lanes] * states[1][:, lanes]
            column = jnp.sum(square, axis=0, keepdims=True)
            norm = jnp.sum(column, axis=1, keepdims=True)
            rms = jnp.sqrt(norm / (CH * TILE) + eps_norm)
            factors.append(jnp.broadcast_to(rms / (rms + lam_shrink), (1, TILE)))
        factor = jnp.concatenate(factors, axis=1)
        states = [state * factor for state in states]
        if step == ITERS - 1:
            break
        for g in range(2):
            high, low = split(states[g])
            both = jnp.dot(
                jnp.concatenate([high, low], axis=0), gram_ref[g], preferred_element_type=jnp.float32
            )
            product = both[:chans] + both[chans:] + states[g] * diags[g]
            states[g] = states[g] + descent_stride * (datas[g] - product)
    for r in range(slots):
        last_ref[r] = states[0][:, r * TILE : (r + 1) * TILE]
    rank = ranks_ref[0, base]
    kept = last_ref[jnp.minimum(rank, slots - 1)]
    out_ref[...] = jnp.where(rank < slots, kept, 0.0)


def gram_plan(sensing_operator_parts, sampled_correlations, first_sky_estimate, patch_order_record):
    a = sensing_operator_parts[0]
    chans, m_dev = sampled_correlations.shape
    n_base, n_pix = lax.axis_size("base"), lax.axis_size("pix")
    slots = n_base * n_pix // 4
    quarter = m_dev // n_pix
    x0 = first_sky_estimate[:, 0, 0, :]
    ranks = patch_order_record
    where = jnp.stack([lax.axis_index("pix"), lax.axis_index("base")]).astype(jnp.int32)
    shape = jax.ShapeDtypeStruct
    bf16, f32 = jnp.bfloat16, jnp.float32

    x0_round = x0.astype(bf16)
    shares = [x0_round] + [swap(x0_round, "base", d) for d in range(1, n_base)]
    packed = call(
        functools.partial(pack_body, slots),
        [shape((quarter, slots * TILE), bf16)] * n_pix,
        (where, ranks, a),
        smem=(0, 1),
        name="pack",
    )
    parts = [packed[0]] + [swap(packed[d], "pix", d) for d in range(1, n_pix)]
    firsts = call(
        first_body,
        [shape((chans, quarter), f32)] * n_pix,
        (where, a, *shares),
        scratch=[pltpu.VMEM((chans, n_base * TILE), bf16)],
        smem=(0,),
        name="first",
    )
    preds = [firsts[0]] + [swap(firsts[d], "pix", d) for d in range(1, n_pix)]

    n_pairs = slots * (slots + 1) // 2
    g_rows = n_pairs * TILE // n_base
    per = slots // n_base
    rows = g_rows + per * (4 * chans + PAD)
    chunk = shape((rows, TILE), bf16)
    outs = call(
        functools.partial(gram_body, slots, n_pix),
        [chunk] * n_base,
        (where, ranks, sampled_correlations, x0, *parts, *preds),
        scratch=[pltpu.VMEM((n_base, rows, TILE), bf16)],
        smem=(0, 1),
        name="gram",
    )
    add = functools.partial(sum_body, g_rows, chans, per)
    part = call(add, chunk, [outs[0]] + [swap(outs[d], "base", d) for d in range(1, n_base)], name="sum_base")
    total = call(add, chunk, [part] + [swap(part, "pix", d) for d in range(1, n_pix)], name="sum_pix")

    axes = ("freq", "base")
    got = {0: total}
    for offset in range(2, 2 * n_base, 2):
        got[offset] = swap(total, axes, offset)
    got[1] = swap(total, axes, 1)
    for offset in range(2, 2 * n_base, 2):
        got[offset + 1] = swap(got[offset], axes, 1)
    image = call(
        functools.partial(iterate_body, slots, n_base, g_rows, chans),
        shape((chans, TILE), f32),
        (where, ranks, *[got[i] for i in range(2 * n_base)]),
        scratch=[
            pltpu.VMEM((2, slots * TILE, slots * TILE), bf16),
            pltpu.VMEM((slots, chans, TILE), f32),
        ],
        smem=(0, 1),
        name="iterate",
    )
    return image.reshape(chans, 1, 1, TILE)


def on_device(sensing_operator_parts, sampled_correlations, first_sky_estimate, patch_order_record):
    n_base, n_pix = lax.axis_size("base"), lax.axis_size("pix")
    slots = n_base * n_pix // 4
    chans, m_dev = sampled_correlations.shape
    fits = (
        first_sky_estimate.shape[3] == TILE
        and (slots * TILE) ** 2 <= GRAM_LIMIT
        and n_base & (n_base - 1) == 0
        and n_pix & (n_pix - 1) == 0
        and slots % n_base == 0
        and slots * (slots + 1) // 2 * TILE % (n_base * 16) == 0
        and m_dev % (n_pix * TILE) == 0
        and lax.axis_size("freq") == 2
        and chans % 16 == 0
    )
    plan = gram_plan if fits else streaming
    return plan(sensing_operator_parts, sampled_correlations, first_sky_estimate, patch_order_record)


def solution(mesh):
    in_specs = (
        P("freq", "base", "pix"),
        P("freq", "base"),
        P("freq", "pix", "base", None),
        P(None, "pix"),
    )
    out_specs = P("freq", "pix", "base", None)
    return jax.shard_map(
        on_device, mesh=mesh, in_specs=in_specs, out_specs=out_specs, check_vma=False
    )
```

```python
import functools

import jax
import jax.numpy as jnp
from jax import lax
from jax.experimental import pallas as pl
from jax.experimental.pallas import tpu as pltpu
from jax.sharding import PartitionSpec as P

CH = 64
TILE = 128
ITERS = 6


descent_stride = 0.6
lam_shrink = 0.3
eps_norm = 1e-06

GRAM_LIMIT = 1 << 20
PAD = 16
VMEM_LIMIT = 12 << 20


def project_rows(rounded_amount, columns):
    return lax.dot_general(
        rounded_amount, columns, (((1,), (1,)), ((), ())), preferred_element_type=jnp.float32
    )


def residual_of(sampled_correlations, partial_value):
    shares = lax.psum_scatter(partial_value, "pix", scatter_dimension=1, tiled=True)
    width = shares.shape[1]
    own_rows = lax.dynamic_slice_in_dim(
        sampled_correlations, lax.axis_index("pix") * width, width, 1
    )
    return lax.all_gather((own_rows - shares).astype(jnp.bfloat16), "pix", axis=1, tiled=True)


def streaming(sensing_operator_parts, sampled_correlations, first_sky_estimate, patch_order_record):
    sensing_operator = sensing_operator_parts[0]
    chans, m_dev = sampled_correlations.shape
    share_width = first_sky_estimate.shape[3]
    tiles_share = share_width // TILE
    keep_count = tiles_share * lax.axis_size("base") * lax.axis_size("pix") // 4
    base_index = lax.axis_index("base")
    own_share = first_sky_estimate[:, 0, 0, :]
    current = own_share
    for step in range(ITERS):
        rounded_amount = current.astype(jnp.bfloat16)
        partial_value = project_rows(
            lax.all_gather(rounded_amount, "base", axis=1, tiled=True), sensing_operator
        )
        resid = residual_of(sampled_correlations, partial_value)
        gradient_portion = jnp.dot(resid, sensing_operator, preferred_element_type=jnp.float32)
        grad_share = lax.psum_scatter(gradient_portion, "base", scatter_dimension=1, tiled=True)
        moved = current + descent_stride * grad_share
        tiles = moved.reshape(chans, tiles_share, TILE)
        local_sum = jnp.sum(tiles * tiles, axis=(0, 2))
        total = lax.psum(local_sum, "freq")
        ranks = lax.dynamic_slice_in_dim(
            patch_order_record[step], base_index * tiles_share, tiles_share, 0
        )
        rms_tile = jnp.sqrt(total / (CH * TILE) + eps_norm)
        keeping = (ranks < keep_count).astype(jnp.float32)
        factor = keeping * rms_tile / (rms_tile + lam_shrink)
        current = (tiles * factor[None, :, None]).reshape(chans, share_width)
    return current.reshape(chans, 1, 1, share_width)


def swap(value, axis, offset):
    size = lax.axis_size(axis)
    return lax.ppermute(value, axis, [(i, i ^ offset) for i in range(size)])


def call(body, out_shape, args, scratch=(), smem=(), name=None):
    specs = [
        pl.BlockSpec(memory_space=pltpu.SMEM if i in smem else pltpu.VMEM) for i in range(len(args))
    ]
    out_specs = jax.tree.map(lambda _: pl.BlockSpec(memory_space=pltpu.VMEM), out_shape)
    return pl.pallas_call(
        body,
        out_shape=out_shape,
        in_specs=specs,
        out_specs=out_specs,
        scratch_shapes=list(scratch),
        compiler_params=pltpu.CompilerParams(vmem_limit_bytes=VMEM_LIMIT),
        name=name,
    )(*args)


def split(value):
    high = value.astype(jnp.bfloat16)
    return high, (value - high.astype(jnp.float32)).astype(jnp.bfloat16)


def pack_body(slots, where_ref, ranks_ref, a_ref, *outs):
    pix = where_ref[0]
    tiles = a_ref.shape[1] // TILE
    quarter = outs[0].shape[0]
    for d, out in enumerate(outs):
        rows = pl.ds(pl.multiple_of((pix ^ d) * quarter, quarter), quarter)
        for r in range(slots):
            tile = jnp.int32(0)
            owned = jnp.int32(0)
            for j in range(tiles):
                hit = ranks_ref[0, j] == r
                tile = jnp.where(hit, j, tile)
                owned = jnp.where(hit, 1, owned)
            block = a_ref[rows, pl.ds(pl.multiple_of(tile * TILE, TILE), TILE)]
            out[:, r * TILE : (r + 1) * TILE] = jnp.where(owned == 1, block, jnp.zeros_like(block))


def first_body(where_ref, a_ref, *refs):
    pix, base = where_ref[0], where_ref[1]
    n_base = a_ref.shape[1] // TILE
    shares, rest = refs[:n_base], refs[n_base:]
    outs, x_ref = rest[:-1], rest[-1]
    quarter = outs[0].shape[1]
    for d, share in enumerate(shares):
        x_ref[:, pl.ds(pl.multiple_of((base ^ d) * TILE, TILE), TILE)] = share[...]
    for d, out in enumerate(outs):
        rows = pl.ds(pl.multiple_of((pix ^ d) * quarter, quarter), quarter)
        out[...] = lax.dot_general(
            x_ref[...], a_ref[rows, :], (((1,), (1,)), ((), ())), preferred_element_type=jnp.float32
        )


def in_order(values, index):
    bit = 1
    while bit < len(values):
        odd = (index & bit) != 0
        values = [jnp.where(odd, values[d ^ bit], values[d]) for d in range(len(values))]
        bit *= 2
    return values


def pairs(slots):
    return [(r, s) for r in range(slots) for s in range(r, slots)]


def gram_body(slots, n_pix, where_ref, ranks_ref, y_ref, x0_ref, *refs):
    pix, base = where_ref[0], where_ref[1]
    parts, preds = refs[:n_pix], refs[n_pix : 2 * n_pix]
    *outs, all_ref = refs[2 * n_pix :]
    n_base = len(outs)
    chans, quarter = preds[0].shape
    a = parts[0][...]
    for part in parts[1:]:
        a = a + part[...]
    pred = preds[0][...]
    for piece in preds[1:]:
        pred = pred + piece[...]
    y = y_ref[:, pl.ds(pl.multiple_of(pix * quarter, quarter), quarter)]
    resid = (y - pred).astype(jnp.bfloat16)
    y_hi, y_lo = split(y)
    left = jnp.concatenate([y_hi, y_lo, resid], axis=0)
    sides = jnp.dot(left, a, preferred_element_type=jnp.float32)
    data = sides[:chans] + sides[chans : 2 * chans]
    moved = descent_stride * sides[2 * chans :]
    rank = ranks_ref[0, base]
    gram = lax.dot_general(a, a, (((0,), (0,)), ((), ())), preferred_element_type=jnp.float32)
    rows = lax.broadcasted_iota(jnp.int32, (TILE, TILE), 0)
    cols = lax.broadcasted_iota(jnp.int32, (TILE, TILE), 1)
    here = rows == cols
    n_pairs = len(pairs(slots))
    g_rows = n_pairs * TILE // n_base
    per = slots // n_base
    side_rows = 4 * chans + PAD
    half = min(TILE, g_rows & -g_rows)
    diags = {}
    for i, (r, s) in enumerate(pairs(slots)):
        block = gram[r * TILE : (r + 1) * TILE, s * TILE : (s + 1) * TILE]
        if r == s:
            diags[r] = jnp.sum(jnp.where(here, block, 0.0), axis=0, keepdims=True)
            block = jnp.where(here, 0.0, block)
        block = block.astype(jnp.bfloat16)
        for q in range(TILE // half):
            at = i * TILE + q * half
            all_ref[at // g_rows, at % g_rows : at % g_rows + half, :] = block[q * half : (q + 1) * half]
    for r in range(slots):
        lanes = slice(r * TILE, (r + 1) * TILE)
        start = jnp.where(rank == r, x0_ref[...], 0.0)
        d_hi, d_lo = split(diags[r])
        stack = [
            *split(data[:, lanes]),
            *split(moved[:, lanes] + start),
            d_hi,
            d_lo,
            jnp.zeros((PAD - 2, TILE), jnp.bfloat16),
        ]
        at = g_rows + (r % per) * side_rows
        for piece in stack[:4]:
            all_ref[r // per, at : at + chans, :] = piece
            at += chans
        all_ref[r // per, at : at + PAD, :] = jnp.concatenate(stack[4:], axis=0)
    for d, out in enumerate(outs):
        out[...] = all_ref[base ^ d]


def sum_body(g_rows, chans, per, *refs):
    *parts, out = refs

    def total(at, size):
        value = parts[0][at : at + size].astype(jnp.float32)
        for part in parts[1:]:
            value = value + part[at : at + size].astype(jnp.float32)
        return value

    out[:g_rows] = total(0, g_rows).astype(jnp.bfloat16)
    at = g_rows
    for _ in range(per):
        for _ in range(2):
            high, low = split(total(at, chans) + total(at + chans, chans))
            out[at : at + chans] = high
            out[at + chans : at + 2 * chans] = low
            at += 2 * chans
        tail = total(at, PAD)
        high, low = split(tail[0:1] + tail[1:2])
        rest = jnp.zeros((PAD - 2, TILE), jnp.bfloat16)
        out[at : at + PAD] = jnp.concatenate([high, low, rest], axis=0)
        at += PAD


def iterate_body(slots, n_base, g_rows, chans, where_ref, ranks_ref, *refs):
    base = where_ref[1]
    per = slots // n_base
    side_rows = 4 * chans + PAD
    chunks = [refs[:n_base], refs[n_base : 2 * n_base]]
    out_ref, gram_ref, last_ref = refs[2 * n_base :]
    states, datas, diags = [], [], []
    for g in range(2):
        full = in_order([ref[...] for ref in chunks[g]], base)
        half = min(TILE, g_rows & -g_rows)
        for i, (r, s) in enumerate(pairs(slots)):
            pieces = []
            for q in range(TILE // half):
                at = i * TILE + q * half
                pieces.append(full[at // g_rows][at % g_rows : at % g_rows + half])
            block = jnp.concatenate(pieces, axis=0)
            gram_ref[g, r * TILE : (r + 1) * TILE, s * TILE : (s + 1) * TILE] = block
            if r != s:
                gram_ref[g, s * TILE : (s + 1) * TILE, r * TILE : (r + 1) * TILE] = block.T
        sides = [full[r // per][g_rows + (r % per) * side_rows :][:side_rows].astype(jnp.float32) for r in range(slots)]
        wide = lambda at: jnp.concatenate([v[at : at + chans] + v[at + chans : at + 2 * chans] for v in sides], axis=1)
        datas.append(wide(0))
        states.append(wide(2 * chans))
        tails = [v[4 * chans :] for v in sides]
        diags.append(jnp.concatenate([t[0:1] + t[1:2] for t in tails], axis=1))
    for step in range(ITERS):
        factors = []
        for r in range(slots):
            lanes = slice(r * TILE, (r + 1) * TILE)
            square = states[0][:, lanes] * states[0][:, lanes] + states[1][:, lanes] * states[1][:, lanes]
            column = jnp.sum(square, axis=0, keepdims=True)
            norm = jnp.sum(column, axis=1, keepdims=True)
            rms = jnp.sqrt(norm / (CH * TILE) + eps_norm)
            factors.append(jnp.broadcast_to(rms / (rms + lam_shrink), (1, TILE)))
        factor = jnp.concatenate(factors, axis=1)
        states = [state * factor for state in states]
        if step == ITERS - 1:
            break
        for g in range(2):
            high, low = split(states[g])
            both = jnp.dot(
                jnp.concatenate([high, low], axis=0), gram_ref[g], preferred_element_type=jnp.float32
            )
            product = both[:chans] + both[chans:] + states[g] * diags[g]
            states[g] = states[g] + descent_stride * (datas[g] - product)
    for r in range(slots):
        last_ref[r] = states[0][:, r * TILE : (r + 1) * TILE]
    rank = ranks_ref[0, base]
    kept = last_ref[jnp.minimum(rank, slots - 1)]
    out_ref[...] = jnp.where(rank < slots, kept, 0.0)


def gram_plan(sensing_operator_parts, sampled_correlations, first_sky_estimate, patch_order_record):
    a = sensing_operator_parts[0]
    chans, m_dev = sampled_correlations.shape
    n_base, n_pix = lax.axis_size("base"), lax.axis_size("pix")
    slots = n_base * n_pix // 4
    quarter = m_dev // n_pix
    x0 = first_sky_estimate[:, 0, 0, :]
    ranks = patch_order_record
    where = jnp.stack([lax.axis_index("pix"), lax.axis_index("base")]).astype(jnp.int32)
    shape = jax.ShapeDtypeStruct
    bf16, f32 = jnp.bfloat16, jnp.float32

    x0_round = x0.astype(bf16)
    shares = [x0_round] + [swap(x0_round, "base", d) for d in range(1, n_base)]
    packed = call(
        functools.partial(pack_body, slots),
        [shape((quarter, slots * TILE), bf16)] * n_pix,
        (where, ranks, a),
        smem=(0, 1),
        name="pack",
    )
    parts = [packed[0]] + [swap(packed[d], "pix", d) for d in range(1, n_pix)]
    firsts = call(
        first_body,
        [shape((chans, quarter), f32)] * n_pix,
        (where, a, *shares),
        scratch=[pltpu.VMEM((chans, n_base * TILE), bf16)],
        smem=(0,),
        name="first",
    )
    preds = [firsts[0]] + [swap(firsts[d], "pix", d) for d in range(1, n_pix)]

    n_pairs = slots * (slots + 1) // 2
    g_rows = n_pairs * TILE // n_base
    per = slots // n_base
    rows = g_rows + per * (4 * chans + PAD)
    chunk = shape((rows, TILE), bf16)
    outs = call(
        functools.partial(gram_body, slots, n_pix),
        [chunk] * n_base,
        (where, ranks, sampled_correlations, x0, *parts, *preds),
        scratch=[pltpu.VMEM((n_base, rows, TILE), bf16)],
        smem=(0, 1),
        name="gram",
    )
    add = functools.partial(sum_body, g_rows, chans, per)
    part = call(add, chunk, [outs[0]] + [swap(outs[d], "base", d) for d in range(1, n_base)], name="sum_base")
    total = call(add, chunk, [part] + [swap(part, "pix", d) for d in range(1, n_pix)], name="sum_pix")

    axes = ("freq", "base")
    got = {0: total}
    for offset in range(2, 2 * n_base, 2):
        got[offset] = swap(total, axes, offset)
    got[1] = swap(total, axes, 1)
    for offset in range(2, 2 * n_base, 2):
        got[offset + 1] = swap(got[offset], axes, 1)
    image = call(
        functools.partial(iterate_body, slots, n_base, g_rows, chans),
        shape((chans, TILE), f32),
        (where, ranks, *[got[i] for i in range(2 * n_base)]),
        scratch=[
            pltpu.VMEM((2, slots * TILE, slots * TILE), bf16),
            pltpu.VMEM((slots, chans, TILE), f32),
        ],
        smem=(0, 1),
        name="iterate",
    )
    return image.reshape(chans, 1, 1, TILE)


def on_device(sensing_operator_parts, sampled_correlations, first_sky_estimate, patch_order_record):
    n_base, n_pix = lax.axis_size("base"), lax.axis_size("pix")
    slots = n_base * n_pix // 4
    chans, m_dev = sampled_correlations.shape
    fits = (
        first_sky_estimate.shape[3] == TILE
        and (slots * TILE) ** 2 <= GRAM_LIMIT
        and n_base & (n_base - 1) == 0
        and n_pix & (n_pix - 1) == 0
        and slots % n_base == 0
        and slots * (slots + 1) // 2 * TILE % (n_base * 16) == 0
        and m_dev % (n_pix * TILE) == 0
        and lax.axis_size("freq") == 2
        and chans % 16 == 0
    )
    plan = gram_plan if fits else streaming
    return plan(sensing_operator_parts, sampled_correlations, first_sky_estimate, patch_order_record)


def solution(mesh):
    in_specs = (
        P("freq", "base", "pix"),
        P("freq", "base"),
        P("freq", "pix", "base", None),
        P(None, "pix"),
    )
    out_specs = P("freq", "pix", "base", None)
    return jax.shard_map(
        on_device, mesh=mesh, in_specs=in_specs, out_specs=out_specs, check_vma=False
    )
```

```python
import functools

import jax
import jax.numpy as jnp
from jax import lax
from jax.experimental import pallas as pl
from jax.experimental.pallas import tpu as pltpu
from jax.sharding import PartitionSpec as P

CH = 64
TILE = 128
ITERS = 6


descent_stride = 0.6
lam_shrink = 0.3
eps_norm = 1e-06

GRAM_LIMIT = 1 << 20
PAD = 16
CAPACITY = 2
VMEM_LIMIT = 12 << 20


def project_rows(rounded_amount, columns):
    return lax.dot_general(
        rounded_amount, columns, (((1,), (1,)), ((), ())), preferred_element_type=jnp.float32
    )


def residual_of(sampled_correlations, partial_value):
    shares = lax.psum_scatter(partial_value, "pix", scatter_dimension=1, tiled=True)
    width = shares.shape[1]
    own_rows = lax.dynamic_slice_in_dim(
        sampled_correlations, lax.axis_index("pix") * width, width, 1
    )
    return lax.all_gather((own_rows - shares).astype(jnp.bfloat16), "pix", axis=1, tiled=True)


def streaming(sensing_operator_parts, sampled_correlations, first_sky_estimate, patch_order_record):
    sensing_operator = sensing_operator_parts[0]
    chans, m_dev = sampled_correlations.shape
    share_width = first_sky_estimate.shape[3]
    tiles_share = share_width // TILE
    keep_count = tiles_share * lax.axis_size("base") * lax.axis_size("pix") // 4
    base_index = lax.axis_index("base")
    own_share = first_sky_estimate[:, 0, 0, :]
    current = own_share
    for step in range(ITERS):
        rounded_amount = current.astype(jnp.bfloat16)
        partial_value = project_rows(
            lax.all_gather(rounded_amount, "base", axis=1, tiled=True), sensing_operator
        )
        resid = residual_of(sampled_correlations, partial_value)
        gradient_portion = jnp.dot(resid, sensing_operator, preferred_element_type=jnp.float32)
        grad_share = lax.psum_scatter(gradient_portion, "base", scatter_dimension=1, tiled=True)
        moved = current + descent_stride * grad_share
        tiles = moved.reshape(chans, tiles_share, TILE)
        local_sum = jnp.sum(tiles * tiles, axis=(0, 2))
        total = lax.psum(local_sum, "freq")
        ranks = lax.dynamic_slice_in_dim(
            patch_order_record[step], base_index * tiles_share, tiles_share, 0
        )
        rms_tile = jnp.sqrt(total / (CH * TILE) + eps_norm)
        keeping = (ranks < keep_count).astype(jnp.float32)
        factor = keeping * rms_tile / (rms_tile + lam_shrink)
        current = (tiles * factor[None, :, None]).reshape(chans, share_width)
    return current.reshape(chans, 1, 1, share_width)


def swap(value, axis, offset):
    size = lax.axis_size(axis)
    return lax.ppermute(value, axis, [(i, i ^ offset) for i in range(size)])


def call(body, out_shape, args, scratch=(), smem=(), name=None):
    specs = [
        pl.BlockSpec(memory_space=pltpu.SMEM if i in smem else pltpu.VMEM) for i in range(len(args))
    ]
    out_specs = jax.tree.map(lambda _: pl.BlockSpec(memory_space=pltpu.VMEM), out_shape)
    return pl.pallas_call(
        body,
        out_shape=out_shape,
        in_specs=specs,
        out_specs=out_specs,
        scratch_shapes=list(scratch),
        compiler_params=pltpu.CompilerParams(vmem_limit_bytes=VMEM_LIMIT),
        name=name,
    )(*args)


def split(value):
    high = value.astype(jnp.bfloat16)
    return high, (value - high.astype(jnp.float32)).astype(jnp.bfloat16)


def kept_tiles(ranks_ref, slots):
    count = jnp.int32(0)
    table = []
    for j in range(ranks_ref.shape[0]):
        rank = ranks_ref[j, 0]
        kept = rank < slots
        table.append((rank, kept, count))
        count = count + jnp.where(kept, 1, 0)
    return table, count


def pack_body(slots, first, where_ref, ranks_ref, a_ref, *outs):
    pix = where_ref[0]
    quarter = a_ref.shape[0] // (len(outs) + 1)
    places = (outs[0].shape[0] - PAD) // quarter
    table, count = kept_tiles(ranks_ref, slots)
    rows = lax.broadcasted_iota(jnp.int32, (PAD, TILE), 0)
    notes = jnp.where(rows == PAD - 1, count, -1)
    for i in range(places):
        tile, slot = jnp.int32(0), jnp.int32(-1)
        for j, (rank, kept, before) in enumerate(table):
            hit = jnp.logical_and(kept, before == first + i)
            tile = jnp.where(hit, j, tile)
            slot = jnp.where(hit, rank, slot)
        notes = jnp.where(rows == i, slot, notes)
        lanes = pl.ds(pl.multiple_of(tile * TILE, TILE), TILE)
        for d, out in enumerate(outs):
            at = pl.ds(pl.multiple_of((pix ^ (d + 1)) * quarter, quarter), quarter)
            out[i * quarter : (i + 1) * quarter, :] = a_ref[at, lanes]
    for out in outs:
        out[places * quarter :, :] = notes.astype(jnp.float32).astype(jnp.bfloat16)


def first_body(where_ref, a_ref, *refs):
    pix, base = where_ref[0], where_ref[1]
    n_base = a_ref.shape[1] // TILE
    shares, rest = refs[:n_base], refs[n_base:]
    outs, x_ref = rest[:-1], rest[-1]
    quarter = outs[0].shape[1]
    for d, share in enumerate(shares):
        x_ref[:, pl.ds(pl.multiple_of((base ^ d) * TILE, TILE), TILE)] = share[...]
    for d, out in enumerate(outs):
        rows = pl.ds(pl.multiple_of((pix ^ d) * quarter, quarter), quarter)
        piece = lax.dot_general(
            x_ref[...], a_ref[rows, :], (((1,), (1,)), ((), ())), preferred_element_type=jnp.float32
        )
        out[...] = piece.astype(out.dtype)


def in_order(values, index):
    bit = 1
    while bit < len(values):
        odd = (index & bit) != 0
        values = [jnp.where(odd, values[d ^ bit], values[d]) for d in range(len(values))]
        bit *= 2
    return values


def pairs(slots):
    return [(r, s) for r in range(slots) for s in range(r, slots)]


def gram_body(slots, n_pix, n_parts, where_ref, ranks_ref, y_ref, x0_ref, a_ref, *refs):
    pix, base = where_ref[0], where_ref[1]
    parts, preds = refs[:n_parts], refs[n_parts : n_parts + n_pix]
    *outs, all_ref = refs[n_parts + n_pix :]
    n_base = len(outs)
    chans, quarter = preds[0].shape
    table, _ = kept_tiles(ranks_ref, slots)
    own_rows = pl.ds(pl.multiple_of(pix * quarter, quarter), quarter)
    columns = []
    for r in range(slots):
        tile, owned = jnp.int32(0), jnp.int32(0)
        for j, (rank, _, _) in enumerate(table):
            tile = jnp.where(rank == r, j, tile)
            owned = jnp.where(rank == r, 1, owned)
        block = a_ref[own_rows, pl.ds(pl.multiple_of(tile * TILE, TILE), TILE)]
        block = jnp.where(owned == 1, block, jnp.zeros_like(block))
        for part in parts:
            places = (part.shape[0] - PAD) // quarter
            notes = part[places * quarter :, :].astype(jnp.float32)
            for i in range(places):
                hit = jnp.broadcast_to(notes[i : i + 1] == r, block.shape)
                block = jnp.where(hit, part[i * quarter : (i + 1) * quarter, :], block)
        columns.append(block)
    a = jnp.concatenate(columns, axis=1)
    pred = preds[0][...].astype(jnp.float32)
    for piece in preds[1:]:
        pred = pred + piece[...].astype(jnp.float32)
    y = y_ref[:, pl.ds(pl.multiple_of(pix * quarter, quarter), quarter)]
    resid = (y - pred).astype(jnp.bfloat16)
    y_hi, y_lo = split(y)
    left = jnp.concatenate([y_hi, y_lo, resid], axis=0)
    sides = jnp.dot(left, a, preferred_element_type=jnp.float32)
    data = sides[:chans] + sides[chans : 2 * chans]
    moved = descent_stride * sides[2 * chans :]
    rank = ranks_ref[base, 0]
    gram = lax.dot_general(a, a, (((0,), (0,)), ((), ())), preferred_element_type=jnp.float32)
    rows = lax.broadcasted_iota(jnp.int32, (TILE, TILE), 0)
    cols = lax.broadcasted_iota(jnp.int32, (TILE, TILE), 1)
    here = rows == cols
    n_pairs = len(pairs(slots))
    g_rows = n_pairs * TILE // n_base
    per = slots // n_base
    side_rows = 4 * chans + PAD
    half = min(TILE, g_rows & -g_rows)
    diags = {}
    for i, (r, s) in enumerate(pairs(slots)):
        block = gram[r * TILE : (r + 1) * TILE, s * TILE : (s + 1) * TILE]
        if r == s:
            diags[r] = jnp.sum(jnp.where(here, block, 0.0), axis=0, keepdims=True)
            block = jnp.where(here, 0.0, block)
        block = block.astype(jnp.bfloat16)
        for q in range(TILE // half):
            at = i * TILE + q * half
            all_ref[at // g_rows, at % g_rows : at % g_rows + half, :] = block[q * half : (q + 1) * half]
    for r in range(slots):
        lanes = slice(r * TILE, (r + 1) * TILE)
        start = jnp.where(rank == r, x0_ref[...], 0.0)
        d_hi, d_lo = split(diags[r])
        stack = [
            *split(data[:, lanes]),
            *split(moved[:, lanes] + start),
            d_hi,
            d_lo,
            jnp.zeros((PAD - 2, TILE), jnp.bfloat16),
        ]
        at = g_rows + (r % per) * side_rows
        for piece in stack[:4]:
            all_ref[r // per, at : at + chans, :] = piece
            at += chans
        all_ref[r // per, at : at + PAD, :] = jnp.concatenate(stack[4:], axis=0)
    for d, out in enumerate(outs):
        out[...] = all_ref[base ^ d]


def sum_body(g_rows, chans, per, *refs):
    *parts, out = refs

    def total(at, size):
        value = parts[0][at : at + size].astype(jnp.float32)
        for part in parts[1:]:
            value = value + part[at : at + size].astype(jnp.float32)
        return value

    out[:g_rows] = total(0, g_rows).astype(jnp.bfloat16)
    at = g_rows
    for _ in range(per):
        for _ in range(2):
            high, low = split(total(at, chans) + total(at + chans, chans))
            out[at : at + chans] = high
            out[at + chans : at + 2 * chans] = low
            at += 2 * chans
        tail = total(at, PAD)
        high, low = split(tail[0:1] + tail[1:2])
        rest = jnp.zeros((PAD - 2, TILE), jnp.bfloat16)
        out[at : at + PAD] = jnp.concatenate([high, low, rest], axis=0)
        at += PAD


def iterate_body(slots, n_base, g_rows, chans, where_ref, ranks_ref, *refs):
    base = where_ref[1]
    per = slots // n_base
    side_rows = 4 * chans + PAD
    chunks = [refs[:n_base], refs[n_base : 2 * n_base]]
    out_ref, gram_ref, last_ref = refs[2 * n_base :]
    states, datas, diags = [], [], []
    for g in range(2):
        full = in_order([ref[...] for ref in chunks[g]], base)
        half = min(TILE, g_rows & -g_rows)
        for i, (r, s) in enumerate(pairs(slots)):
            pieces = []
            for q in range(TILE // half):
                at = i * TILE + q * half
                pieces.append(full[at // g_rows][at % g_rows : at % g_rows + half])
            block = jnp.concatenate(pieces, axis=0)
            gram_ref[g, r * TILE : (r + 1) * TILE, s * TILE : (s + 1) * TILE] = block
            if r != s:
                gram_ref[g, s * TILE : (s + 1) * TILE, r * TILE : (r + 1) * TILE] = block.T
        sides = [full[r // per][g_rows + (r % per) * side_rows :][:side_rows].astype(jnp.float32) for r in range(slots)]
        wide = lambda at: jnp.concatenate([v[at : at + chans] + v[at + chans : at + 2 * chans] for v in sides], axis=1)
        datas.append(wide(0))
        states.append(wide(2 * chans))
        tails = [v[4 * chans :] for v in sides]
        diags.append(jnp.concatenate([t[0:1] + t[1:2] for t in tails], axis=1))
    for step in range(ITERS):
        factors = []
        for r in range(slots):
            lanes = slice(r * TILE, (r + 1) * TILE)
            square = states[0][:, lanes] * states[0][:, lanes] + states[1][:, lanes] * states[1][:, lanes]
            column = jnp.sum(square, axis=0, keepdims=True)
            norm = jnp.sum(column, axis=1, keepdims=True)
            rms = jnp.sqrt(norm / (CH * TILE) + eps_norm)
            factors.append(jnp.broadcast_to(rms / (rms + lam_shrink), (1, TILE)))
        factor = jnp.concatenate(factors, axis=1)
        states = [state * factor for state in states]
        if step == ITERS - 1:
            break
        for g in range(2):
            high, low = split(states[g])
            both = jnp.dot(
                jnp.concatenate([high, low], axis=0), gram_ref[g], preferred_element_type=jnp.float32
            )
            product = both[:chans] + both[chans:] + states[g] * diags[g]
            states[g] = states[g] + descent_stride * (datas[g] - product)
    for r in range(slots):
        last_ref[r] = states[0][:, r * TILE : (r + 1) * TILE]
    rank = ranks_ref[base, 0]
    kept = last_ref[jnp.minimum(rank, slots - 1)]
    out_ref[...] = jnp.where(rank < slots, kept, 0.0)


def gram_plan(sensing_operator_parts, sampled_correlations, first_sky_estimate, patch_order_record):
    a = sensing_operator_parts[0]
    chans, m_dev = sampled_correlations.shape
    n_base, n_pix = lax.axis_size("base"), lax.axis_size("pix")
    slots = n_base * n_pix // 4
    quarter = m_dev // n_pix
    x0 = first_sky_estimate[:, 0, 0, :]
    ranks = patch_order_record.T
    where = jnp.stack([lax.axis_index("pix"), lax.axis_index("base")]).astype(jnp.int32)
    shape = jax.ShapeDtypeStruct
    bf16, f32 = jnp.bfloat16, jnp.float32

    def exchange(first, places):
        packed = call(
            functools.partial(pack_body, slots, first),
            [shape((places * quarter + PAD, TILE), bf16)] * (n_pix - 1),
            (where, ranks, a),
            smem=(0, 1),
            name="pack",
        )
        return [swap(piece, "pix", d + 1) for d, piece in enumerate(packed)]

    places = min(CAPACITY, ranks.shape[0])
    parts = exchange(0, places)
    x0_round = x0.astype(bf16)
    shares = [x0_round] + [swap(x0_round, "base", d) for d in range(1, n_base)]
    firsts = call(
        first_body,
        [shape((chans, quarter), bf16)] * n_pix,
        (where, a, *shares),
        scratch=[pltpu.VMEM((chans, n_base * TILE), bf16)],
        smem=(0,),
        name="first",
    )
    preds = [firsts[0]] + [swap(firsts[d], "pix", d) for d in range(1, n_pix)]

    n_pairs = slots * (slots + 1) // 2
    g_rows = n_pairs * TILE // n_base
    per = slots // n_base
    rows = g_rows + per * (4 * chans + PAD)
    chunk = shape((rows, TILE), bf16)

    def gram(parts):
        return call(
            functools.partial(gram_body, slots, n_pix, len(parts)),
            [chunk] * n_base,
            (where, ranks, sampled_correlations, x0, a, *parts, *preds),
            scratch=[pltpu.VMEM((n_base, rows, TILE), bf16)],
            smem=(0, 1),
            name="gram",
        )

    counts = [part[-1, 0].astype(f32) for part in parts]
    counts.append(jnp.sum((ranks[:, 0] < slots).astype(f32)))
    crowded = functools.reduce(jnp.maximum, counts) > places
    outs = lax.cond(
        crowded,
        lambda: gram(parts + exchange(places, ranks.shape[0] - places)),
        lambda: gram(parts),
    )
    add = functools.partial(sum_body, g_rows, chans, per)
    part = call(add, chunk, [outs[0]] + [swap(outs[d], "base", d) for d in range(1, n_base)], name="sum_base")
    total = call(add, chunk, [part] + [swap(part, "pix", d) for d in range(1, n_pix)], name="sum_pix")

    axes = ("freq", "base")
    got = {0: total}
    for offset in range(2, 2 * n_base, 2):
        got[offset] = swap(total, axes, offset)
    got[1] = swap(total, axes, 1)
    for offset in range(2, 2 * n_base, 2):
        got[offset + 1] = swap(got[offset], axes, 1)
    image = call(
        functools.partial(iterate_body, slots, n_base, g_rows, chans),
        shape((chans, TILE), f32),
        (where, ranks, *[got[i] for i in range(2 * n_base)]),
        scratch=[
            pltpu.VMEM((2, slots * TILE, slots * TILE), bf16),
            pltpu.VMEM((slots, chans, TILE), f32),
        ],
        smem=(0, 1),
        name="iterate",
    )
    return image.reshape(chans, 1, 1, TILE)


def on_device(sensing_operator_parts, sampled_correlations, first_sky_estimate, patch_order_record):
    n_base, n_pix = lax.axis_size("base"), lax.axis_size("pix")
    slots = n_base * n_pix // 4
    chans, m_dev = sampled_correlations.shape
    fits = (
        first_sky_estimate.shape[3] == TILE
        and (slots * TILE) ** 2 <= GRAM_LIMIT
        and n_base & (n_base - 1) == 0
        and n_pix & (n_pix - 1) == 0
        and slots % n_base == 0
        and slots * (slots + 1) // 2 * TILE % (n_base * 16) == 0
        and m_dev % (n_pix * TILE) == 0
        and lax.axis_size("freq") == 2
        and chans % 16 == 0
    )
    plan = gram_plan if fits else streaming
    return plan(sensing_operator_parts, sampled_correlations, first_sky_estimate, patch_order_record)


def solution(mesh):
    in_specs = (
        P("freq", "base", "pix"),
        P("freq", "base"),
        P("freq", "pix", "base", None),
        P(None, "pix"),
    )
    out_specs = P("freq", "pix", "base", None)
    return jax.shard_map(
        on_device, mesh=mesh, in_specs=in_specs, out_specs=out_specs, check_vma=False
    )
```

```python
import functools

import jax
import jax.numpy as jnp
from jax import lax
from jax.experimental import pallas as pl
from jax.experimental.pallas import tpu as pltpu
from jax.sharding import PartitionSpec as P

CH = 64
TILE = 128
ITERS = 6


descent_stride = 0.6
lam_shrink = 0.3
eps_norm = 1e-06

GRAM_LIMIT = 1 << 20
PAD = 16
CAPACITY = 2
VMEM_LIMIT = 12 << 20


def project_rows(rounded_amount, columns):
    return lax.dot_general(
        rounded_amount, columns, (((1,), (1,)), ((), ())), preferred_element_type=jnp.float32
    )


def residual_of(sampled_correlations, partial_value):
    shares = lax.psum_scatter(partial_value, "pix", scatter_dimension=1, tiled=True)
    width = shares.shape[1]
    own_rows = lax.dynamic_slice_in_dim(
        sampled_correlations, lax.axis_index("pix") * width, width, 1
    )
    return lax.all_gather((own_rows - shares).astype(jnp.bfloat16), "pix", axis=1, tiled=True)


def streaming(sensing_operator_parts, sampled_correlations, first_sky_estimate, patch_order_record):
    sensing_operator = sensing_operator_parts[0]
    chans, m_dev = sampled_correlations.shape
    share_width = first_sky_estimate.shape[3]
    tiles_share = share_width // TILE
    keep_count = tiles_share * lax.axis_size("base") * lax.axis_size("pix") // 4
    base_index = lax.axis_index("base")
    own_share = first_sky_estimate[:, 0, 0, :]
    current = own_share
    for step in range(ITERS):
        rounded_amount = current.astype(jnp.bfloat16)
        partial_value = project_rows(
            lax.all_gather(rounded_amount, "base", axis=1, tiled=True), sensing_operator
        )
        resid = residual_of(sampled_correlations, partial_value)
        gradient_portion = jnp.dot(resid, sensing_operator, preferred_element_type=jnp.float32)
        grad_share = lax.psum_scatter(gradient_portion, "base", scatter_dimension=1, tiled=True)
        moved = current + descent_stride * grad_share
        tiles = moved.reshape(chans, tiles_share, TILE)
        local_sum = jnp.sum(tiles * tiles, axis=(0, 2))
        total = lax.psum(local_sum, "freq")
        ranks = lax.dynamic_slice_in_dim(
            patch_order_record[step], base_index * tiles_share, tiles_share, 0
        )
        rms_tile = jnp.sqrt(total / (CH * TILE) + eps_norm)
        keeping = (ranks < keep_count).astype(jnp.float32)
        factor = keeping * rms_tile / (rms_tile + lam_shrink)
        current = (tiles * factor[None, :, None]).reshape(chans, share_width)
    return current.reshape(chans, 1, 1, share_width)


def swap(value, axis, offset):
    size = lax.axis_size(axis)
    return lax.ppermute(value, axis, [(i, i ^ offset) for i in range(size)])


def call(body, out_shape, args, scratch=(), smem=(), hbm=(), out_space=pltpu.VMEM, name=None):
    places = [pltpu.SMEM if i in smem else pl.ANY if i in hbm else pltpu.VMEM for i in range(len(args))]
    specs = [pl.BlockSpec(memory_space=place) for place in places]
    out_specs = jax.tree.map(lambda _: pl.BlockSpec(memory_space=out_space), out_shape)
    return pl.pallas_call(
        body,
        out_shape=out_shape,
        in_specs=specs,
        out_specs=out_specs,
        scratch_shapes=list(scratch),
        compiler_params=pltpu.CompilerParams(vmem_limit_bytes=VMEM_LIMIT),
        name=name,
    )(*args)


def split(value):
    high = value.astype(jnp.bfloat16)
    return high, (value - high.astype(jnp.float32)).astype(jnp.bfloat16)


def kept_tiles(ranks_ref, slots):
    count = jnp.int32(0)
    table = []
    for j in range(ranks_ref.shape[0]):
        rank = ranks_ref[j, 0]
        kept = rank < slots
        table.append((rank, kept, count))
        count = count + jnp.where(kept, 1, 0)
    return table, count


def pack_body(slots, first, where_ref, ranks_ref, a_ref, *outs):
    pix = where_ref[0]
    quarter = a_ref.shape[0] // (len(outs) + 1)
    places = (outs[0].shape[0] - PAD) // quarter
    table, count = kept_tiles(ranks_ref, slots)
    rows = lax.broadcasted_iota(jnp.int32, (PAD, TILE), 0)
    notes = jnp.where(rows == PAD - 1, count, -1)
    for i in range(places):
        tile, slot = jnp.int32(0), jnp.int32(-1)
        for j, (rank, kept, before) in enumerate(table):
            hit = jnp.logical_and(kept, before == first + i)
            tile = jnp.where(hit, j, tile)
            slot = jnp.where(hit, rank, slot)
        notes = jnp.where(rows == i, slot, notes)
        lanes = pl.ds(pl.multiple_of(tile * TILE, TILE), TILE)
        for d, out in enumerate(outs):
            at = pl.ds(pl.multiple_of((pix ^ (d + 1)) * quarter, quarter), quarter)
            out[i * quarter : (i + 1) * quarter, :] = a_ref[at, lanes]
    for out in outs:
        out[places * quarter :, :] = notes.astype(jnp.float32).astype(jnp.bfloat16)


def crowd_body(slots, places, ranks_ref, *refs):
    *parts, out_ref = refs
    _, count = kept_tiles(ranks_ref, slots)
    most = parts[0][-PAD:, :].astype(jnp.float32)
    for part in parts[1:]:
        most = jnp.maximum(most, part[-PAD:, :].astype(jnp.float32))
    rows = lax.broadcasted_iota(jnp.int32, (PAD, TILE), 0)
    others = jnp.max(jnp.where(rows == PAD - 1, most, -1.0))
    over = jnp.logical_or(others > places, count > places)
    out_ref[0] = jnp.where(over, 1, 0)


def first_body(where_ref, a_ref, *refs):
    pix, base = where_ref[0], where_ref[1]
    n_base = a_ref.shape[1] // TILE
    shares, rest = refs[:n_base], refs[n_base:]
    outs, x_ref = rest[:-1], rest[-1]
    quarter = outs[0].shape[1]
    for d, share in enumerate(shares):
        x_ref[:, pl.ds(pl.multiple_of((base ^ d) * TILE, TILE), TILE)] = share[...]
    for d, out in enumerate(outs):
        rows = pl.ds(pl.multiple_of((pix ^ d) * quarter, quarter), quarter)
        piece = lax.dot_general(
            x_ref[...], a_ref[rows, :], (((1,), (1,)), ((), ())), preferred_element_type=jnp.float32
        )
        out[...] = piece.astype(out.dtype)


def in_order(values, index):
    bit = 1
    while bit < len(values):
        odd = (index & bit) != 0
        values = [jnp.where(odd, values[d ^ bit], values[d]) for d in range(len(values))]
        bit *= 2
    return values


def pairs(slots):
    return [(r, s) for r in range(slots) for s in range(r + 1, slots)] + [(r, r + 1) for r in range(0, slots, 2)]


def pack_rows(slots, n_base):
    return len(pairs(slots)) * TILE // n_base


def corner():
    rows = lax.broadcasted_iota(jnp.int32, (TILE, TILE), 0)
    cols = lax.broadcasted_iota(jnp.int32, (TILE, TILE), 1)
    return rows, cols


def gram_body(slots, n_pix, n_parts, where_ref, ranks_ref, y_ref, x0_ref, a_ref, *refs):
    pix, base = where_ref[0], where_ref[1]
    parts, preds = refs[:n_parts], refs[n_parts : n_parts + n_pix]
    *outs, all_ref = refs[n_parts + n_pix :]
    n_base = len(outs)
    chans, quarter = preds[0].shape
    table, _ = kept_tiles(ranks_ref, slots)
    own_rows = pl.ds(pl.multiple_of(pix * quarter, quarter), quarter)
    columns = []
    for r in range(slots):
        tile, owned = jnp.int32(0), jnp.int32(0)
        for j, (rank, _, _) in enumerate(table):
            tile = jnp.where(rank == r, j, tile)
            owned = jnp.where(rank == r, 1, owned)
        block = a_ref[own_rows, pl.ds(pl.multiple_of(tile * TILE, TILE), TILE)]
        block = jnp.where(owned == 1, block, jnp.zeros_like(block))
        for part in parts:
            places = (part.shape[0] - PAD) // quarter
            notes = part[places * quarter :, :].astype(jnp.float32)
            for i in range(places):
                hit = jnp.broadcast_to(notes[i : i + 1] == r, block.shape)
                block = jnp.where(hit, part[i * quarter : (i + 1) * quarter, :], block)
        columns.append(block)
    a = jnp.concatenate(columns, axis=1)
    pred = preds[0][...].astype(jnp.float32)
    for piece in preds[1:]:
        pred = pred + piece[...].astype(jnp.float32)
    y = y_ref[:, pl.ds(pl.multiple_of(pix * quarter, quarter), quarter)]
    resid = (y - pred).astype(jnp.bfloat16)
    y_hi, y_lo = split(y)
    left = jnp.concatenate([y_hi, y_lo, resid], axis=0)
    sides = jnp.dot(left, a, preferred_element_type=jnp.float32)
    data = sides[:chans] + sides[chans : 2 * chans]
    moved = descent_stride * sides[2 * chans :]
    rank = ranks_ref[base, 0]
    gram = lax.dot_general(a, a, (((0,), (0,)), ((), ())), preferred_element_type=jnp.float32)
    rows, cols = corner()
    g_rows = pack_rows(slots, n_base)
    per = slots // n_base
    side_rows = 4 * chans + PAD
    half = min(TILE, g_rows & -g_rows)

    def block_of(r, s):
        return gram[r * TILE : (r + 1) * TILE, s * TILE : (s + 1) * TILE]

    diags = [jnp.sum(jnp.where(rows == cols, block_of(r, r), 0.0), axis=0, keepdims=True) for r in range(slots)]
    n_off = slots * (slots - 1) // 2
    for i, (r, s) in enumerate(pairs(slots)):
        block = block_of(r, s) if i < n_off else jnp.where(rows < cols, block_of(r, r), block_of(s, s))
        block = block.astype(jnp.bfloat16)
        for q in range(TILE // half):
            at = i * TILE + q * half
            all_ref[at // g_rows, at % g_rows : at % g_rows + half, :] = block[q * half : (q + 1) * half]
    for r in range(slots):
        lanes = slice(r * TILE, (r + 1) * TILE)
        start = jnp.where(rank == r, x0_ref[...], 0.0)
        d_hi, d_lo = split(diags[r])
        stack = [
            *split(data[:, lanes]),
            *split(moved[:, lanes] + start),
            d_hi,
            d_lo,
            jnp.zeros((PAD - 2, TILE), jnp.bfloat16),
        ]
        at = g_rows + (r % per) * side_rows
        for piece in stack[:4]:
            all_ref[r // per, at : at + chans, :] = piece
            at += chans
        all_ref[r // per, at : at + PAD, :] = jnp.concatenate(stack[4:], axis=0)
    for d, out in enumerate(outs):
        out[...] = all_ref[base ^ d]


def sum_body(g_rows, chans, per, *refs):
    *parts, out = refs

    def total(at, size):
        value = parts[0][at : at + size].astype(jnp.float32)
        for part in parts[1:]:
            value = value + part[at : at + size].astype(jnp.float32)
        return value

    out[:g_rows] = total(0, g_rows).astype(jnp.bfloat16)
    at = g_rows
    for _ in range(per):
        for _ in range(2):
            high, low = split(total(at, chans) + total(at + chans, chans))
            out[at : at + chans] = high
            out[at + chans : at + 2 * chans] = low
            at += 2 * chans
        tail = total(at, PAD)
        high, low = split(tail[0:1] + tail[1:2])
        rest = jnp.zeros((PAD - 2, TILE), jnp.bfloat16)
        out[at : at + PAD] = jnp.concatenate([high, low, rest], axis=0)
        at += PAD


def iterate_body(slots, n_base, g_rows, chans, where_ref, ranks_ref, *refs):
    base = where_ref[1]
    per = slots // n_base
    side_rows = 4 * chans + PAD
    chunks = [refs[:n_base], refs[n_base : 2 * n_base]]
    out_ref, gram_ref, last_ref = refs[2 * n_base :]
    states, datas, diags = [], [], []
    rows, cols = corner()
    n_off = slots * (slots - 1) // 2

    def put(g, r, s, block):
        gram_ref[g, r * TILE : (r + 1) * TILE, s * TILE : (s + 1) * TILE] = block

    for g in range(2):
        full = in_order([ref[...] for ref in chunks[g]], base)
        half = min(TILE, g_rows & -g_rows)
        for i, (r, s) in enumerate(pairs(slots)):
            pieces = []
            for q in range(TILE // half):
                at = i * TILE + q * half
                pieces.append(full[at // g_rows][at % g_rows : at % g_rows + half])
            block = jnp.concatenate(pieces, axis=0)
            if i < n_off:
                put(g, r, s, block)
                put(g, s, r, block.T)
            else:
                upper = jnp.where(rows < cols, block, jnp.zeros_like(block))
                lower = jnp.where(rows > cols, block, jnp.zeros_like(block))
                put(g, r, r, upper + upper.T)
                put(g, s, s, lower + lower.T)
        sides = [full[r // per][g_rows + (r % per) * side_rows :][:side_rows].astype(jnp.float32) for r in range(slots)]
        wide = lambda at: jnp.concatenate([v[at : at + chans] + v[at + chans : at + 2 * chans] for v in sides], axis=1)
        datas.append(wide(0))
        states.append(wide(2 * chans))
        tails = [v[4 * chans :] for v in sides]
        diags.append(jnp.concatenate([t[0:1] + t[1:2] for t in tails], axis=1))
    for step in range(ITERS):
        factors = []
        for r in range(slots):
            lanes = slice(r * TILE, (r + 1) * TILE)
            square = states[0][:, lanes] * states[0][:, lanes] + states[1][:, lanes] * states[1][:, lanes]
            column = jnp.sum(square, axis=0, keepdims=True)
            norm = jnp.sum(column, axis=1, keepdims=True)
            rms = jnp.sqrt(norm / (CH * TILE) + eps_norm)
            factors.append(jnp.broadcast_to(rms / (rms + lam_shrink), (1, TILE)))
        factor = jnp.concatenate(factors, axis=1)
        states = [state * factor for state in states]
        if step == ITERS - 1:
            break
        for g in range(2):
            high, low = split(states[g])
            both = jnp.dot(
                jnp.concatenate([high, low], axis=0), gram_ref[g], preferred_element_type=jnp.float32
            )
            product = both[:chans] + both[chans:] + states[g] * diags[g]
            states[g] = states[g] + descent_stride * (datas[g] - product)
    for r in range(slots):
        last_ref[r] = states[0][:, r * TILE : (r + 1) * TILE]
    rank = ranks_ref[base, 0]
    kept = last_ref[jnp.minimum(rank, slots - 1)]
    out_ref[...] = jnp.where(rank < slots, kept, 0.0)


def gram_plan(sensing_operator_parts, sampled_correlations, first_sky_estimate, patch_order_record):
    a = sensing_operator_parts[0]
    chans, m_dev = sampled_correlations.shape
    n_base, n_pix = lax.axis_size("base"), lax.axis_size("pix")
    slots = n_base * n_pix // 4
    quarter = m_dev // n_pix
    x0 = first_sky_estimate[:, 0, 0, :]
    ranks = patch_order_record.T
    where = jnp.stack([lax.axis_index("pix"), lax.axis_index("base")]).astype(jnp.int32)
    shape = jax.ShapeDtypeStruct
    bf16, f32 = jnp.bfloat16, jnp.float32

    def exchange(first, places):
        packed = call(
            functools.partial(pack_body, slots, first),
            [shape((places * quarter + PAD, TILE), bf16)] * (n_pix - 1),
            (where, ranks, a),
            smem=(0, 1),
            name="pack",
        )
        return [swap(piece, "pix", d + 1) for d, piece in enumerate(packed)]

    places = min(CAPACITY, ranks.shape[0])
    parts = exchange(0, places)
    x0_round = x0.astype(bf16)
    shares = [x0_round] + [swap(x0_round, "base", d) for d in range(1, n_base)]
    firsts = call(
        first_body,
        [shape((chans, quarter), bf16)] * n_pix,
        (where, a, *shares),
        scratch=[pltpu.VMEM((chans, n_base * TILE), bf16)],
        smem=(0,),
        name="first",
    )
    preds = [firsts[0]] + [swap(firsts[d], "pix", d) for d in range(1, n_pix)]

    g_rows = pack_rows(slots, n_base)
    per = slots // n_base
    rows = g_rows + per * (4 * chans + PAD)
    chunk = shape((rows, TILE), bf16)

    def gram(parts):
        return call(
            functools.partial(gram_body, slots, n_pix, len(parts)),
            [chunk] * n_base,
            (where, ranks, sampled_correlations, x0, a, *parts, *preds),
            scratch=[pltpu.VMEM((n_base, rows, TILE), bf16)],
            smem=(0, 1),
            name="gram",
        )

    crowded = call(
        functools.partial(crowd_body, slots, places),
        shape((1,), jnp.int32),
        (ranks, *parts),
        smem=(0,),
        out_space=pltpu.SMEM,
        name="crowd",
    )[0]
    outs = lax.cond(
        crowded != 0,
        lambda: gram(parts + exchange(places, ranks.shape[0] - places)),
        lambda: gram(parts),
    )
    add = functools.partial(sum_body, g_rows, chans, per)
    part = call(add, chunk, [outs[0]] + [swap(outs[d], "base", d) for d in range(1, n_base)], name="sum_base")
    total = call(add, chunk, [part] + [swap(part, "pix", d) for d in range(1, n_pix)], name="sum_pix")

    axes = ("freq", "base")
    got = {0: total}
    for offset in range(2, 2 * n_base, 2):
        got[offset] = swap(total, axes, offset)
    got[1] = swap(total, axes, 1)
    for offset in range(2, 2 * n_base, 2):
        got[offset + 1] = swap(got[offset], axes, 1)
    image = call(
        functools.partial(iterate_body, slots, n_base, g_rows, chans),
        shape((chans, TILE), f32),
        (where, ranks, *[got[i] for i in range(2 * n_base)]),
        scratch=[
            pltpu.VMEM((2, slots * TILE, slots * TILE), bf16),
            pltpu.VMEM((slots, chans, TILE), f32),
        ],
        smem=(0, 1),
        name="iterate",
    )
    return image.reshape(chans, 1, 1, TILE)


def on_device(sensing_operator_parts, sampled_correlations, first_sky_estimate, patch_order_record):
    n_base, n_pix = lax.axis_size("base"), lax.axis_size("pix")
    slots = n_base * n_pix // 4
    chans, m_dev = sampled_correlations.shape
    fits = (
        first_sky_estimate.shape[3] == TILE
        and (slots * TILE) ** 2 <= GRAM_LIMIT
        and n_base & (n_base - 1) == 0
        and n_pix & (n_pix - 1) == 0
        and slots % n_base == 0
        and slots % 2 == 0
        and len(pairs(slots)) * TILE % (n_base * 16) == 0
        and m_dev % (n_pix * TILE) == 0
        and lax.axis_size("freq") == 2
        and chans % 16 == 0
    )
    plan = gram_plan if fits else streaming
    return plan(sensing_operator_parts, sampled_correlations, first_sky_estimate, patch_order_record)


def solution(mesh):
    in_specs = (
        P("freq", "base", "pix"),
        P("freq", "base"),
        P("freq", "pix", "base", None),
        P(None, "pix"),
    )
    out_specs = P("freq", "pix", "base", None)
    return jax.shard_map(
        on_device, mesh=mesh, in_specs=in_specs, out_specs=out_specs, check_vma=False
    )
```

```python
import functools

import jax
import jax.numpy as jnp
from jax import lax
from jax.experimental import pallas as pl
from jax.experimental.pallas import tpu as pltpu
from jax.sharding import PartitionSpec as P

CH = 64
TILE = 128
ITERS = 6


descent_stride = 0.6
lam_shrink = 0.3
eps_norm = 1e-06


GRAM_LIMIT = 1 << 20
PAD = 16
CAPACITY = 2
VMEM_LIMIT = 12 << 20


def project_rows(rounded_amount, columns):
    return lax.dot_general(
        rounded_amount, columns, (((1,), (1,)), ((), ())), preferred_element_type=jnp.float32
    )


def residual_of(sampled_correlations, partial_value):
    shares = lax.psum_scatter(partial_value, "pix", scatter_dimension=1, tiled=True)
    width = shares.shape[1]
    own_rows = lax.dynamic_slice_in_dim(
        sampled_correlations, lax.axis_index("pix") * width, width, 1
    )
    return lax.all_gather((own_rows - shares).astype(jnp.bfloat16), "pix", axis=1, tiled=True)


def streaming(sensing_operator_parts, sampled_correlations, first_sky_estimate, patch_order_record):
    sensing_operator = sensing_operator_parts[0]
    chans, _ = sampled_correlations.shape
    share_width = first_sky_estimate.shape[3]
    tiles_share = share_width // TILE
    keep_count = tiles_share * lax.axis_size("base") * lax.axis_size("pix") // 4
    base_index = lax.axis_index("base")
    own_share = first_sky_estimate[:, 0, 0, :]
    current = own_share
    for step in range(ITERS):
        rounded_amount = current.astype(jnp.bfloat16)
        partial_value = project_rows(
            lax.all_gather(rounded_amount, "base", axis=1, tiled=True), sensing_operator
        )
        resid = residual_of(sampled_correlations, partial_value)
        gradient_portion = jnp.dot(resid, sensing_operator, preferred_element_type=jnp.float32)
        grad_share = lax.psum_scatter(gradient_portion, "base", scatter_dimension=1, tiled=True)
        moved = current + descent_stride * grad_share
        tiles = moved.reshape(chans, tiles_share, TILE)
        local_sum = jnp.sum(tiles * tiles, axis=(0, 2))
        total = lax.psum(local_sum, "freq")
        ranks = lax.dynamic_slice_in_dim(
            patch_order_record[step], base_index * tiles_share, tiles_share, 0
        )
        rms_tile = jnp.sqrt(total / (CH * TILE) + eps_norm)
        keeping = (ranks < keep_count).astype(jnp.float32)
        factor = keeping * rms_tile / (rms_tile + lam_shrink)
        current = (tiles * factor[None, :, None]).reshape(chans, share_width)
    return current.reshape(chans, 1, 1, share_width)


def swap(value, axis, offset):
    size = lax.axis_size(axis)
    return lax.ppermute(value, axis, [(i, i ^ offset) for i in range(size)])


def call(body, out_shape, args, scratch=(), smem=(), hbm=(), out_space=pltpu.VMEM):
    places = [pltpu.SMEM if i in smem else pl.ANY if i in hbm else pltpu.VMEM for i in range(len(args))]
    specs = [pl.BlockSpec(memory_space=place) for place in places]
    out_specs = jax.tree.map(lambda _: pl.BlockSpec(memory_space=out_space), out_shape)
    return pl.pallas_call(
        body,
        out_shape=out_shape,
        in_specs=specs,
        out_specs=out_specs,
        scratch_shapes=list(scratch),
        compiler_params=pltpu.CompilerParams(vmem_limit_bytes=VMEM_LIMIT),
    )(*args)


def split(value):
    high = value.astype(jnp.bfloat16)
    return high, (value - high.astype(jnp.float32)).astype(jnp.bfloat16)


def kept_tiles(ranks_ref, slots):
    count = jnp.int32(0)
    table = []
    for j in range(ranks_ref.shape[0]):
        rank = ranks_ref[j, 0]
        kept = rank < slots
        table.append((rank, kept, count))
        count = count + jnp.where(kept, 1, 0)
    return table, count


def pack_body(slots, first, where_ref, ranks_ref, a_ref, *outs):
    pix = where_ref[0]
    quarter = a_ref.shape[0] // (len(outs) + 1)
    places = (outs[0].shape[0] - PAD) // quarter
    table, count = kept_tiles(ranks_ref, slots)
    rows = lax.broadcasted_iota(jnp.int32, (PAD, TILE), 0)
    notes = jnp.where(rows == PAD - 1, count, -1)
    for i in range(places):
        tile, slot = jnp.int32(0), jnp.int32(-1)
        for j, (rank, kept, before) in enumerate(table):
            hit = jnp.logical_and(kept, before == first + i)
            tile = jnp.where(hit, j, tile)
            slot = jnp.where(hit, rank, slot)
        notes = jnp.where(rows == i, slot, notes)
        lanes = pl.ds(pl.multiple_of(tile * TILE, TILE), TILE)
        for d, out in enumerate(outs):
            at = pl.ds(pl.multiple_of((pix ^ (d + 1)) * quarter, quarter), quarter)
            out[i * quarter : (i + 1) * quarter, :] = a_ref[at, lanes]
    for out in outs:
        out[places * quarter :, :] = notes.astype(jnp.float32).astype(jnp.bfloat16)


def crowd_body(slots, places, ranks_ref, *refs):
    *parts, out_ref = refs
    _, count = kept_tiles(ranks_ref, slots)
    most = parts[0][-PAD:, :].astype(jnp.float32)
    for part in parts[1:]:
        most = jnp.maximum(most, part[-PAD:, :].astype(jnp.float32))
    rows = lax.broadcasted_iota(jnp.int32, (PAD, TILE), 0)
    others = jnp.max(jnp.where(rows == PAD - 1, most, -1.0))
    over = jnp.logical_or(others > places, count > places)
    out_ref[0] = jnp.where(over, 1, 0)


def first_body(where_ref, a_ref, *refs):
    pix, base = where_ref[0], where_ref[1]
    n_base = a_ref.shape[1] // TILE
    shares, rest = refs[:n_base], refs[n_base:]
    outs, x_ref = rest[:-1], rest[-1]
    quarter = outs[0].shape[1]
    for d, share in enumerate(shares):
        x_ref[:, pl.ds(pl.multiple_of((base ^ d) * TILE, TILE), TILE)] = share[...]
    for d, out in enumerate(outs):
        rows = pl.ds(pl.multiple_of((pix ^ d) * quarter, quarter), quarter)
        piece = lax.dot_general(
            x_ref[...], a_ref[rows, :], (((1,), (1,)), ((), ())), preferred_element_type=jnp.float32
        )
        out[...] = piece.astype(out.dtype)


def in_order(values, index):
    bit = 1
    while bit < len(values):
        odd = (index & bit) != 0
        values = [jnp.where(odd, values[d ^ bit], values[d]) for d in range(len(values))]
        bit *= 2
    return values


def pairs(slots):
    return [(r, s) for r in range(slots) for s in range(r + 1, slots)] + [(r, r + 1) for r in range(0, slots, 2)]


def pack_rows(slots, n_base):
    return len(pairs(slots)) * TILE // n_base


def corner():
    rows = lax.broadcasted_iota(jnp.int32, (TILE, TILE), 0)
    cols = lax.broadcasted_iota(jnp.int32, (TILE, TILE), 1)
    return rows, cols


def gram_body(slots, n_parts, where_ref, ranks_ref, y_ref, a_ref, *refs):
    pix, base = where_ref[0], where_ref[1]
    parts = refs[:n_parts]
    cols_ref, *outs, all_ref = refs[n_parts:]
    n_base = len(outs)
    chans, quarter = y_ref.shape[0], cols_ref.shape[0]
    table, _ = kept_tiles(ranks_ref, slots)
    own_rows = pl.ds(pl.multiple_of(pix * quarter, quarter), quarter)
    columns = []
    for r in range(slots):
        tile, owned = jnp.int32(0), jnp.int32(0)
        for j, (rank, _, _) in enumerate(table):
            tile = jnp.where(rank == r, j, tile)
            owned = jnp.where(rank == r, 1, owned)
        block = a_ref[own_rows, pl.ds(pl.multiple_of(tile * TILE, TILE), TILE)]
        block = jnp.where(owned == 1, block, jnp.zeros_like(block))
        for part in parts:
            places = (part.shape[0] - PAD) // quarter
            notes = part[places * quarter :, :].astype(jnp.float32)
            for i in range(places):
                hit = jnp.broadcast_to(notes[i : i + 1] == r, block.shape)
                block = jnp.where(hit, part[i * quarter : (i + 1) * quarter, :], block)
        columns.append(block)
    a = jnp.concatenate(columns, axis=1)
    cols_ref[...] = a
    y = y_ref[:, pl.ds(pl.multiple_of(pix * quarter, quarter), quarter)]
    both = jnp.dot(jnp.concatenate(split(y), axis=0), a, preferred_element_type=jnp.float32)
    data = both[:chans] + both[chans:]
    gram = lax.dot_general(a, a, (((0,), (0,)), ((), ())), preferred_element_type=jnp.float32)
    rows, cols = corner()
    g_rows = pack_rows(slots, n_base)
    per = slots // n_base
    half = min(TILE, g_rows & -g_rows)

    def block_of(r, s):
        return gram[r * TILE : (r + 1) * TILE, s * TILE : (s + 1) * TILE]

    n_off = slots * (slots - 1) // 2
    for i, (r, s) in enumerate(pairs(slots)):
        block = block_of(r, s) if i < n_off else jnp.where(rows < cols, block_of(r, r), block_of(s, s))
        block = block.astype(jnp.bfloat16)
        for q in range(TILE // half):
            at = i * TILE + q * half
            all_ref[at // g_rows, at % g_rows : at % g_rows + half, :] = block[q * half : (q + 1) * half]
    for r in range(slots):
        diag = jnp.sum(jnp.where(rows == cols, block_of(r, r), 0.0), axis=0, keepdims=True)
        at = g_rows + (r % per) * (2 * chans + PAD)
        wide = jnp.concatenate(split(data[:, r * TILE : (r + 1) * TILE]), axis=0)
        all_ref[r // per, at : at + 2 * chans, :] = wide
        all_ref[r // per, at + 2 * chans : at + 2 * chans + PAD, :] = tail_of(diag)
    for d, out in enumerate(outs):
        out[...] = all_ref[base ^ d]


def tail_of(row):
    return jnp.concatenate([*split(row), jnp.zeros((PAD - 2, TILE), jnp.bfloat16)], axis=0)


def start_body(slots, n_pix, where_ref, ranks_ref, y_ref, x0_ref, cols_ref, *refs):
    pix, base = where_ref[0], where_ref[1]
    preds = refs[:n_pix]
    *outs, all_ref = refs[n_pix:]
    per = slots // len(outs)
    chans, quarter = preds[0].shape
    pred = preds[0][...].astype(jnp.float32)
    for piece in preds[1:]:
        pred = pred + piece[...].astype(jnp.float32)
    y = y_ref[:, pl.ds(pl.multiple_of(pix * quarter, quarter), quarter)]
    resid = (y - pred).astype(jnp.bfloat16)
    moved = descent_stride * jnp.dot(resid, cols_ref[...], preferred_element_type=jnp.float32)
    rank = ranks_ref[base, 0]
    for r in range(slots):
        start = moved[:, r * TILE : (r + 1) * TILE] + jnp.where(rank == r, x0_ref[...], 0.0)
        at = (r % per) * 2 * chans
        all_ref[r // per, at : at + 2 * chans, :] = jnp.concatenate(split(start), axis=0)
    for d, out in enumerate(outs):
        out[...] = all_ref[base ^ d]


def sections(g_rows, chans, per):
    first = [(g_rows, 0)] + [(2 * chans, chans), (PAD, 1)] * per
    return first, [(2 * chans, chans)] * per


def sum_body(layouts, *refs):
    *parts, out = refs
    groups = [parts[i :: len(layouts)] for i in range(len(layouts))]
    to = 0
    for group, layout in zip(groups, layouts):
        at = 0
        for size, pair in layout:
            value = group[0][at : at + size].astype(jnp.float32)
            for part in group[1:]:
                value = value + part[at : at + size].astype(jnp.float32)
            if pair == 0:
                out[to : to + size] = value.astype(jnp.bfloat16)
            elif pair == 1:
                out[to : to + size] = tail_of(value[0:1] + value[1:2])
            else:
                out[to : to + size] = jnp.concatenate(split(value[:pair] + value[pair:]), axis=0)
            at += size
            to += size


def iterate_body(slots, n_base, g_rows, chans, where_ref, ranks_ref, *refs):
    base = where_ref[1]
    per = slots // n_base
    data_rows = 2 * chans + PAD
    image_at = g_rows + per * data_rows
    chunks = [refs[:n_base], refs[n_base : 2 * n_base]]
    out_ref, gram_ref, last_ref = refs[2 * n_base :]
    states, datas, diags = [], [], []
    rows, cols = corner()
    n_off = slots * (slots - 1) // 2

    def put(g, r, s, block):
        gram_ref[g, r * TILE : (r + 1) * TILE, s * TILE : (s + 1) * TILE] = block

    for g in range(2):
        full = in_order([ref[...] for ref in chunks[g]], base)
        half = min(TILE, g_rows & -g_rows)
        for i, (r, s) in enumerate(pairs(slots)):
            pieces = []
            for q in range(TILE // half):
                at = i * TILE + q * half
                pieces.append(full[at // g_rows][at % g_rows : at % g_rows + half])
            block = jnp.concatenate(pieces, axis=0)
            if i < n_off:
                put(g, r, s, block)
                put(g, s, r, block.T)
            else:
                upper = jnp.where(rows < cols, block, jnp.zeros_like(block))
                lower = jnp.where(rows > cols, block, jnp.zeros_like(block))
                put(g, r, r, upper + upper.T)
                put(g, s, s, lower + lower.T)
        sides = [full[r // per][g_rows + (r % per) * data_rows :][:data_rows].astype(jnp.float32) for r in range(slots)]
        images = [full[r // per][image_at + (r % per) * 2 * chans :][: 2 * chans].astype(jnp.float32) for r in range(slots)]
        datas.append(jnp.concatenate([v[:chans] + v[chans : 2 * chans] for v in sides], axis=1))
        states.append(jnp.concatenate([v[:chans] + v[chans:] for v in images], axis=1))
        tails = [v[2 * chans :] for v in sides]
        diags.append(jnp.concatenate([t[0:1] + t[1:2] for t in tails], axis=1))
    for step in range(ITERS):
        factors = []
        for r in range(slots):
            lanes = slice(r * TILE, (r + 1) * TILE)
            square = states[0][:, lanes] * states[0][:, lanes] + states[1][:, lanes] * states[1][:, lanes]
            column = jnp.sum(square, axis=0, keepdims=True)
            norm = jnp.sum(column, axis=1, keepdims=True)
            rms = jnp.sqrt(norm / (CH * TILE) + eps_norm)
            factors.append(jnp.broadcast_to(rms / (rms + lam_shrink), (1, TILE)))
        factor = jnp.concatenate(factors, axis=1)
        states = [state * factor for state in states]
        if step == ITERS - 1:
            break
        for g in range(2):
            high, low = split(states[g])
            both = jnp.dot(
                jnp.concatenate([high, low], axis=0), gram_ref[g], preferred_element_type=jnp.float32
            )
            product = both[:chans] + both[chans:] + states[g] * diags[g]
            states[g] = states[g] + descent_stride * (datas[g] - product)
    for r in range(slots):
        last_ref[r] = states[0][:, r * TILE : (r + 1) * TILE]
    rank = ranks_ref[base, 0]
    kept = last_ref[jnp.minimum(rank, slots - 1)]
    out_ref[...] = jnp.where(rank < slots, kept, 0.0)


def gram_plan(sensing_operator_parts, sampled_correlations, first_sky_estimate, patch_order_record):
    a = sensing_operator_parts[0]
    chans, m_dev = sampled_correlations.shape
    n_base, n_pix = lax.axis_size("base"), lax.axis_size("pix")
    slots = n_base * n_pix // 4
    quarter = m_dev // n_pix
    x0 = first_sky_estimate[:, 0, 0, :]
    ranks = patch_order_record.T
    where = jnp.stack([lax.axis_index("pix"), lax.axis_index("base")]).astype(jnp.int32)
    shape = jax.ShapeDtypeStruct
    bf16, f32 = jnp.bfloat16, jnp.float32

    def exchange(first, places):
        packed = call(
            functools.partial(pack_body, slots, first),
            [shape((places * quarter + PAD, TILE), bf16)] * (n_pix - 1),
            (where, ranks, a),
            smem=(0, 1),
        )
        return [swap(packed[d - 1], "pix", d) for d in range(n_pix - 1, 0, -1)]

    places = min(CAPACITY, ranks.shape[0])
    parts = exchange(0, places)
    x0_round = x0.astype(bf16)
    shares = [x0_round] + [swap(x0_round, "base", d) for d in range(1, n_base)]
    firsts = call(
        first_body,
        [shape((chans, quarter), bf16)] * n_pix,
        (where, a, *shares),
        scratch=[pltpu.VMEM((chans, n_base * TILE), bf16)],
        smem=(0,),
    )
    preds = [firsts[0]] + [swap(firsts[d], "pix", d) for d in range(n_pix - 1, 0, -1)]

    g_rows = pack_rows(slots, n_base)
    per = slots // n_base
    layouts = sections(g_rows, chans, per)
    gram_chunk, image_chunk = [shape((sum(size for size, _ in layout), TILE), bf16) for layout in layouts]
    chunk = shape((gram_chunk.shape[0] + image_chunk.shape[0], TILE), bf16)

    def spread(parts):
        columns, *grams = call(
            functools.partial(gram_body, slots, len(parts)),
            [shape((quarter, slots * TILE), bf16)] + [gram_chunk] * n_base,
            (where, ranks, sampled_correlations, a, *parts),
            scratch=[pltpu.VMEM((n_base, *gram_chunk.shape), bf16)],
            smem=(0, 1),
        )
        grams = [grams[0]] + [swap(grams[d], "base", d) for d in range(1, n_base)]
        images = call(
            functools.partial(start_body, slots, n_pix),
            [image_chunk] * n_base,
            (where, ranks, sampled_correlations, x0, columns, *preds),
            scratch=[pltpu.VMEM((n_base, *image_chunk.shape), bf16)],
            smem=(0, 1),
        )
        images = [images[0]] + [swap(images[d], "base", d) for d in range(1, n_base)]
        return [piece for pair in zip(grams, images) for piece in pair]

    def add(layouts, pieces):
        return call(functools.partial(sum_body, layouts), chunk, pieces)

    crowded = call(
        functools.partial(crowd_body, slots, places),
        shape((1,), jnp.int32),
        (ranks, *parts),
        smem=(0,),
        out_space=pltpu.SMEM,
    )[0]
    pieces = spread(parts)
    part = lax.cond(
        crowded != 0,
        lambda: add(layouts, spread(parts + exchange(places, ranks.shape[0] - places))),
        lambda: add(layouts, pieces),
    )
    total = add([layouts[0] + layouts[1]], [part] + [swap(part, "pix", d) for d in range(n_pix - 1, 0, -1)])

    axes = ("freq", "base")
    got = {0: total}
    for offset in range(2, 2 * n_base, 2):
        got[offset] = swap(total, axes, offset)
    got[1] = swap(total, axes, 1)
    for offset in range(2, 2 * n_base, 2):
        got[offset + 1] = swap(got[offset], axes, 1)
    image = call(
        functools.partial(iterate_body, slots, n_base, g_rows, chans),
        shape((chans, TILE), f32),
        (where, ranks, *[got[i] for i in range(2 * n_base)]),
        scratch=[
            pltpu.VMEM((2, slots * TILE, slots * TILE), bf16),
            pltpu.VMEM((slots, chans, TILE), f32),
        ],
        smem=(0, 1),
    )
    return image.reshape(chans, 1, 1, TILE)


def on_device(sensing_operator_parts, sampled_correlations, first_sky_estimate, patch_order_record):
    n_base, n_pix = lax.axis_size("base"), lax.axis_size("pix")
    slots = n_base * n_pix // 4
    chans, m_dev = sampled_correlations.shape
    fits = (
        first_sky_estimate.shape[3] == TILE
        and (slots * TILE) ** 2 <= GRAM_LIMIT
        and n_base & (n_base - 1) == 0
        and n_pix & (n_pix - 1) == 0
        and slots % n_base == 0
        and slots % 2 == 0
        and len(pairs(slots)) * TILE % (n_base * 16) == 0
        and m_dev % (n_pix * TILE) == 0
        and lax.axis_size("freq") == 2
        and chans % 16 == 0
    )
    plan = gram_plan if fits else streaming
    return plan(sensing_operator_parts, sampled_correlations, first_sky_estimate, patch_order_record)


def solution(mesh):
    in_specs = (
        P("freq", "base", "pix"),
        P("freq", "base"),
        P("freq", "pix", "base", None),
        P(None, "pix"),
    )
    out_specs = P("freq", "pix", "base", None)
    return jax.shard_map(
        on_device, mesh=mesh, in_specs=in_specs, out_specs=out_specs, check_vma=False
    )
```

```python
import functools

import jax
import jax.numpy as jnp
from jax import lax
from jax.experimental import pallas as pl
from jax.experimental.pallas import tpu as pltpu
from jax.sharding import PartitionSpec as P

CH = 64
TILE = 128
ITERS = 6


descent_stride = 0.6
lam_shrink = 0.3
eps_norm = 1e-06


GRAM_LIMIT = 1 << 20
PAD = 16
CAPACITY = 2
VMEM_LIMIT = 12 << 20


def project_rows(rounded_amount, columns):
    return lax.dot_general(
        rounded_amount, columns, (((1,), (1,)), ((), ())), preferred_element_type=jnp.float32
    )


def residual_of(sampled_correlations, partial_value):
    shares = lax.psum_scatter(partial_value, "pix", scatter_dimension=1, tiled=True)
    width = shares.shape[1]
    own_rows = lax.dynamic_slice_in_dim(
        sampled_correlations, lax.axis_index("pix") * width, width, 1
    )
    return lax.all_gather((own_rows - shares).astype(jnp.bfloat16), "pix", axis=1, tiled=True)


def streaming(sensing_operator_parts, sampled_correlations, first_sky_estimate, patch_order_record):
    sensing_operator = sensing_operator_parts[0]
    chans, _ = sampled_correlations.shape
    share_width = first_sky_estimate.shape[3]
    tiles_share = share_width // TILE
    keep_count = tiles_share * lax.axis_size("base") * lax.axis_size("pix") // 4
    base_index = lax.axis_index("base")
    own_share = first_sky_estimate[:, 0, 0, :]
    current = own_share
    for step in range(ITERS):
        rounded_amount = current.astype(jnp.bfloat16)
        partial_value = project_rows(
            lax.all_gather(rounded_amount, "base", axis=1, tiled=True), sensing_operator
        )
        resid = residual_of(sampled_correlations, partial_value)
        gradient_portion = jnp.dot(resid, sensing_operator, preferred_element_type=jnp.float32)
        grad_share = lax.psum_scatter(gradient_portion, "base", scatter_dimension=1, tiled=True)
        moved = current + descent_stride * grad_share
        tiles = moved.reshape(chans, tiles_share, TILE)
        local_sum = jnp.sum(tiles * tiles, axis=(0, 2))
        total = lax.psum(local_sum, "freq")
        ranks = lax.dynamic_slice_in_dim(
            patch_order_record[step], base_index * tiles_share, tiles_share, 0
        )
        rms_tile = jnp.sqrt(total / (CH * TILE) + eps_norm)
        keeping = (ranks < keep_count).astype(jnp.float32)
        factor = keeping * rms_tile / (rms_tile + lam_shrink)
        current = (tiles * factor[None, :, None]).reshape(chans, share_width)
    return current.reshape(chans, 1, 1, share_width)


def swap(value, axis, offset):
    size = lax.axis_size(axis)
    return lax.ppermute(value, axis, [(i, i ^ offset) for i in range(size)])


def routes(size):
    if size == 4:
        return [(1, 3, 0, 2), (3, 2, 1, 0), (2, 0, 3, 1)]
    return [tuple(i ^ d for i in range(size)) for d in range(1, size)]


def send(pieces):
    got = []
    for piece, route in zip(pieces, routes(lax.axis_size("pix"))):
        got.append(lax.ppermute(piece, "pix", list(enumerate(route))))
    return got


def target(pix, k, size):
    if k == 0:
        return pix
    place = jnp.int32(0)
    for i, to in enumerate(routes(size)[k - 1]):
        place = jnp.where(pix == i, to, place)
    return place


def call(body, out_shape, args, scratch=(), smem=(), scalars=()):
    places = [pltpu.SMEM if i in smem else pltpu.VMEM for i in range(len(args))]
    specs = [pl.BlockSpec(memory_space=place) for place in places]
    place = lambda i: pltpu.SMEM if i in scalars else pltpu.VMEM
    if isinstance(out_shape, list):
        out_specs = [pl.BlockSpec(memory_space=place(i)) for i in range(len(out_shape))]
    else:
        out_specs = pl.BlockSpec(memory_space=place(0))
    return pl.pallas_call(
        body,
        out_shape=out_shape,
        in_specs=specs,
        out_specs=out_specs,
        scratch_shapes=list(scratch),
        compiler_params=pltpu.CompilerParams(vmem_limit_bytes=VMEM_LIMIT),
    )(*args)


def split(value):
    high = value.astype(jnp.bfloat16)
    return high, (value - high.astype(jnp.float32)).astype(jnp.bfloat16)


def kept_tiles(ranks_ref, slots):
    count = jnp.int32(0)
    table = []
    for j in range(ranks_ref.shape[0]):
        rank = ranks_ref[j, 0]
        kept = rank < slots
        table.append((rank, kept, count))
        count = count + jnp.where(kept, 1, 0)
    return table, count


def pack_body(slots, first, where_ref, ranks_ref, a_ref, *outs):
    pix = where_ref[0]
    quarter = a_ref.shape[0] // (len(outs) + 1)
    places = (outs[0].shape[0] - PAD) // quarter
    table, count = kept_tiles(ranks_ref, slots)
    rows = lax.broadcasted_iota(jnp.int32, (PAD, TILE), 0)
    notes = jnp.where(rows == PAD - 1, count, -1)
    for i in range(places):
        tile, slot = jnp.int32(0), jnp.int32(-1)
        for j, (rank, kept, before) in enumerate(table):
            hit = jnp.logical_and(kept, before == first + i)
            tile = jnp.where(hit, j, tile)
            slot = jnp.where(hit, rank, slot)
        notes = jnp.where(rows == i, slot, notes)
        lanes = pl.ds(pl.multiple_of(tile * TILE, TILE), TILE)
        for d, out in enumerate(outs):
            at = pl.ds(pl.multiple_of(target(pix, d + 1, len(outs) + 1) * quarter, quarter), quarter)
            out[i * quarter : (i + 1) * quarter, :] = a_ref[at, lanes]
    for out in outs:
        out[places * quarter :, :] = notes.astype(jnp.float32).astype(jnp.bfloat16)


def crowd_body(slots, places, ranks_ref, *refs):
    *parts, out_ref = refs
    _, count = kept_tiles(ranks_ref, slots)
    most = parts[0][-PAD:, :].astype(jnp.float32)
    for part in parts[1:]:
        most = jnp.maximum(most, part[-PAD:, :].astype(jnp.float32))
    rows = lax.broadcasted_iota(jnp.int32, (PAD, TILE), 0)
    others = jnp.max(jnp.where(rows == PAD - 1, most, -1.0))
    over = jnp.logical_or(others > places, count > places)
    out_ref[0] = jnp.where(over, 1, 0)


def first_body(where_ref, a_ref, *refs):
    pix, base = where_ref[0], where_ref[1]
    n_base = a_ref.shape[1] // TILE
    shares, rest = refs[:n_base], refs[n_base:]
    outs, x_ref = rest[:-1], rest[-1]
    quarter = outs[0].shape[1]
    for d, share in enumerate(shares):
        x_ref[:, pl.ds(pl.multiple_of((base ^ d) * TILE, TILE), TILE)] = share[...]
    for d, out in enumerate(outs):
        rows = pl.ds(pl.multiple_of(target(pix, d, len(outs)) * quarter, quarter), quarter)
        piece = lax.dot_general(
            x_ref[...], a_ref[rows, :], (((1,), (1,)), ((), ())), preferred_element_type=jnp.float32
        )
        out[...] = piece.astype(out.dtype)


def in_order(values, index):
    bit = 1
    while bit < len(values):
        odd = (index & bit) != 0
        values = [jnp.where(odd, values[d ^ bit], values[d]) for d in range(len(values))]
        bit *= 2
    return values


def pairs(slots):
    return [(r, s) for r in range(slots) for s in range(r + 1, slots)] + [(r, r + 1) for r in range(0, slots, 2)]


def pack_rows(slots, n_base):
    return len(pairs(slots)) * TILE // n_base


def corner():
    rows = lax.broadcasted_iota(jnp.int32, (TILE, TILE), 0)
    cols = lax.broadcasted_iota(jnp.int32, (TILE, TILE), 1)
    return rows, cols


def gram_body(slots, n_parts, where_ref, ranks_ref, y_ref, a_ref, *refs):
    pix, base = where_ref[0], where_ref[1]
    parts = refs[:n_parts]
    cols_ref, own_ref, sent_ref, all_ref = refs[n_parts:]
    n_base = all_ref.shape[0]
    chans, quarter = y_ref.shape[0], cols_ref.shape[0]
    table, _ = kept_tiles(ranks_ref, slots)
    own_rows = pl.ds(pl.multiple_of(pix * quarter, quarter), quarter)
    columns = []
    for r in range(slots):
        tile, owned = jnp.int32(0), jnp.int32(0)
        for j, (rank, _, _) in enumerate(table):
            tile = jnp.where(rank == r, j, tile)
            owned = jnp.where(rank == r, 1, owned)
        block = a_ref[own_rows, pl.ds(pl.multiple_of(tile * TILE, TILE), TILE)]
        block = jnp.where(owned == 1, block, jnp.zeros_like(block))
        for part in parts:
            places = (part.shape[0] - PAD) // quarter
            notes = part[places * quarter :, :].astype(jnp.float32)
            for i in range(places):
                hit = jnp.broadcast_to(notes[i : i + 1] == r, block.shape)
                block = jnp.where(hit, part[i * quarter : (i + 1) * quarter, :], block)
        columns.append(block)
    a = jnp.concatenate(columns, axis=1)
    cols_ref[...] = a
    y = y_ref[:, pl.ds(pl.multiple_of(pix * quarter, quarter), quarter)]
    both = jnp.dot(jnp.concatenate(split(y), axis=0), a, preferred_element_type=jnp.float32)
    data = both[:chans] + both[chans:]
    gram = lax.dot_general(a, a, (((0,), (0,)), ((), ())), preferred_element_type=jnp.float32)
    rows, cols = corner()
    g_rows = pack_rows(slots, n_base)
    per = slots // n_base
    half = min(TILE, g_rows & -g_rows)

    def block_of(r, s):
        return gram[r * TILE : (r + 1) * TILE, s * TILE : (s + 1) * TILE]

    n_off = slots * (slots - 1) // 2
    for i, (r, s) in enumerate(pairs(slots)):
        block = block_of(r, s) if i < n_off else jnp.where(rows < cols, block_of(r, r), block_of(s, s))
        block = block.astype(jnp.bfloat16)
        for q in range(TILE // half):
            at = i * TILE + q * half
            all_ref[at // g_rows, at % g_rows : at % g_rows + half, :] = block[q * half : (q + 1) * half]
    for r in range(slots):
        diag = jnp.sum(jnp.where(rows == cols, block_of(r, r), 0.0), axis=0, keepdims=True)
        at = g_rows + (r % per) * (2 * chans + PAD)
        wide = jnp.concatenate(split(data[:, r * TILE : (r + 1) * TILE]), axis=0)
        all_ref[r // per, at : at + 2 * chans, :] = wide
        all_ref[r // per, at + 2 * chans : at + 2 * chans + PAD, :] = tail_of(diag)
    by_core(base, all_ref, own_ref, sent_ref)


def by_core(base, all_ref, own_ref, sent_ref):
    size = all_ref.shape[1]
    for k in range(all_ref.shape[0] // 2):
        own_ref[k * size : (k + 1) * size, :] = all_ref[base ^ (2 * k)]
        sent_ref[k * size : (k + 1) * size, :] = all_ref[base ^ (2 * k + 1)]


def tail_of(row):
    return jnp.concatenate([*split(row), jnp.zeros((PAD - 2, TILE), jnp.bfloat16)], axis=0)


def start_body(slots, n_pix, where_ref, ranks_ref, y_ref, x0_ref, cols_ref, *refs):
    pix, base = where_ref[0], where_ref[1]
    preds = refs[:n_pix]
    own_ref, sent_ref, all_ref = refs[n_pix:]
    per = slots // all_ref.shape[0]
    chans, quarter = preds[0].shape
    pred = preds[0][...].astype(jnp.float32)
    for piece in preds[1:]:
        pred = pred + piece[...].astype(jnp.float32)
    y = y_ref[:, pl.ds(pl.multiple_of(pix * quarter, quarter), quarter)]
    resid = (y - pred).astype(jnp.bfloat16)
    moved = descent_stride * jnp.dot(resid, cols_ref[...], preferred_element_type=jnp.float32)
    rank = ranks_ref[base, 0]
    for r in range(slots):
        start = moved[:, r * TILE : (r + 1) * TILE] + jnp.where(rank == r, x0_ref[...], 0.0)
        at = (r % per) * 2 * chans
        all_ref[r // per, at : at + 2 * chans, :] = jnp.concatenate(split(start), axis=0)
    by_core(base, all_ref, own_ref, sent_ref)


def summed(parts, at, size, pair):
    value = parts[0][at : at + size].astype(jnp.float32)
    for part in parts[1:]:
        value = value + part[at : at + size].astype(jnp.float32)
    if pair == 0:
        return value.astype(jnp.bfloat16)
    if pair == 1:
        return tail_of(value[0:1] + value[1:2])
    return jnp.concatenate(split(value[:pair] + value[pair:]), axis=0)


def core_body(layout, own_ref, got_ref, *outs):
    at = 0
    for out in outs:
        to = 0
        for size, pair in layout:
            out[to : to + size] = summed([own_ref, got_ref], at, size, pair)
            at += size
            to += size


def join_body(layouts, *refs):
    *parts, out = refs
    to = 0
    for i, layout in enumerate(layouts):
        at = 0
        for size, pair in layout:
            out[to : to + size] = summed(parts[i :: len(layouts)], at, size, pair)
            at += size
            to += size


def total_body(layout, *refs):
    *parts, out, short = refs
    at = to = 0
    for size, pair in layout:
        value = summed(parts, at, size, pair)
        out[at : at + size] = value
        kept = pair if pair > 1 else size
        short[to : to + kept] = value[:kept]
        at += size
        to += kept


def iterate_body(slots, n_base, where_ref, ranks_ref, *refs):
    base = where_ref[1]
    *chunks, out_ref, gram_ref, last_ref = refs
    chans = out_ref.shape[0]
    rows, cols = corner()
    n_off = slots * (slots - 1) // 2
    g_rows = pack_rows(slots, n_base)
    half = min(TILE, g_rows & -g_rows)
    states, datas, diags = [], [], []

    def put(g, r, s, block):
        gram_ref[g, r * TILE : (r + 1) * TILE, s * TILE : (s + 1) * TILE] = block

    for g in range(2):
        full = in_order([ref[...] for ref in chunks[g * n_base : (g + 1) * n_base]], base)
        for i, (r, s) in enumerate(pairs(slots)):
            pieces = []
            for q in range(TILE // half):
                at = i * TILE + q * half
                pieces.append(full[at // g_rows][at % g_rows : at % g_rows + half])
            block = jnp.concatenate(pieces, axis=0)
            if i < n_off:
                put(g, r, s, block)
                put(g, s, r, block.T)
            else:
                upper = jnp.where(rows < cols, block, jnp.zeros_like(block))
                lower = jnp.where(rows > cols, block, jnp.zeros_like(block))
                put(g, r, r, upper + upper.T)
                put(g, s, s, lower + lower.T)
        per = slots // n_base
        wide = (full[0].shape[0] - g_rows - per * PAD) // (2 * per)

        def gather(at, pitch):
            values = []
            for r in range(slots):
                v = full[r // per][at + (r % per) * pitch :][:wide].astype(jnp.float32)
                values.append(v[:chans] + v[chans:] if wide > chans else v)
            return jnp.concatenate(values, axis=1)

        datas.append(gather(g_rows, wide + PAD))
        states.append(gather(g_rows + per * (wide + PAD), wide))
        tails = []
        for r in range(slots):
            v = full[r // per][g_rows + (r % per) * (wide + PAD) + wide :][:PAD].astype(jnp.float32)
            tails.append(v[0:1] + v[1:2])
        diags.append(jnp.concatenate(tails, axis=1))
    for step in range(ITERS):
        factors = []
        for r in range(slots):
            lanes = slice(r * TILE, (r + 1) * TILE)
            square = states[0][:, lanes] * states[0][:, lanes] + states[1][:, lanes] * states[1][:, lanes]
            column = jnp.sum(square, axis=0, keepdims=True)
            norm = jnp.sum(column, axis=1, keepdims=True)
            rms = jnp.sqrt(norm / (CH * TILE) + eps_norm)
            factors.append(jnp.broadcast_to(rms / (rms + lam_shrink), (1, TILE)))
        factor = jnp.concatenate(factors, axis=1)
        states = [state * factor for state in states]
        if step == ITERS - 1:
            break
        for g in range(2):
            high, low = split(states[g])
            left = jnp.concatenate([high, low], axis=0) if g == 0 else high
            product = jnp.dot(left, gram_ref[g], preferred_element_type=jnp.float32)
            if g == 0:
                product = product[:chans] + product[chans:]
            product = product + states[g] * diags[g]
            states[g] = states[g] + descent_stride * (datas[g] - product)
    for r in range(slots):
        last_ref[r] = states[0][:, r * TILE : (r + 1) * TILE]
    rank = ranks_ref[base, 0]
    kept = last_ref[jnp.minimum(rank, slots - 1)]
    out_ref[...] = jnp.where(rank < slots, kept, 0.0)


def gram_plan(sensing_operator_parts, sampled_correlations, first_sky_estimate, patch_order_record):
    a = sensing_operator_parts[0]
    chans, m_dev = sampled_correlations.shape
    n_base, n_pix = lax.axis_size("base"), lax.axis_size("pix")
    slots = n_base * n_pix // 4
    quarter = m_dev // n_pix
    x0 = first_sky_estimate[:, 0, 0, :]
    ranks = patch_order_record.T
    where = jnp.stack([lax.axis_index("pix"), lax.axis_index("base")]).astype(jnp.int32)
    shape = jax.ShapeDtypeStruct
    bf16, f32 = jnp.bfloat16, jnp.float32

    def exchange(first, places):
        packed = call(
            functools.partial(pack_body, slots, first),
            [shape((places * quarter + PAD, TILE), bf16)] * (n_pix - 1),
            (where, ranks, a),
            smem=(0, 1),
        )
        return send(packed)

    places = min(CAPACITY, ranks.shape[0])
    parts = exchange(0, places)
    x0_round = x0.astype(bf16)
    shares = [x0_round] + [swap(x0_round, "base", d) for d in range(1, n_base)]
    firsts = call(
        first_body,
        [shape((chans, quarter), bf16)] * n_pix,
        (where, a, *shares),
        scratch=[pltpu.VMEM((chans, n_base * TILE), bf16)],
        smem=(0,),
    )
    preds = [firsts[0]] + send(firsts[1:])

    per = slots // n_base
    gram_layout = [(pack_rows(slots, n_base), 0)] + [(2 * chans, chans), (PAD, 1)] * per
    side_layout = [(2 * chans, chans)] * per
    layouts = [gram_layout, side_layout]
    heights = [sum(size for size, _ in layout) for layout in layouts]
    chunk = shape((sum(heights), TILE), bf16)
    short = shape((chunk.shape[0] - 2 * chans * per, TILE), bf16)

    def halves(height):
        return [shape((n_base // 2 * height, TILE), bf16)] * 2

    def base_sum(parts):
        columns, *gram = call(
            functools.partial(gram_body, slots, len(parts)),
            [shape((quarter, slots * TILE), bf16)] + halves(heights[0]),
            (where, ranks, sampled_correlations, a, *parts),
            scratch=[pltpu.VMEM((n_base, heights[0], TILE), bf16)],
            smem=(0, 1),
        )
        side = call(
            functools.partial(start_body, slots, n_pix),
            halves(heights[1]),
            (where, ranks, sampled_correlations, x0, columns, *preds),
            scratch=[pltpu.VMEM((n_base, heights[1], TILE), bf16)],
            smem=(0, 1),
        )
        pieces = []
        for (own, sent), layout in zip((gram, side), layouts):
            height = sum(size for size, _ in layout)
            sums = call(
                functools.partial(core_body, layout),
                [shape((height, TILE), bf16)] * (n_base // 2),
                (own, swap(sent, "base", 1)),
            )
            far = [swap(sums[k], "base", 2 * k) for k in range(1, n_base // 2)]
            pieces.append([sums[0], *far])
        return [piece for pair in zip(*pieces) for piece in pair]

    def join(pieces):
        return call(functools.partial(join_body, layouts), chunk, pieces)

    crowded = call(
        functools.partial(crowd_body, slots, places), shape((1,), jnp.int32), (ranks, *parts), smem=(0,), scalars=(0,)
    )[0]
    pieces = base_sum(parts)
    part = lax.cond(
        crowded != 0, lambda: join(base_sum(parts + exchange(places, ranks.shape[0] - places))), lambda: join(pieces)
    )
    total, brief = call(
        functools.partial(total_body, gram_layout + side_layout), [chunk, short], [part] + send([part] * (n_pix - 1))
    )

    axes = ("freq", "base")
    got = {0: total, n_base: swap(brief, axes, n_base)}
    for offset in range(2, n_base, 2):
        got[n_base + offset] = swap(brief, axes, n_base + offset)
        got[offset] = swap(total, axes, offset)
    got[1] = swap(total, axes, 1)
    for offset in range(2, 2 * n_base, 2):
        got[offset + 1] = swap(got[offset], axes, 1)
    image = call(
        functools.partial(iterate_body, slots, n_base),
        shape((chans, TILE), f32),
        (where, ranks, *[got[i] for i in range(2 * n_base)]),
        scratch=[
            pltpu.VMEM((2, slots * TILE, slots * TILE), bf16),
            pltpu.VMEM((slots, chans, TILE), f32),
        ],
        smem=(0, 1),
    )
    return image.reshape(chans, 1, 1, TILE)


def on_device(sensing_operator_parts, sampled_correlations, first_sky_estimate, patch_order_record):
    n_base, n_pix = lax.axis_size("base"), lax.axis_size("pix")
    slots = n_base * n_pix // 4
    chans, m_dev = sampled_correlations.shape
    fits = (
        first_sky_estimate.shape[3] == TILE
        and (slots * TILE) ** 2 <= GRAM_LIMIT
        and n_base & (n_base - 1) == 0
        and n_pix & (n_pix - 1) == 0
        and slots % n_base == 0
        and slots % 2 == 0
        and len(pairs(slots)) * TILE % (n_base * 16) == 0
        and m_dev % (n_pix * TILE) == 0
        and lax.axis_size("freq") == 2
        and chans % 16 == 0
    )
    plan = gram_plan if fits else streaming
    return plan(sensing_operator_parts, sampled_correlations, first_sky_estimate, patch_order_record)


def solution(mesh):
    in_specs = (
        P("freq", "base", "pix"),
        P("freq", "base"),
        P("freq", "pix", "base", None),
        P(None, "pix"),
    )
    out_specs = P("freq", "pix", "base", None)
    return jax.shard_map(
        on_device, mesh=mesh, in_specs=in_specs, out_specs=out_specs, check_vma=False
    )
```

```python
import functools

import jax
import jax.numpy as jnp
from jax import lax
from jax.experimental import pallas as pl
from jax.experimental.pallas import tpu as pltpu
from jax.sharding import PartitionSpec as P

CH = 64
TILE = 128
ITERS = 6


descent_stride = 0.6
lam_shrink = 0.3
eps_norm = 1e-06


GRAM_LIMIT = 1 << 20
PAD = 16
CAPACITY = 2
VMEM_LIMIT = 12 << 20


def project_rows(rounded_amount, columns):
    return lax.dot_general(
        rounded_amount, columns, (((1,), (1,)), ((), ())), preferred_element_type=jnp.float32
    )


def residual_of(sampled_correlations, partial_value):
    shares = lax.psum_scatter(partial_value, "pix", scatter_dimension=1, tiled=True)
    width = shares.shape[1]
    own_rows = lax.dynamic_slice_in_dim(
        sampled_correlations, lax.axis_index("pix") * width, width, 1
    )
    return lax.all_gather((own_rows - shares).astype(jnp.bfloat16), "pix", axis=1, tiled=True)


def streaming(sensing_operator_parts, sampled_correlations, first_sky_estimate, patch_order_record):
    sensing_operator = sensing_operator_parts[0]
    chans, _ = sampled_correlations.shape
    share_width = first_sky_estimate.shape[3]
    tiles_share = share_width // TILE
    keep_count = tiles_share * lax.axis_size("base") * lax.axis_size("pix") // 4
    base_index = lax.axis_index("base")
    own_share = first_sky_estimate[:, 0, 0, :]
    current = own_share
    for step in range(ITERS):
        rounded_amount = current.astype(jnp.bfloat16)
        partial_value = project_rows(
            lax.all_gather(rounded_amount, "base", axis=1, tiled=True), sensing_operator
        )
        resid = residual_of(sampled_correlations, partial_value)
        gradient_portion = jnp.dot(resid, sensing_operator, preferred_element_type=jnp.float32)
        grad_share = lax.psum_scatter(gradient_portion, "base", scatter_dimension=1, tiled=True)
        moved = current + descent_stride * grad_share
        tiles = moved.reshape(chans, tiles_share, TILE)
        local_sum = jnp.sum(tiles * tiles, axis=(0, 2))
        total = lax.psum(local_sum, "freq")
        ranks = lax.dynamic_slice_in_dim(
            patch_order_record[step], base_index * tiles_share, tiles_share, 0
        )
        rms_tile = jnp.sqrt(total / (CH * TILE) + eps_norm)
        keeping = (ranks < keep_count).astype(jnp.float32)
        factor = keeping * rms_tile / (rms_tile + lam_shrink)
        current = (tiles * factor[None, :, None]).reshape(chans, share_width)
    return current.reshape(chans, 1, 1, share_width)


def swap(value, axis, offset):
    size = lax.axis_size(axis)
    return lax.ppermute(value, axis, [(i, i ^ offset) for i in range(size)])


def routes(size):
    if size == 4:
        return [(1, 3, 0, 2), (3, 2, 1, 0), (2, 0, 3, 1)]
    return [tuple(i ^ d for i in range(size)) for d in range(1, size)]


def send(pieces):
    got = []
    for piece, route in zip(pieces, routes(lax.axis_size("pix"))):
        got.append(lax.ppermute(piece, "pix", list(enumerate(route))))
    return got


def target(pix, k, size):
    if k == 0:
        return pix
    place = jnp.int32(0)
    for i, to in enumerate(routes(size)[k - 1]):
        place = jnp.where(pix == i, to, place)
    return place


def call(body, out_shape, args, scratch=(), smem=(), scalars=()):
    specs = [pl.BlockSpec(memory_space=pltpu.SMEM if i in smem else pltpu.VMEM) for i in range(len(args))]
    place = lambda i: pltpu.SMEM if i in scalars else pltpu.VMEM
    if isinstance(out_shape, list):
        out_specs = [pl.BlockSpec(memory_space=place(i)) for i in range(len(out_shape))]
    else:
        out_specs = pl.BlockSpec(memory_space=place(0))
    return pl.pallas_call(
        body,
        out_shape=out_shape,
        in_specs=specs,
        out_specs=out_specs,
        scratch_shapes=list(scratch),
        compiler_params=pltpu.CompilerParams(vmem_limit_bytes=VMEM_LIMIT),
    )(*args)


def split(value):
    high = value.astype(jnp.bfloat16)
    return high, (value - high.astype(jnp.float32)).astype(jnp.bfloat16)


def pack_body(slots, ranks_ref, a_ref, x0_ref, *outs):
    *outs, notes_ref, round_ref = outs
    round_ref[...] = x0_ref[...].astype(jnp.bfloat16)
    pix, base = lax.axis_index("pix"), lax.axis_index("base")
    tiles = ranks_ref.shape[0]
    quarter = a_ref.shape[0] // (len(outs) + 1)
    places = (outs[0].shape[0] - PAD) // quarter
    rows = lax.broadcasted_iota(jnp.int32, (PAD, TILE), 0)
    count = jnp.int32(0)
    table = []
    notes = jnp.full((PAD, TILE), -1, jnp.int32)
    for j in range(tiles):
        rank = ranks_ref[j, 0]
        slot = jnp.where(rank < slots, rank, -1)
        table.append((slot, count))
        notes = jnp.where(rows == j, slot, notes)
        notes = jnp.where(jnp.logical_and(rows == PAD - 2, base == j), slot, notes)
        count = count + jnp.where(rank < slots, 1, 0)
    notes = jnp.where(rows == PAD - 1, count, notes)
    notes_ref[...] = notes.astype(jnp.float32).astype(jnp.bfloat16)
    sent = jnp.where(rows == PAD - 1, count, -1)
    for i in range(places):
        tile = jnp.int32(0)
        for j, (slot, before) in enumerate(table):
            hit = jnp.logical_and(slot >= 0, before == i)
            tile = jnp.where(hit, j, tile)
            sent = jnp.where(jnp.logical_and(rows == i, hit), slot, sent)
        lanes = pl.ds(pl.multiple_of(tile * TILE, TILE), TILE)
        for d, out in enumerate(outs):
            at = pl.ds(pl.multiple_of(target(pix, d + 1, len(outs) + 1) * quarter, quarter), quarter)
            out[i * quarter : (i + 1) * quarter, :] = a_ref[at, lanes]
    for out in outs:
        out[places * quarter :, :] = sent.astype(jnp.float32).astype(jnp.bfloat16)


def rest_body(first, notes_ref, a_ref, *outs):
    pix = lax.axis_index("pix")
    quarter = a_ref.shape[0] // (len(outs) + 1)
    places = (outs[0].shape[0] - PAD) // quarter
    notes = notes_ref[...].astype(jnp.float32)
    tiles = a_ref.shape[1] // TILE
    rows = lax.broadcasted_iota(jnp.int32, (PAD, TILE), 0)
    before = jnp.zeros((1, TILE), jnp.float32)
    sent = jnp.full((PAD, TILE), -1.0, jnp.float32)
    hits = []
    for j in range(tiles):
        slot = notes[j : j + 1]
        hits.append([jnp.logical_and(slot >= 0, before == first + i) for i in range(places)])
        for i in range(places):
            sent = jnp.where(jnp.logical_and(rows == i, hits[j][i]), slot, sent)
        before = before + jnp.where(slot >= 0, 1.0, 0.0)
    for d, out in enumerate(outs):
        at = pl.ds(pl.multiple_of(target(pix, d + 1, len(outs) + 1) * quarter, quarter), quarter)
        for i in range(places):
            block = a_ref[at, :TILE]
            for j in range(1, tiles):
                tile = a_ref[at, j * TILE : (j + 1) * TILE]
                block = jnp.where(jnp.broadcast_to(hits[j][i], block.shape), tile, block)
            out[i * quarter : (i + 1) * quarter, :] = block
        out[places * quarter :, :] = sent.astype(jnp.bfloat16)


def crowd_body(places, *refs):
    *parts, out_ref = refs
    most = parts[0][-PAD:, :].astype(jnp.float32)
    for part in parts[1:]:
        most = jnp.maximum(most, part[-PAD:, :].astype(jnp.float32))
    rows = lax.broadcasted_iota(jnp.int32, (PAD, TILE), 0)
    most = jnp.max(jnp.where(rows == PAD - 1, most, -1.0))
    out_ref[0] = jnp.where(most > places, 1, 0)


def first_body(a_ref, *refs):
    pix, base = lax.axis_index("pix"), lax.axis_index("base")
    n_base = a_ref.shape[1] // TILE
    shares, rest = refs[:n_base], refs[n_base:]
    outs, x_ref = rest[:-1], rest[-1]
    quarter = outs[0].shape[1]
    for d, share in enumerate(shares):
        x_ref[:, pl.ds(pl.multiple_of((base ^ d) * TILE, TILE), TILE)] = share[...]
    for d, out in enumerate(outs):
        rows = pl.ds(pl.multiple_of(target(pix, d, len(outs)) * quarter, quarter), quarter)
        piece = lax.dot_general(
            x_ref[...], a_ref[rows, :], (((1,), (1,)), ((), ())), preferred_element_type=jnp.float32
        )
        out[...] = piece.astype(out.dtype)


def in_order(values, index):
    bit = 1
    while bit < len(values):
        odd = (index & bit) != 0
        values = [jnp.where(odd, values[d ^ bit], values[d]) for d in range(len(values))]
        bit *= 2
    return values


def pairs(slots):
    return [(r, s) for r in range(slots) for s in range(r + 1, slots)] + [(r, r + 1) for r in range(0, slots, 2)]


def pack_rows(slots, n_base):
    return len(pairs(slots)) * TILE // n_base


def corner():
    rows = lax.broadcasted_iota(jnp.int32, (TILE, TILE), 0)
    cols = lax.broadcasted_iota(jnp.int32, (TILE, TILE), 1)
    return rows, cols


def gram_body(slots, n_parts, y_ref, a_ref, notes_ref, *refs):
    pix, base = lax.axis_index("pix"), lax.axis_index("base")
    parts = refs[:n_parts]
    cols_ref, own_ref, sent_ref, all_ref = refs[n_parts:]
    n_base = all_ref.shape[0]
    chans, quarter = y_ref.shape[0], cols_ref.shape[0]
    own_rows = pl.ds(pl.multiple_of(pix * quarter, quarter), quarter)
    tiles = a_ref.shape[1] // TILE
    blocks = [a_ref[own_rows, j * TILE : (j + 1) * TILE] for j in range(tiles)]
    notes = notes_ref[...].astype(jnp.float32)
    marks = [notes[j : j + 1] for j in range(tiles)]
    for part in parts:
        places = (part.shape[0] - PAD) // quarter
        notes = part[places * quarter :, :].astype(jnp.float32)
        blocks += [part[i * quarter : (i + 1) * quarter, :] for i in range(places)]
        marks += [notes[i : i + 1] for i in range(places)]
    columns = []
    for r in range(slots):
        column = jnp.zeros((quarter, TILE), jnp.bfloat16)
        for block, mark in zip(blocks, marks):
            column = jnp.where(jnp.broadcast_to(mark == r, column.shape), block, column)
        columns.append(column)
    a = jnp.concatenate(columns, axis=1)
    cols_ref[...] = a
    y = y_ref[:, pl.ds(pl.multiple_of(pix * quarter, quarter), quarter)]
    both = jnp.dot(jnp.concatenate(split(y), axis=0), a, preferred_element_type=jnp.float32)
    data = both[:chans] + both[chans:]
    gram = lax.dot_general(a, a, (((0,), (0,)), ((), ())), preferred_element_type=jnp.float32)
    rows, cols = corner()
    g_rows = pack_rows(slots, n_base)
    per = slots // n_base
    half = min(TILE, g_rows & -g_rows)

    def block_of(r, s):
        return gram[r * TILE : (r + 1) * TILE, s * TILE : (s + 1) * TILE]

    n_off = slots * (slots - 1) // 2
    for i, (r, s) in enumerate(pairs(slots)):
        block = block_of(r, s) if i < n_off else jnp.where(rows < cols, block_of(r, r), block_of(s, s))
        block = block.astype(jnp.bfloat16)
        for q in range(TILE // half):
            at = i * TILE + q * half
            all_ref[at // g_rows, at % g_rows : at % g_rows + half, :] = block[q * half : (q + 1) * half]
    for r in range(slots):
        diag = jnp.sum(jnp.where(rows == cols, block_of(r, r), 0.0), axis=0, keepdims=True)
        at = g_rows + (r % per) * (2 * chans + PAD)
        wide = jnp.concatenate(split(data[:, r * TILE : (r + 1) * TILE]), axis=0)
        all_ref[r // per, at : at + 2 * chans, :] = wide
        all_ref[r // per, at + 2 * chans : at + 2 * chans + PAD, :] = tail_of(diag)
    by_core(base, all_ref, own_ref, sent_ref)


def by_core(base, all_ref, own_ref, sent_ref):
    size = all_ref.shape[1]
    for k in range(all_ref.shape[0] // 2):
        own_ref[k * size : (k + 1) * size, :] = all_ref[base ^ (2 * k)]
        sent_ref[k * size : (k + 1) * size, :] = all_ref[base ^ (2 * k + 1)]


def tail_of(row):
    return jnp.concatenate([*split(row), jnp.zeros((PAD - 2, TILE), jnp.bfloat16)], axis=0)


def start_body(slots, n_pix, y_ref, x0_ref, notes_ref, cols_ref, *refs):
    pix, base = lax.axis_index("pix"), lax.axis_index("base")
    preds = refs[:n_pix]
    own_ref, sent_ref, all_ref = refs[n_pix:]
    per = slots // all_ref.shape[0]
    chans, quarter = preds[0].shape
    pred = preds[0][...].astype(jnp.float32)
    for piece in preds[1:]:
        pred = pred + piece[...].astype(jnp.float32)
    y = y_ref[:, pl.ds(pl.multiple_of(pix * quarter, quarter), quarter)]
    resid = (y - pred).astype(jnp.bfloat16)
    moved = descent_stride * jnp.dot(resid, cols_ref[...], preferred_element_type=jnp.float32)
    mark = notes_ref[PAD - 2 : PAD - 1, :].astype(jnp.float32)
    for r in range(slots):
        start = moved[:, r * TILE : (r + 1) * TILE] + jnp.where(mark == r, x0_ref[...], 0.0)
        at = (r % per) * 2 * chans
        all_ref[r // per, at : at + 2 * chans, :] = jnp.concatenate(split(start), axis=0)
    by_core(base, all_ref, own_ref, sent_ref)


def summed(parts, at, size, pair):
    value = parts[0][at : at + size].astype(jnp.float32)
    for part in parts[1:]:
        value = value + part[at : at + size].astype(jnp.float32)
    if pair == 0:
        return value.astype(jnp.bfloat16)
    if pair == 1:
        return tail_of(value[0:1] + value[1:2])
    return jnp.concatenate(split(value[:pair] + value[pair:]), axis=0)


def core_body(layout, own_ref, got_ref, *outs):
    at = 0
    for out in outs:
        to = 0
        for size, pair in layout:
            out[to : to + size] = summed([own_ref, got_ref], at, size, pair)
            at += size
            to += size


def join_body(layouts, *refs):
    *parts, out = refs
    to = 0
    for i, layout in enumerate(layouts):
        at = 0
        for size, pair in layout:
            out[to : to + size] = summed(parts[i :: len(layouts)], at, size, pair)
            at += size
            to += size


def total_body(layout, *refs):
    *parts, out, short = refs
    at = to = 0
    for size, pair in layout:
        value = summed(parts, at, size, pair)
        out[at : at + size] = value
        kept = pair if pair > 1 else size
        short[to : to + kept] = value[:kept]
        at += size
        to += kept


def iterate_body(slots, n_base, notes_ref, *refs):
    base = lax.axis_index("base")
    *chunks, out_ref, gram_ref = refs
    chans = out_ref.shape[0]
    rows, cols = corner()
    n_off = slots * (slots - 1) // 2
    g_rows = pack_rows(slots, n_base)
    half = min(TILE, g_rows & -g_rows)
    states, datas, diags = [], [], []

    def put(g, r, s, block):
        gram_ref[g, r * TILE : (r + 1) * TILE, s * TILE : (s + 1) * TILE] = block

    for g in range(2):
        full = in_order([ref[...] for ref in chunks[g * n_base : (g + 1) * n_base]], base)
        for i, (r, s) in enumerate(pairs(slots)):
            pieces = []
            for q in range(TILE // half):
                at = i * TILE + q * half
                pieces.append(full[at // g_rows][at % g_rows : at % g_rows + half])
            block = jnp.concatenate(pieces, axis=0)
            if i < n_off:
                put(g, r, s, block)
                put(g, s, r, block.T)
            else:
                upper = jnp.where(rows < cols, block, jnp.zeros_like(block))
                lower = jnp.where(rows > cols, block, jnp.zeros_like(block))
                put(g, r, r, upper + upper.T)
                put(g, s, s, lower + lower.T)
        per = slots // n_base
        wide = (full[0].shape[0] - g_rows - per * PAD) // (2 * per)

        def gather(at, pitch):
            values = []
            for r in range(slots):
                v = full[r // per][at + (r % per) * pitch :][:wide].astype(jnp.float32)
                values.append(v[:chans] + v[chans:] if wide > chans else v)
            return jnp.concatenate(values, axis=1)

        datas.append(gather(g_rows, wide + PAD))
        states.append(gather(g_rows + per * (wide + PAD), wide))
        tails = []
        for r in range(slots):
            v = full[r // per][g_rows + (r % per) * (wide + PAD) + wide :][:PAD].astype(jnp.float32)
            tails.append(v[0:1] + v[1:2])
        diags.append(jnp.concatenate(tails, axis=1))
    tile = lambda v, r: v[:, r * TILE : (r + 1) * TILE]
    for step in range(ITERS):
        parts = [[], []]
        if step < ITERS - 1:
            for g in range(2):
                high, low = split(states[g])
                left = jnp.concatenate([high, low], axis=0) if g == 0 else high
                for r in range(slots):
                    rows_r = gram_ref[g, r * TILE : (r + 1) * TILE, :]
                    part = jnp.dot(tile(left, r), rows_r, preferred_element_type=jnp.float32)
                    parts[g].append(part[:chans] + part[chans:] if g == 0 else part)
        squares = states[0] * states[0] + states[1] * states[1]
        column = jnp.sum(squares, axis=0, keepdims=True)
        factors = []
        for r in range(slots):
            norm = jnp.sum(tile(column, r), axis=1, keepdims=True)
            rms = jnp.sqrt(norm / (CH * TILE) + eps_norm)
            factors.append(rms / (rms + lam_shrink))
        factor = jnp.concatenate([jnp.broadcast_to(f, (1, TILE)) for f in factors], axis=1)
        states = [state * factor for state in states]
        if step == ITERS - 1:
            break
        for g in range(2):
            product = states[g] * diags[g]
            for f, part in zip(factors, parts[g]):
                product = product + f * part
            states[g] = states[g] + descent_stride * (datas[g] - product)
    mark = notes_ref[PAD - 2 : PAD - 1, :].astype(jnp.float32)
    image = jnp.zeros(out_ref.shape, jnp.float32)
    for r in range(slots):
        image = jnp.where(mark == r, states[0][:, r * TILE : (r + 1) * TILE], image)
    out_ref[...] = image


def gram_plan(sensing_operator_parts, sampled_correlations, first_sky_estimate, patch_order_record):
    a = sensing_operator_parts[0]
    chans, m_dev = sampled_correlations.shape
    n_base, n_pix = lax.axis_size("base"), lax.axis_size("pix")
    slots = n_base * n_pix // 4
    quarter = m_dev // n_pix
    x0 = first_sky_estimate[:, 0, 0, :]
    ranks = pltpu.with_memory_space_constraint(patch_order_record.T, pltpu.HBM)
    shape = jax.ShapeDtypeStruct
    bf16, f32 = jnp.bfloat16, jnp.float32

    def pieces_of(places):
        return [shape((places * quarter + PAD, TILE), bf16)] * (n_pix - 1)

    tiles = ranks.shape[0]
    places = min(CAPACITY, tiles)
    *packed, notes, x0_round = call(
        functools.partial(pack_body, slots),
        pieces_of(places) + [shape((PAD, TILE), bf16), shape(x0.shape, bf16)],
        (ranks, a, x0),
        smem=(0,),
    )
    parts = send(packed)

    def rest():
        packed = call(functools.partial(rest_body, places), pieces_of(tiles - places), (notes, a))
        return send(packed)

    shares = [x0_round] + [swap(x0_round, "base", d) for d in range(1, n_base)]
    firsts = call(
        first_body,
        [shape((chans, quarter), bf16)] * n_pix,
        (a, *shares),
        scratch=[pltpu.VMEM((chans, n_base * TILE), bf16)],
    )
    preds = [firsts[0]] + send(firsts[1:])

    per = slots // n_base
    gram_layout = [(pack_rows(slots, n_base), 0)] + [(2 * chans, chans), (PAD, 1)] * per
    side_layout = [(2 * chans, chans)] * per
    layouts = [gram_layout, side_layout]
    heights = [sum(size for size, _ in layout) for layout in layouts]
    chunk = shape((sum(heights), TILE), bf16)
    short = shape((chunk.shape[0] - 2 * chans * per, TILE), bf16)

    def halves(height):
        return [shape((n_base // 2 * height, TILE), bf16)] * 2

    def base_sum(parts):
        columns, *gram = call(
            functools.partial(gram_body, slots, len(parts)),
            [shape((quarter, slots * TILE), bf16)] + halves(heights[0]),
            (sampled_correlations, a, notes, *parts),
            scratch=[pltpu.VMEM((n_base, heights[0], TILE), bf16)],
        )
        side = call(
            functools.partial(start_body, slots, n_pix),
            halves(heights[1]),
            (sampled_correlations, x0, notes, columns, *preds),
            scratch=[pltpu.VMEM((n_base, heights[1], TILE), bf16)],
        )
        pieces = []
        for (own, sent), layout in zip((gram, side), layouts):
            height = sum(size for size, _ in layout)
            sums = call(
                functools.partial(core_body, layout),
                [shape((height, TILE), bf16)] * (n_base // 2),
                (own, swap(sent, "base", 1)),
            )
            far = [swap(sums[k], "base", 2 * k) for k in range(1, n_base // 2)]
            pieces.append([sums[0], *far])
        return [piece for pair in zip(*pieces) for piece in pair]

    def join(pieces):
        return call(functools.partial(join_body, layouts), chunk, pieces)

    crowded = call(functools.partial(crowd_body, places), shape((1,), jnp.int32), (notes, *parts), scalars=(0,))[0]
    pieces = base_sum(parts)
    part = lax.cond(crowded != 0, lambda: join(base_sum(parts + rest())), lambda: join(pieces))
    total, brief = call(
        functools.partial(total_body, gram_layout + side_layout), [chunk, short], [part] + send([part] * (n_pix - 1))
    )

    axes = ("freq", "base")
    got = {0: total, n_base: swap(brief, axes, n_base)}
    for offset in range(2, n_base, 2):
        got[n_base + offset] = swap(brief, axes, n_base + offset)
        got[offset] = swap(total, axes, offset)
    got[1] = swap(total, axes, 1)
    for offset in range(2, 2 * n_base, 2):
        got[offset + 1] = swap(got[offset], axes, 1)
    image = call(
        functools.partial(iterate_body, slots, n_base),
        shape((chans, TILE), f32),
        (notes, *[got[i] for i in range(2 * n_base)]),
        scratch=[
            pltpu.VMEM((2, slots * TILE, slots * TILE), bf16),
        ],
    )
    return image.reshape(chans, 1, 1, TILE)


def on_device(sensing_operator_parts, sampled_correlations, first_sky_estimate, patch_order_record):
    n_base, n_pix = lax.axis_size("base"), lax.axis_size("pix")
    slots = n_base * n_pix // 4
    chans, m_dev = sampled_correlations.shape
    fits = (
        first_sky_estimate.shape[3] == TILE
        and (slots * TILE) ** 2 <= GRAM_LIMIT
        and n_base & (n_base - 1) == 0
        and n_pix & (n_pix - 1) == 0
        and slots % n_base == 0
        and slots % 2 == 0
        and len(pairs(slots)) * TILE % (n_base * 16) == 0
        and m_dev % (n_pix * TILE) == 0
        and lax.axis_size("freq") == 2
        and chans % 16 == 0
    )
    plan = gram_plan if fits else streaming
    return plan(sensing_operator_parts, sampled_correlations, first_sky_estimate, patch_order_record)


def solution(mesh):
    in_specs = (
        P("freq", "base", "pix"),
        P("freq", "base"),
        P("freq", "pix", "base", None),
        P(None, "pix"),
    )
    out_specs = P("freq", "pix", "base", None)
    return jax.shard_map(
        on_device, mesh=mesh, in_specs=in_specs, out_specs=out_specs, check_vma=False
    )
```

```python
import functools

import jax
import jax.numpy as jnp
from jax import lax
from jax.experimental import pallas as pl
from jax.experimental.pallas import tpu as pltpu
from jax.sharding import PartitionSpec as P

CH = 64
TILE = 128
ITERS = 6


descent_stride = 0.6
lam_shrink = 0.3
eps_norm = 1e-06


GRAM_LIMIT = 1 << 20
PAD = 8
CAPACITY = 2
VMEM_LIMIT = 12 << 20


def project_rows(rounded_amount, columns):
    return lax.dot_general(
        rounded_amount, columns, (((1,), (1,)), ((), ())), preferred_element_type=jnp.float32
    )


def residual_of(sampled_correlations, partial_value):
    shares = lax.psum_scatter(partial_value, "pix", scatter_dimension=1, tiled=True)
    width = shares.shape[1]
    own_rows = lax.dynamic_slice_in_dim(
        sampled_correlations, lax.axis_index("pix") * width, width, 1
    )
    return lax.all_gather((own_rows - shares).astype(jnp.bfloat16), "pix", axis=1, tiled=True)


def streaming(sensing_operator_parts, sampled_correlations, first_sky_estimate, patch_order_record):
    sensing_operator = sensing_operator_parts[0]
    chans, _ = sampled_correlations.shape
    share_width = first_sky_estimate.shape[3]
    tiles_share = share_width // TILE
    keep_count = tiles_share * lax.axis_size("base") * lax.axis_size("pix") // 4
    base_index = lax.axis_index("base")
    own_share = first_sky_estimate[:, 0, 0, :]
    current = own_share
    for step in range(ITERS):
        rounded_amount = current.astype(jnp.bfloat16)
        partial_value = project_rows(
            lax.all_gather(rounded_amount, "base", axis=1, tiled=True), sensing_operator
        )
        resid = residual_of(sampled_correlations, partial_value)
        gradient_portion = jnp.dot(resid, sensing_operator, preferred_element_type=jnp.float32)
        grad_share = lax.psum_scatter(gradient_portion, "base", scatter_dimension=1, tiled=True)
        moved = current + descent_stride * grad_share
        tiles = moved.reshape(chans, tiles_share, TILE)
        local_sum = jnp.sum(tiles * tiles, axis=(0, 2))
        total = lax.psum(local_sum, "freq")
        ranks = lax.dynamic_slice_in_dim(
            patch_order_record[step], base_index * tiles_share, tiles_share, 0
        )
        rms_tile = jnp.sqrt(total / (CH * TILE) + eps_norm)
        keeping = (ranks < keep_count).astype(jnp.float32)
        factor = keeping * rms_tile / (rms_tile + lam_shrink)
        current = (tiles * factor[None, :, None]).reshape(chans, share_width)
    return current.reshape(chans, 1, 1, share_width)


def swap(value, axis, offset):
    size = lax.axis_size(axis)
    return lax.ppermute(value, axis, [(i, i ^ offset) for i in range(size)])


def routes(size):
    if size == 4:
        return [(1, 3, 0, 2), (3, 2, 1, 0), (2, 0, 3, 1)]
    return [tuple(i ^ d for i in range(size)) for d in range(1, size)]


def send(pieces):
    got = []
    for piece, route in zip(pieces, routes(lax.axis_size("pix"))):
        got.append(lax.ppermute(piece, "pix", list(enumerate(route))))
    return got


def target(pix, k, size):
    if k == 0:
        return pix
    place = jnp.int32(0)
    for i, to in enumerate(routes(size)[k - 1]):
        place = jnp.where(pix == i, to, place)
    return place


def call(body, out_shape, args, scratch=(), smem=(), scalars=()):
    specs = [pl.BlockSpec(memory_space=pltpu.SMEM if i in smem else pltpu.VMEM) for i in range(len(args))]
    place = lambda i: pltpu.SMEM if i in scalars else pltpu.VMEM
    if isinstance(out_shape, list):
        out_specs = [pl.BlockSpec(memory_space=place(i)) for i in range(len(out_shape))]
    else:
        out_specs = pl.BlockSpec(memory_space=place(0))
    return pl.pallas_call(
        body,
        out_shape=out_shape,
        in_specs=specs,
        out_specs=out_specs,
        scratch_shapes=list(scratch),
        compiler_params=pltpu.CompilerParams(vmem_limit_bytes=VMEM_LIMIT),
    )(*args)


def split(value):
    high = value.astype(jnp.bfloat16)
    return high, (value - high.astype(jnp.float32)).astype(jnp.bfloat16)


def pack_body(slots, ranks_ref, a_ref, x0_ref, *outs):
    *outs, notes_ref, round_ref = outs
    round_ref[...] = x0_ref[...].astype(jnp.bfloat16)
    pix, base = lax.axis_index("pix"), lax.axis_index("base")
    tiles = ranks_ref.shape[0]
    quarter = a_ref.shape[0] // (len(outs) + 1)
    places = (outs[0].shape[0] - PAD) // quarter
    rows = lax.broadcasted_iota(jnp.int32, (PAD, TILE), 0)
    count = jnp.int32(0)
    table = []
    notes = jnp.full((PAD, TILE), -1, jnp.int32)
    for j in range(tiles):
        rank = ranks_ref[j, 0]
        slot = jnp.where(rank < slots, rank, -1)
        table.append((slot, count))
        notes = jnp.where(rows == j, slot, notes)
        notes = jnp.where(jnp.logical_and(rows == PAD - 2, base == j), slot, notes)
        count = count + jnp.where(rank < slots, 1, 0)
    notes = jnp.where(rows == PAD - 1, count, notes)
    notes_ref[...] = notes.astype(jnp.float32).astype(jnp.bfloat16)
    sent = jnp.where(rows == PAD - 1, count, -1)
    for i in range(places):
        tile = jnp.int32(0)
        for j, (slot, before) in enumerate(table):
            hit = jnp.logical_and(slot >= 0, before == i)
            tile = jnp.where(hit, j, tile)
            sent = jnp.where(jnp.logical_and(rows == i, hit), slot, sent)
        lanes = pl.ds(pl.multiple_of(tile * TILE, TILE), TILE)
        for d, out in enumerate(outs):
            at = pl.ds(pl.multiple_of(target(pix, d + 1, len(outs) + 1) * quarter, quarter), quarter)
            out[i * quarter : (i + 1) * quarter, :] = a_ref[at, lanes]
    for out in outs:
        out[places * quarter :, :] = sent.astype(jnp.float32).astype(jnp.bfloat16)


def rest_body(first, notes_ref, a_ref, *outs):
    pix = lax.axis_index("pix")
    quarter = a_ref.shape[0] // (len(outs) + 1)
    places = (outs[0].shape[0] - PAD) // quarter
    notes = notes_ref[...].astype(jnp.float32)
    tiles = a_ref.shape[1] // TILE
    rows = lax.broadcasted_iota(jnp.int32, (PAD, TILE), 0)
    before = jnp.zeros((1, TILE), jnp.float32)
    sent = jnp.full((PAD, TILE), -1.0, jnp.float32)
    hits = []
    for j in range(tiles):
        slot = notes[j : j + 1]
        hits.append([jnp.logical_and(slot >= 0, before == first + i) for i in range(places)])
        for i in range(places):
            sent = jnp.where(jnp.logical_and(rows == i, hits[j][i]), slot, sent)
        before = before + jnp.where(slot >= 0, 1.0, 0.0)
    for d, out in enumerate(outs):
        at = pl.ds(pl.multiple_of(target(pix, d + 1, len(outs) + 1) * quarter, quarter), quarter)
        for i in range(places):
            block = a_ref[at, :TILE]
            for j in range(1, tiles):
                tile = a_ref[at, j * TILE : (j + 1) * TILE]
                block = jnp.where(jnp.broadcast_to(hits[j][i], block.shape), tile, block)
            out[i * quarter : (i + 1) * quarter, :] = block
        out[places * quarter :, :] = sent.astype(jnp.bfloat16)


def crowd_body(places, *refs):
    *parts, out_ref = refs
    most = parts[0][-PAD:, :].astype(jnp.float32)
    for part in parts[1:]:
        most = jnp.maximum(most, part[-PAD:, :].astype(jnp.float32))
    rows = lax.broadcasted_iota(jnp.int32, (PAD, TILE), 0)
    most = jnp.max(jnp.where(rows == PAD - 1, most, -1.0))
    out_ref[0] = jnp.where(most > places, 1, 0)


def first_body(a_ref, *refs):
    pix, base = lax.axis_index("pix"), lax.axis_index("base")
    n_base = a_ref.shape[1] // TILE
    shares, rest = refs[:n_base], refs[n_base:]
    outs, x_ref = rest[:-1], rest[-1]
    quarter = outs[0].shape[1]
    for d, share in enumerate(shares):
        x_ref[:, pl.ds(pl.multiple_of((base ^ d) * TILE, TILE), TILE)] = share[...]
    for d, out in enumerate(outs):
        rows = pl.ds(pl.multiple_of(target(pix, d, len(outs)) * quarter, quarter), quarter)
        piece = lax.dot_general(
            x_ref[...], a_ref[rows, :], (((1,), (1,)), ((), ())), preferred_element_type=jnp.float32
        )
        out[...] = piece.astype(out.dtype)


def in_order(values, index):
    bit = 1
    while bit < len(values):
        odd = (index & bit) != 0
        values = [jnp.where(odd, values[d ^ bit], values[d]) for d in range(len(values))]
        bit *= 2
    return values


def pairs(slots):
    return [(r, s) for r in range(slots) for s in range(r + 1, slots)] + [(r, r + 1) for r in range(0, slots, 2)]


def pack_rows(slots, n_base):
    return len(pairs(slots)) * TILE // n_base


def corner():
    rows = lax.broadcasted_iota(jnp.int32, (TILE, TILE), 0)
    cols = lax.broadcasted_iota(jnp.int32, (TILE, TILE), 1)
    return rows, cols


def gram_body(slots, n_parts, y_ref, a_ref, notes_ref, *refs):
    pix, base = lax.axis_index("pix"), lax.axis_index("base")
    parts = refs[:n_parts]
    cols_ref, own_ref, sent_ref, all_ref = refs[n_parts:]
    n_base = all_ref.shape[0]
    chans, quarter = y_ref.shape[0], cols_ref.shape[0]
    own_rows = pl.ds(pl.multiple_of(pix * quarter, quarter), quarter)
    tiles = a_ref.shape[1] // TILE
    blocks = [a_ref[own_rows, j * TILE : (j + 1) * TILE] for j in range(tiles)]
    notes = notes_ref[...].astype(jnp.float32)
    marks = [notes[j : j + 1] for j in range(tiles)]
    for part in parts:
        places = (part.shape[0] - PAD) // quarter
        notes = part[places * quarter :, :].astype(jnp.float32)
        blocks += [part[i * quarter : (i + 1) * quarter, :] for i in range(places)]
        marks += [notes[i : i + 1] for i in range(places)]
    columns = []
    for r in range(slots):
        column = jnp.zeros((quarter, TILE), jnp.bfloat16)
        for block, mark in zip(blocks, marks):
            column = jnp.where(jnp.broadcast_to(mark == r, column.shape), block, column)
        columns.append(column)
    a = jnp.concatenate(columns, axis=1)
    cols_ref[...] = a
    y = y_ref[:, pl.ds(pl.multiple_of(pix * quarter, quarter), quarter)]
    both = jnp.dot(jnp.concatenate(split(y), axis=0), a, preferred_element_type=jnp.float32)
    data = both[:chans] + both[chans:]
    gram = lax.dot_general(a, a, (((0,), (0,)), ((), ())), preferred_element_type=jnp.float32)
    rows, cols = corner()
    g_rows = pack_rows(slots, n_base)
    per = slots // n_base
    half = min(TILE, g_rows & -g_rows)

    def block_of(r, s):
        return gram[r * TILE : (r + 1) * TILE, s * TILE : (s + 1) * TILE]

    n_off = slots * (slots - 1) // 2
    for i, (r, s) in enumerate(pairs(slots)):
        block = block_of(r, s) if i < n_off else jnp.where(rows < cols, block_of(r, r), block_of(s, s))
        block = block.astype(jnp.bfloat16)
        for q in range(TILE // half):
            at = i * TILE + q * half
            all_ref[at // g_rows, at % g_rows : at % g_rows + half, :] = block[q * half : (q + 1) * half]
    for r in range(slots):
        diag = jnp.sum(jnp.where(rows == cols, block_of(r, r), 0.0), axis=0, keepdims=True)
        at = g_rows + (r % per) * (2 * chans + PAD)
        wide = jnp.concatenate(split(data[:, r * TILE : (r + 1) * TILE]), axis=0)
        all_ref[r // per, at : at + 2 * chans, :] = wide
        all_ref[r // per, at + 2 * chans : at + 2 * chans + PAD, :] = tail_of(diag)
    by_core(base, all_ref, own_ref, sent_ref)


def by_core(base, all_ref, own_ref, sent_ref):
    size = all_ref.shape[1]
    for k in range(all_ref.shape[0] // 2):
        own_ref[k * size : (k + 1) * size, :] = all_ref[base ^ (2 * k)]
        sent_ref[k * size : (k + 1) * size, :] = all_ref[base ^ (2 * k + 1)]


def tail_of(row):
    return jnp.concatenate([*split(row), jnp.zeros((PAD - 2, TILE), jnp.bfloat16)], axis=0)


def start_body(slots, n_pix, y_ref, x0_ref, notes_ref, cols_ref, *refs):
    pix, base = lax.axis_index("pix"), lax.axis_index("base")
    preds = refs[:n_pix]
    own_ref, sent_ref, all_ref = refs[n_pix:]
    per = slots // all_ref.shape[0]
    chans, quarter = preds[0].shape
    pred = preds[0][...].astype(jnp.float32)
    for piece in preds[1:]:
        pred = pred + piece[...].astype(jnp.float32)
    y = y_ref[:, pl.ds(pl.multiple_of(pix * quarter, quarter), quarter)]
    resid = (y - pred).astype(jnp.bfloat16)
    moved = descent_stride * jnp.dot(resid, cols_ref[...], preferred_element_type=jnp.float32)
    mark = notes_ref[PAD - 2 : PAD - 1, :].astype(jnp.float32)
    for r in range(slots):
        start = moved[:, r * TILE : (r + 1) * TILE] + jnp.where(mark == r, x0_ref[...], 0.0)
        at = (r % per) * 2 * chans
        all_ref[r // per, at : at + 2 * chans, :] = jnp.concatenate(split(start), axis=0)
    by_core(base, all_ref, own_ref, sent_ref)


def summed(parts, at, size, pair):
    value = parts[0][at : at + size].astype(jnp.float32)
    for part in parts[1:]:
        value = value + part[at : at + size].astype(jnp.float32)
    if pair == 0:
        return value.astype(jnp.bfloat16)
    if pair == 1:
        return tail_of(value[0:1] + value[1:2])
    return jnp.concatenate(split(value[:pair] + value[pair:]), axis=0)


def core_body(layout, own_ref, got_ref, *outs):
    at = 0
    for out in outs:
        to = 0
        for size, pair in layout:
            out[to : to + size] = summed([own_ref, got_ref], at, size, pair)
            at += size
            to += size


def join_body(layouts, *refs):
    *parts, out = refs
    to = 0
    for i, layout in enumerate(layouts):
        at = 0
        for size, pair in layout:
            place = out.shape[0] - size if pair == 1 else to
            out[place : place + size] = summed(parts[i :: len(layouts)], at, size, pair)
            at += size
            to += 0 if pair == 1 else size


def total_body(layout, *refs):
    *parts, out, short = refs
    at = to = 0
    for size, pair in layout:
        value = summed(parts, at, size, pair)
        out[at : at + size] = value
        kept = pair if pair > 1 else size
        short[to : to + kept] = value[:kept]
        at += size
        to += kept


def iterate_body(slots, n_base, notes_ref, *refs):
    base = lax.axis_index("base")
    *chunks, out_ref, gram_ref = refs
    chans = out_ref.shape[0]
    rows, cols = corner()
    n_off = slots * (slots - 1) // 2
    g_rows = pack_rows(slots, n_base)
    half = min(TILE, g_rows & -g_rows)
    states, datas, diags = [], [], []

    def put(g, r, s, block):
        gram_ref[g, r * TILE : (r + 1) * TILE, s * TILE : (s + 1) * TILE] = block

    for g in range(2):
        full = in_order([ref[...] for ref in chunks[g * n_base : (g + 1) * n_base]], base)
        for i, (r, s) in enumerate(pairs(slots)):
            pieces = []
            for q in range(TILE // half):
                at = i * TILE + q * half
                pieces.append(full[at // g_rows][at % g_rows : at % g_rows + half])
            block = jnp.concatenate(pieces, axis=0)
            if i < n_off:
                put(g, r, s, block)
                put(g, s, r, block.T)
            else:
                upper = jnp.where(rows < cols, block, jnp.zeros_like(block))
                lower = jnp.where(rows > cols, block, jnp.zeros_like(block))
                put(g, r, r, upper + upper.T)
                put(g, s, s, lower + lower.T)
        wide = (full[0].shape[0] - g_rows - PAD) // 2

        def gather(at):
            values = [v[at : at + wide].astype(jnp.float32) for v in full]
            return jnp.concatenate([v[:chans] + v[chans:] if wide > chans else v for v in values], axis=1)

        datas.append(gather(g_rows))
        states.append(gather(g_rows + wide))
        tails = [v[g_rows + 2 * wide :].astype(jnp.float32) for v in full]
        diags.append(jnp.concatenate([t[0:1] + t[1:2] for t in tails], axis=1))
    tile = lambda v, r: v[:, r * TILE : (r + 1) * TILE]
    for step in range(ITERS):
        parts = [[], []]
        if step < ITERS - 1:
            for g in range(2):
                high, low = split(states[g])
                left = jnp.concatenate([high, low], axis=0) if g == 0 else high
                for r in range(slots):
                    rows_r = gram_ref[g, r * TILE : (r + 1) * TILE, :]
                    part = jnp.dot(tile(left, r), rows_r, preferred_element_type=jnp.float32)
                    parts[g].append(part[:chans] + part[chans:] if g == 0 else part)
        squares = states[0] * states[0] + states[1] * states[1]
        column = jnp.sum(squares, axis=0, keepdims=True)
        factors = []
        for r in range(slots):
            norm = jnp.sum(tile(column, r), axis=1, keepdims=True)
            rms = jnp.sqrt(norm / (CH * TILE) + eps_norm)
            factors.append(rms / (rms + lam_shrink))
        factor = jnp.concatenate([jnp.broadcast_to(f, (1, TILE)) for f in factors], axis=1)
        states = [state * factor for state in states]
        if step == ITERS - 1:
            break
        for g in range(2):
            product = states[g] * diags[g]
            for f, part in zip(factors, parts[g]):
                product = product + f * part
            states[g] = states[g] + descent_stride * (datas[g] - product)
    mark = notes_ref[PAD - 2 : PAD - 1, :].astype(jnp.float32)
    image = jnp.zeros(out_ref.shape, jnp.float32)
    for r in range(slots):
        image = jnp.where(mark == r, states[0][:, r * TILE : (r + 1) * TILE], image)
    out_ref[...] = image


def gram_plan(sensing_operator_parts, sampled_correlations, first_sky_estimate, patch_order_record):
    a = sensing_operator_parts[0]
    chans, m_dev = sampled_correlations.shape
    n_base, n_pix = lax.axis_size("base"), lax.axis_size("pix")
    slots = n_base * n_pix // 4
    quarter = m_dev // n_pix
    x0 = first_sky_estimate[:, 0, 0, :]
    ranks = pltpu.with_memory_space_constraint(patch_order_record.T, pltpu.HBM)
    shape = jax.ShapeDtypeStruct
    bf16, f32 = jnp.bfloat16, jnp.float32

    def pieces_of(places):
        return [shape((places * quarter + PAD, TILE), bf16)] * (n_pix - 1)

    tiles = ranks.shape[0]
    places = min(CAPACITY, tiles)
    *packed, notes, x0_round = call(
        functools.partial(pack_body, slots),
        pieces_of(places) + [shape((PAD, TILE), bf16), shape(x0.shape, bf16)],
        (ranks, a, x0),
        smem=(0,),
    )
    parts = send(packed)

    def rest():
        packed = call(functools.partial(rest_body, places), pieces_of(tiles - places), (notes, a))
        return send(packed)

    shares = [x0_round] + [swap(x0_round, "base", d) for d in range(1, n_base)]
    firsts = call(
        first_body,
        [shape((chans, quarter), bf16)] * n_pix,
        (a, *shares),
        scratch=[pltpu.VMEM((chans, n_base * TILE), bf16)],
    )
    preds = [firsts[0]] + send(firsts[1:])

    per = slots // n_base
    gram_layout = [(pack_rows(slots, n_base), 0), (2 * chans, chans), (PAD, 1)]
    side_layout = [(2 * chans, chans)]
    total_layout = [gram_layout[0], gram_layout[1], *side_layout, gram_layout[2]]
    layouts = [gram_layout, side_layout]
    heights = [sum(size for size, _ in layout) for layout in layouts]
    chunk = shape((sum(heights), TILE), bf16)
    short = shape((chunk.shape[0] - 2 * chans * per, TILE), bf16)

    def halves(height):
        return [shape((n_base // 2 * height, TILE), bf16)] * 2

    def base_sum(parts):
        columns, *gram = call(
            functools.partial(gram_body, slots, len(parts)),
            [shape((quarter, slots * TILE), bf16)] + halves(heights[0]),
            (sampled_correlations, a, notes, *parts),
            scratch=[pltpu.VMEM((n_base, heights[0], TILE), bf16)],
        )
        side = call(
            functools.partial(start_body, slots, n_pix),
            halves(heights[1]),
            (sampled_correlations, x0, notes, columns, *preds),
            scratch=[pltpu.VMEM((n_base, heights[1], TILE), bf16)],
        )
        pieces = []
        for (own, sent), layout in zip((gram, side), layouts):
            height = sum(size for size, _ in layout)
            sums = call(
                functools.partial(core_body, layout),
                [shape((height, TILE), bf16)] * (n_base // 2),
                (own, swap(sent, "base", 1)),
            )
            far = [swap(sums[k], "base", 2 * k) for k in range(1, n_base // 2)]
            pieces.append([sums[0], *far])
        return [piece for pair in zip(*pieces) for piece in pair]

    def join(pieces):
        return call(functools.partial(join_body, layouts), chunk, pieces)

    crowded = call(functools.partial(crowd_body, places), shape((1,), jnp.int32), (notes, *parts), scalars=(0,))[0]
    pieces = base_sum(parts)
    part = lax.cond(crowded != 0, lambda: join(base_sum(parts + rest())), lambda: join(pieces))
    total, brief = call(
        functools.partial(total_body, total_layout), [chunk, short], [part] + send([part] * (n_pix - 1))
    )

    axes = ("freq", "base")
    got = {0: total, n_base: swap(brief, axes, n_base)}
    for offset in range(2, n_base, 2):
        got[n_base + offset] = swap(brief, axes, n_base + offset)
        got[offset] = swap(total, axes, offset)
    got[1] = swap(total, axes, 1)
    for offset in range(2, 2 * n_base, 2):
        got[offset + 1] = swap(got[offset], axes, 1)
    image = call(
        functools.partial(iterate_body, slots, n_base),
        shape((chans, TILE), f32),
        (notes, *[got[i] for i in range(2 * n_base)]),
        scratch=[
            pltpu.VMEM((2, slots * TILE, slots * TILE), bf16),
        ],
    )
    return image.reshape(chans, 1, 1, TILE)


def on_device(sensing_operator_parts, sampled_correlations, first_sky_estimate, patch_order_record):
    n_base, n_pix = lax.axis_size("base"), lax.axis_size("pix")
    slots = n_base * n_pix // 4
    chans, m_dev = sampled_correlations.shape
    fits = (
        first_sky_estimate.shape[3] == TILE
        and (slots * TILE) ** 2 <= GRAM_LIMIT
        and n_base & (n_base - 1) == 0
        and n_pix & (n_pix - 1) == 0
        and slots == n_base
        and n_base <= PAD - 2
        and slots % 2 == 0
        and len(pairs(slots)) * TILE % (n_base * 16) == 0
        and m_dev % (n_pix * TILE) == 0
        and lax.axis_size("freq") == 2
        and chans % 16 == 0
    )
    plan = gram_plan if fits else streaming
    return plan(sensing_operator_parts, sampled_correlations, first_sky_estimate, patch_order_record)


def solution(mesh):
    in_specs = (
        P("freq", "base", "pix"),
        P("freq", "base"),
        P("freq", "pix", "base", None),
        P(None, "pix"),
    )
    out_specs = P("freq", "pix", "base", None)
    return jax.shard_map(
        on_device, mesh=mesh, in_specs=in_specs, out_specs=out_specs, check_vma=False
    )
```

```python
import functools

import jax
import jax.numpy as jnp
from jax import lax
from jax.experimental import pallas as pl
from jax.experimental.pallas import tpu as pltpu
from jax.sharding import PartitionSpec as P

CH = 64
TILE = 128
ITERS = 6


descent_stride = 0.6
lam_shrink = 0.3
eps_norm = 1e-06


GRAM_LIMIT = 1 << 20
PAD = 8
CAPACITY = 2
VMEM_LIMIT = 12 << 20


def project_rows(rounded_amount, columns):
    return lax.dot_general(
        rounded_amount, columns, (((1,), (1,)), ((), ())), preferred_element_type=jnp.float32
    )


def residual_of(sampled_correlations, partial_value):
    shares = lax.psum_scatter(partial_value, "pix", scatter_dimension=1, tiled=True)
    width = shares.shape[1]
    own_rows = lax.dynamic_slice_in_dim(
        sampled_correlations, lax.axis_index("pix") * width, width, 1
    )
    return lax.all_gather((own_rows - shares).astype(jnp.bfloat16), "pix", axis=1, tiled=True)


def streaming(sensing_operator_parts, sampled_correlations, first_sky_estimate, patch_order_record):
    sensing_operator = sensing_operator_parts[0]
    chans, _ = sampled_correlations.shape
    share_width = first_sky_estimate.shape[3]
    tiles_share = share_width // TILE
    keep_count = tiles_share * lax.axis_size("base") * lax.axis_size("pix") // 4
    base_index = lax.axis_index("base")
    own_share = first_sky_estimate[:, 0, 0, :]
    current = own_share
    for step in range(ITERS):
        rounded_amount = current.astype(jnp.bfloat16)
        partial_value = project_rows(
            lax.all_gather(rounded_amount, "base", axis=1, tiled=True), sensing_operator
        )
        resid = residual_of(sampled_correlations, partial_value)
        gradient_portion = jnp.dot(resid, sensing_operator, preferred_element_type=jnp.float32)
        grad_share = lax.psum_scatter(gradient_portion, "base", scatter_dimension=1, tiled=True)
        moved = current + descent_stride * grad_share
        tiles = moved.reshape(chans, tiles_share, TILE)
        local_sum = jnp.sum(tiles * tiles, axis=(0, 2))
        total = lax.psum(local_sum, "freq")
        ranks = lax.dynamic_slice_in_dim(
            patch_order_record[step], base_index * tiles_share, tiles_share, 0
        )
        rms_tile = jnp.sqrt(total / (CH * TILE) + eps_norm)
        keeping = (ranks < keep_count).astype(jnp.float32)
        factor = keeping * rms_tile / (rms_tile + lam_shrink)
        current = (tiles * factor[None, :, None]).reshape(chans, share_width)
    return current.reshape(chans, 1, 1, share_width)


def swap(value, axis, offset):
    size = lax.axis_size(axis)
    return lax.ppermute(value, axis, [(i, i ^ offset) for i in range(size)])


def routes(size):
    if size == 4:
        return [(1, 3, 0, 2), (3, 2, 1, 0), (2, 0, 3, 1)]
    return [tuple(i ^ d for i in range(size)) for d in range(1, size)]


def send(pieces):
    got = []
    for piece, route in zip(pieces, routes(lax.axis_size("pix"))):
        got.append(lax.ppermute(piece, "pix", list(enumerate(route))))
    return got


def target(pix, k, size):
    if k == 0:
        return pix
    place = jnp.int32(0)
    for i, to in enumerate(routes(size)[k - 1]):
        place = jnp.where(pix == i, to, place)
    return place


def call(body, out_shape, args, scratch=(), hbm=(), scalars=()):
    specs = [pl.BlockSpec(memory_space=pltpu.HBM if i in hbm else pltpu.VMEM) for i in range(len(args))]
    place = lambda i: pltpu.SMEM if i in scalars else pltpu.VMEM
    if isinstance(out_shape, list):
        out_specs = [pl.BlockSpec(memory_space=place(i)) for i in range(len(out_shape))]
    else:
        out_specs = pl.BlockSpec(memory_space=place(0))
    return pl.pallas_call(
        body,
        out_shape=out_shape,
        in_specs=specs,
        out_specs=out_specs,
        scratch_shapes=list(scratch),
        compiler_params=pltpu.CompilerParams(vmem_limit_bytes=VMEM_LIMIT),
    )(*args)


def split(value):
    high = value.astype(jnp.bfloat16)
    return high, (value - high.astype(jnp.float32)).astype(jnp.bfloat16)


def pack_body(slots, n_pix, ranks_hbm, a_hbm, x0_hbm, out, notes_ref, round_ref, ranks_ref, a_ref, x0_ref, sems):
    pix, base = lax.axis_index("pix"), lax.axis_index("base")
    tiles = ranks_ref.shape[0]
    quarter = a_ref.shape[0]
    places = (out.shape[0] - PAD) // quarter
    at = pl.ds(pl.multiple_of(target(pix, 1, n_pix) * quarter, quarter), quarter)
    copies = [
        pltpu.make_async_copy(ranks_hbm, ranks_ref, sems.at[0]),
        pltpu.make_async_copy(a_hbm.at[at, :], a_ref, sems.at[1]),
        pltpu.make_async_copy(x0_hbm, x0_ref, sems.at[2]),
    ]
    for copy in copies:
        copy.start()
    copies[0].wait()
    rows = lax.broadcasted_iota(jnp.int32, (PAD, TILE), 0)
    count = jnp.int32(0)
    table = []
    notes = jnp.full((PAD, TILE), -1, jnp.int32)
    for j in range(tiles):
        rank = ranks_ref[j, 0]
        slot = jnp.where(rank < slots, rank, -1)
        table.append((slot, count))
        notes = jnp.where(rows == j, slot, notes)
        notes = jnp.where(jnp.logical_and(rows == PAD - 2, base == j), slot, notes)
        count = count + jnp.where(rank < slots, 1, 0)
    notes = jnp.where(rows == PAD - 1, count, notes)
    notes_ref[...] = notes.astype(jnp.float32).astype(jnp.bfloat16)
    sent = jnp.where(rows == PAD - 1, count, -1)
    lanes = []
    for i in range(places):
        tile = jnp.int32(0)
        for j, (slot, before) in enumerate(table):
            hit = jnp.logical_and(slot >= 0, before == i)
            tile = jnp.where(hit, j, tile)
            sent = jnp.where(jnp.logical_and(rows == i, hit), slot, sent)
        lanes.append(pl.ds(pl.multiple_of(tile * TILE, TILE), TILE))
    out[places * quarter :, :] = sent.astype(jnp.float32).astype(jnp.bfloat16)
    copies[1].wait()
    for i in range(places):
        out[i * quarter : (i + 1) * quarter, :] = a_ref[:, lanes[i]]
    copies[2].wait()
    round_ref[...] = x0_ref[...].astype(jnp.bfloat16)


def rest_body(first, route, n_pix, notes_ref, a_ref, *outs):
    pix = lax.axis_index("pix")
    quarter = a_ref.shape[0] // n_pix
    places = (outs[0].shape[0] - PAD) // quarter
    notes = notes_ref[...].astype(jnp.float32)
    tiles = a_ref.shape[1] // TILE
    rows = lax.broadcasted_iota(jnp.int32, (PAD, TILE), 0)
    before = jnp.zeros((1, TILE), jnp.float32)
    sent = jnp.where(rows == PAD - 1, notes, -1.0)
    hits = []
    for j in range(tiles):
        slot = notes[j : j + 1]
        hits.append([jnp.logical_and(slot >= 0, before == first + i) for i in range(places)])
        for i in range(places):
            sent = jnp.where(jnp.logical_and(rows == i, hits[j][i]), slot, sent)
        before = before + jnp.where(slot >= 0, 1.0, 0.0)
    for d, out in enumerate(outs):
        at = pl.ds(pl.multiple_of(target(pix, d + route, n_pix) * quarter, quarter), quarter)
        for i in range(places):
            block = a_ref[at, :TILE]
            for j in range(1, tiles):
                tile = a_ref[at, j * TILE : (j + 1) * TILE]
                block = jnp.where(jnp.broadcast_to(hits[j][i], block.shape), tile, block)
            out[i * quarter : (i + 1) * quarter, :] = block
        out[places * quarter :, :] = sent.astype(jnp.bfloat16)


def crowd_body(places, *refs):
    *parts, out_ref = refs
    most = parts[0][-PAD:, :].astype(jnp.float32)
    for part in parts[1:]:
        most = jnp.maximum(most, part[-PAD:, :].astype(jnp.float32))
    rows = lax.broadcasted_iota(jnp.int32, (PAD, TILE), 0)
    most = jnp.max(jnp.where(rows == PAD - 1, most, -1.0))
    out_ref[0] = jnp.where(most > places, 1, 0)


def first_body(a_ref, *refs):
    pix, base = lax.axis_index("pix"), lax.axis_index("base")
    n_base = a_ref.shape[1] // TILE
    shares, rest = refs[:n_base], refs[n_base:]
    outs, x_ref = rest[:-1], rest[-1]
    quarter = outs[0].shape[1]
    for d, share in enumerate(shares):
        x_ref[:, pl.ds(pl.multiple_of((base ^ d) * TILE, TILE), TILE)] = share[...]
    for d, out in enumerate(outs):
        rows = pl.ds(pl.multiple_of(target(pix, d, len(outs)) * quarter, quarter), quarter)
        piece = lax.dot_general(
            x_ref[...], a_ref[rows, :], (((1,), (1,)), ((), ())), preferred_element_type=jnp.float32
        )
        out[...] = piece.astype(out.dtype)


def in_order(values, index):
    bit = 1
    while bit < len(values):
        odd = (index & bit) != 0
        values = [jnp.where(odd, values[d ^ bit], values[d]) for d in range(len(values))]
        bit *= 2
    return values


def pairs(slots):
    return [(r, s) for r in range(slots) for s in range(r + 1, slots)] + [(r, r + 1) for r in range(0, slots, 2)]


def pack_rows(slots, n_base):
    return len(pairs(slots)) * TILE // n_base


def corner():
    rows = lax.broadcasted_iota(jnp.int32, (TILE, TILE), 0)
    cols = lax.broadcasted_iota(jnp.int32, (TILE, TILE), 1)
    return rows, cols


def gram_body(slots, n_parts, y_ref, a_ref, notes_ref, *refs):
    pix, base = lax.axis_index("pix"), lax.axis_index("base")
    parts = refs[:n_parts]
    cols_ref, own_ref, sent_ref, all_ref = refs[n_parts:]
    n_base = all_ref.shape[0]
    chans, quarter = y_ref.shape[0], cols_ref.shape[0]
    own_rows = pl.ds(pl.multiple_of(pix * quarter, quarter), quarter)
    tiles = a_ref.shape[1] // TILE
    blocks = [a_ref[own_rows, j * TILE : (j + 1) * TILE] for j in range(tiles)]
    notes = notes_ref[...].astype(jnp.float32)
    marks = [notes[j : j + 1] for j in range(tiles)]
    for part in parts:
        places = (part.shape[0] - PAD) // quarter
        notes = part[places * quarter :, :].astype(jnp.float32)
        blocks += [part[i * quarter : (i + 1) * quarter, :] for i in range(places)]
        marks += [notes[i : i + 1] for i in range(places)]
    columns = []
    for r in range(slots):
        column = jnp.zeros((quarter, TILE), jnp.bfloat16)
        for block, mark in zip(blocks, marks):
            column = jnp.where(jnp.broadcast_to(mark == r, column.shape), block, column)
        columns.append(column)
    a = jnp.concatenate(columns, axis=1)
    cols_ref[...] = a
    y = y_ref[:, pl.ds(pl.multiple_of(pix * quarter, quarter), quarter)]
    both = jnp.dot(jnp.concatenate(split(y), axis=0), a, preferred_element_type=jnp.float32)
    data = both[:chans] + both[chans:]
    gram = lax.dot_general(a, a, (((0,), (0,)), ((), ())), preferred_element_type=jnp.float32)
    rows, cols = corner()
    g_rows = pack_rows(slots, n_base)
    per = slots // n_base
    half = min(TILE, g_rows & -g_rows)

    def block_of(r, s):
        return gram[r * TILE : (r + 1) * TILE, s * TILE : (s + 1) * TILE]

    n_off = slots * (slots - 1) // 2
    for i, (r, s) in enumerate(pairs(slots)):
        block = block_of(r, s) if i < n_off else jnp.where(rows < cols, block_of(r, r), block_of(s, s))
        block = block.astype(jnp.bfloat16)
        for q in range(TILE // half):
            at = i * TILE + q * half
            all_ref[at // g_rows, at % g_rows : at % g_rows + half, :] = block[q * half : (q + 1) * half]
    for r in range(slots):
        diag = jnp.sum(jnp.where(rows == cols, block_of(r, r), 0.0), axis=0, keepdims=True)
        at = g_rows + (r % per) * (2 * chans + PAD)
        wide = jnp.concatenate(split(data[:, r * TILE : (r + 1) * TILE]), axis=0)
        all_ref[r // per, at : at + 2 * chans, :] = wide
        all_ref[r // per, at + 2 * chans : at + 2 * chans + PAD, :] = tail_of(diag)
    by_core(base, all_ref, own_ref, sent_ref)


def by_core(base, all_ref, own_ref, sent_ref):
    size = all_ref.shape[1]
    for k in range(all_ref.shape[0] // 2):
        own_ref[k * size : (k + 1) * size, :] = all_ref[base ^ (2 * k)]
        sent_ref[k * size : (k + 1) * size, :] = all_ref[base ^ (2 * k + 1)]


def tail_of(row):
    return jnp.concatenate([*split(row), jnp.zeros((PAD - 2, TILE), jnp.bfloat16)], axis=0)


def start_body(slots, n_pix, y_ref, x0_ref, notes_ref, cols_ref, *refs):
    pix, base = lax.axis_index("pix"), lax.axis_index("base")
    preds = refs[:n_pix]
    own_ref, sent_ref, all_ref = refs[n_pix:]
    per = slots // all_ref.shape[0]
    chans, quarter = preds[0].shape
    pred = preds[0][...].astype(jnp.float32)
    for piece in preds[1:]:
        pred = pred + piece[...].astype(jnp.float32)
    y = y_ref[:, pl.ds(pl.multiple_of(pix * quarter, quarter), quarter)]
    resid = (y - pred).astype(jnp.bfloat16)
    moved = descent_stride * jnp.dot(resid, cols_ref[...], preferred_element_type=jnp.float32)
    mark = notes_ref[PAD - 2 : PAD - 1, :].astype(jnp.float32)
    for r in range(slots):
        start = moved[:, r * TILE : (r + 1) * TILE] + jnp.where(mark == r, x0_ref[...], 0.0)
        at = (r % per) * 2 * chans
        all_ref[r // per, at : at + 2 * chans, :] = jnp.concatenate(split(start), axis=0)
    by_core(base, all_ref, own_ref, sent_ref)


def summed(parts, at, size, pair):
    value = parts[0][at : at + size].astype(jnp.float32)
    for part in parts[1:]:
        value = value + part[at : at + size].astype(jnp.float32)
    if pair == 0:
        return value.astype(jnp.bfloat16)
    if pair == 1:
        return tail_of(value[0:1] + value[1:2])
    return jnp.concatenate(split(value[:pair] + value[pair:]), axis=0)


def core_body(layout, own_ref, got_ref, *outs):
    at = 0
    for out in outs:
        to = 0
        for size, pair in layout:
            out[to : to + size] = summed([own_ref, got_ref], at, size, pair)
            at += size
            to += size


def join_body(layouts, *refs):
    *parts, out = refs
    to = 0
    for i, layout in enumerate(layouts):
        at = 0
        for size, pair in layout:
            place = out.shape[0] - size if pair == 1 else to
            out[place : place + size] = summed(parts[i :: len(layouts)], at, size, pair)
            at += size
            to += 0 if pair == 1 else size


def total_body(layout, *refs):
    *parts, out, short = refs
    at = to = 0
    for size, pair in layout:
        value = summed(parts, at, size, pair)
        out[at : at + size] = value
        kept = pair if pair > 1 else size
        short[to : to + kept] = value[:kept]
        at += size
        to += kept


def iterate_body(slots, n_base, notes_ref, *refs):
    base = lax.axis_index("base")
    *chunks, out_ref, gram_ref = refs
    chans = out_ref.shape[0]
    rows, cols = corner()
    n_off = slots * (slots - 1) // 2
    g_rows = pack_rows(slots, n_base)
    half = min(TILE, g_rows & -g_rows)
    states, datas, diags = [], [], []

    def put(g, r, s, block):
        gram_ref[g, r * TILE : (r + 1) * TILE, s * TILE : (s + 1) * TILE] = block

    for g in range(2):
        full = in_order([ref[...] for ref in chunks[g * n_base : (g + 1) * n_base]], base)
        for i, (r, s) in enumerate(pairs(slots)):
            pieces = []
            for q in range(TILE // half):
                at = i * TILE + q * half
                pieces.append(full[at // g_rows][at % g_rows : at % g_rows + half])
            block = jnp.concatenate(pieces, axis=0)
            if i < n_off:
                put(g, r, s, block)
                put(g, s, r, block.T)
            else:
                upper = jnp.where(rows < cols, block, jnp.zeros_like(block))
                lower = jnp.where(rows > cols, block, jnp.zeros_like(block))
                put(g, r, r, upper + upper.T)
                put(g, s, s, lower + lower.T)
        wide = (full[0].shape[0] - g_rows - PAD) // 2

        def gather(at):
            values = [v[at : at + wide].astype(jnp.float32) for v in full]
            return jnp.concatenate([v[:chans] + v[chans:] if wide > chans else v for v in values], axis=1)

        datas.append(gather(g_rows))
        states.append(gather(g_rows + wide))
        tails = [v[g_rows + 2 * wide :].astype(jnp.float32) for v in full]
        diags.append(jnp.concatenate([t[0:1] + t[1:2] for t in tails], axis=1))
    tile = lambda v, r: v[:, r * TILE : (r + 1) * TILE]
    for step in range(ITERS):
        parts = [[], []]
        if step < ITERS - 1:
            for g in range(2):
                high, low = split(states[g])
                left = jnp.concatenate([high, low], axis=0) if g == 0 else high
                for r in range(slots):
                    rows_r = gram_ref[g, r * TILE : (r + 1) * TILE, :]
                    part = jnp.dot(tile(left, r), rows_r, preferred_element_type=jnp.float32)
                    parts[g].append(part[:chans] + part[chans:] if g == 0 else part)
        squares = states[0] * states[0] + states[1] * states[1]
        column = jnp.sum(squares, axis=0, keepdims=True)
        factors = []
        for r in range(slots):
            norm = jnp.sum(tile(column, r), axis=1, keepdims=True)
            rms = jnp.sqrt(norm / (CH * TILE) + eps_norm)
            factors.append(rms / (rms + lam_shrink))
        factor = jnp.concatenate([jnp.broadcast_to(f, (1, TILE)) for f in factors], axis=1)
        states = [state * factor for state in states]
        if step == ITERS - 1:
            break
        for g in range(2):
            product = states[g] * diags[g]
            for f, part in zip(factors, parts[g]):
                product = product + f * part
            states[g] = states[g] + descent_stride * (datas[g] - product)
    mark = notes_ref[PAD - 2 : PAD - 1, :].astype(jnp.float32)
    image = jnp.zeros(out_ref.shape, jnp.float32)
    for r in range(slots):
        image = jnp.where(mark == r, states[0][:, r * TILE : (r + 1) * TILE], image)
    out_ref[...] = image


def gram_plan(sensing_operator_parts, sampled_correlations, first_sky_estimate, patch_order_record):
    a = sensing_operator_parts[0]
    chans, m_dev = sampled_correlations.shape
    n_base, n_pix = lax.axis_size("base"), lax.axis_size("pix")
    slots = n_base * n_pix // 4
    quarter = m_dev // n_pix
    x0 = first_sky_estimate[:, 0, 0, :]
    ranks = pltpu.with_memory_space_constraint(patch_order_record.T, pltpu.HBM)
    shape = jax.ShapeDtypeStruct
    bf16, f32 = jnp.bfloat16, jnp.float32

    def pieces_of(places):
        return [shape((places * quarter + PAD, TILE), bf16)] * (n_pix - 1)

    tiles = ranks.shape[0]
    places = min(CAPACITY, tiles)
    piece, notes, x0_round = call(
        functools.partial(pack_body, slots, n_pix),
        [pieces_of(places)[0], shape((PAD, TILE), bf16), shape(x0.shape, bf16)],
        (ranks, a, x0),
        scratch=[
            pltpu.SMEM(ranks.shape, jnp.int32),
            pltpu.VMEM((quarter, a.shape[1]), bf16),
            pltpu.VMEM(x0.shape, f32),
            pltpu.SemaphoreType.DMA((3,)),
        ],
        hbm=(0, 1, 2),
    )

    def pack(first, places, route):
        return call(functools.partial(rest_body, first, route, n_pix), pieces_of(places)[route - 1 :], (notes, a))

    parts = send([piece, *pack(0, places, 2)])

    def rest():
        return send(pack(places, tiles - places, 1))

    shares = [x0_round] + [swap(x0_round, "base", d) for d in range(1, n_base)]
    firsts = call(
        first_body,
        [shape((chans, quarter), bf16)] * n_pix,
        (a, *shares),
        scratch=[pltpu.VMEM((chans, n_base * TILE), bf16)],
    )
    preds = [firsts[0]] + send(firsts[1:])

    per = slots // n_base
    gram_layout = [(pack_rows(slots, n_base), 0), (2 * chans, chans), (PAD, 1)]
    side_layout = [(2 * chans, chans)]
    total_layout = [gram_layout[0], gram_layout[1], *side_layout, gram_layout[2]]
    layouts = [gram_layout, side_layout]
    heights = [sum(size for size, _ in layout) for layout in layouts]
    chunk = shape((sum(heights), TILE), bf16)
    short = shape((chunk.shape[0] - 2 * chans * per, TILE), bf16)

    def halves(height):
        return [shape((n_base // 2 * height, TILE), bf16)] * 2

    def base_sum(parts):
        columns, *gram = call(
            functools.partial(gram_body, slots, len(parts)),
            [shape((quarter, slots * TILE), bf16)] + halves(heights[0]),
            (sampled_correlations, a, notes, *parts),
            scratch=[pltpu.VMEM((n_base, heights[0], TILE), bf16)],
        )
        side = call(
            functools.partial(start_body, slots, n_pix),
            halves(heights[1]),
            (sampled_correlations, x0, notes, columns, *preds),
            scratch=[pltpu.VMEM((n_base, heights[1], TILE), bf16)],
        )
        pieces = []
        for (own, sent), layout in zip((gram, side), layouts):
            height = sum(size for size, _ in layout)
            sums = call(
                functools.partial(core_body, layout),
                [shape((height, TILE), bf16)] * (n_base // 2),
                (own, swap(sent, "base", 1)),
            )
            far = [swap(sums[k], "base", 2 * k) for k in range(1, n_base // 2)]
            pieces.append([sums[0], *far])
        return [piece for pair in zip(*pieces) for piece in pair]

    def join(pieces):
        return call(functools.partial(join_body, layouts), chunk, pieces)

    crowded = call(functools.partial(crowd_body, places), shape((1,), jnp.int32), (notes, *parts), scalars=(0,))[0]
    pieces = base_sum(parts)
    part = lax.cond(crowded != 0, lambda: join(base_sum(parts + rest())), lambda: join(pieces))
    total, brief = call(
        functools.partial(total_body, total_layout), [chunk, short], [part] + send([part] * (n_pix - 1))
    )

    axes = ("freq", "base")
    got = {0: total, n_base: swap(brief, axes, n_base)}
    for offset in range(2, n_base, 2):
        got[n_base + offset] = swap(brief, axes, n_base + offset)
        got[offset] = swap(total, axes, offset)
    got[1] = swap(total, axes, 1)
    for offset in range(2, 2 * n_base, 2):
        got[offset + 1] = swap(got[offset], axes, 1)
    image = call(
        functools.partial(iterate_body, slots, n_base),
        shape((chans, TILE), f32),
        (notes, *[got[i] for i in range(2 * n_base)]),
        scratch=[
            pltpu.VMEM((2, slots * TILE, slots * TILE), bf16),
        ],
    )
    return image.reshape(chans, 1, 1, TILE)


def on_device(sensing_operator_parts, sampled_correlations, first_sky_estimate, patch_order_record):
    n_base, n_pix = lax.axis_size("base"), lax.axis_size("pix")
    slots = n_base * n_pix // 4
    chans, m_dev = sampled_correlations.shape
    fits = (
        first_sky_estimate.shape[3] == TILE
        and (slots * TILE) ** 2 <= GRAM_LIMIT
        and n_base & (n_base - 1) == 0
        and n_pix & (n_pix - 1) == 0
        and slots == n_base
        and n_base <= PAD - 2
        and slots % 2 == 0
        and len(pairs(slots)) * TILE % (n_base * 16) == 0
        and m_dev % (n_pix * TILE) == 0
        and lax.axis_size("freq") == 2
        and chans % 16 == 0
    )
    plan = gram_plan if fits else streaming
    return plan(sensing_operator_parts, sampled_correlations, first_sky_estimate, patch_order_record)


def solution(mesh):
    in_specs = (
        P("freq", "base", "pix"),
        P("freq", "base"),
        P("freq", "pix", "base", None),
        P(None, "pix"),
    )
    out_specs = P("freq", "pix", "base", None)
    return jax.shard_map(
        on_device, mesh=mesh, in_specs=in_specs, out_specs=out_specs, check_vma=False
    )
```

```python
import functools

import jax
import jax.numpy as jnp
from jax import lax
from jax.experimental import pallas as pl
from jax.experimental.pallas import tpu as pltpu
from jax.sharding import PartitionSpec as P

CH = 64
TILE = 128
ITERS = 6


descent_stride = 0.6
lam_shrink = 0.3
eps_norm = 1e-06


GRAM_LIMIT = 1 << 20
PAD = 8
CAPACITY = 2
VMEM_LIMIT = 12 << 20


def project_rows(rounded_amount, columns):
    return lax.dot_general(
        rounded_amount, columns, (((1,), (1,)), ((), ())), preferred_element_type=jnp.float32
    )


def residual_of(sampled_correlations, partial_value):
    shares = lax.psum_scatter(partial_value, "pix", scatter_dimension=1, tiled=True)
    width = shares.shape[1]
    own_rows = lax.dynamic_slice_in_dim(
        sampled_correlations, lax.axis_index("pix") * width, width, 1
    )
    return lax.all_gather((own_rows - shares).astype(jnp.bfloat16), "pix", axis=1, tiled=True)


def streaming(sensing_operator_parts, sampled_correlations, first_sky_estimate, patch_order_record):
    sensing_operator = sensing_operator_parts[0]
    chans, _ = sampled_correlations.shape
    share_width = first_sky_estimate.shape[3]
    tiles_share = share_width // TILE
    keep_count = tiles_share * lax.axis_size("base") * lax.axis_size("pix") // 4
    base_index = lax.axis_index("base")
    own_share = first_sky_estimate[:, 0, 0, :]
    current = own_share
    for step in range(ITERS):
        rounded_amount = current.astype(jnp.bfloat16)
        partial_value = project_rows(
            lax.all_gather(rounded_amount, "base", axis=1, tiled=True), sensing_operator
        )
        resid = residual_of(sampled_correlations, partial_value)
        gradient_portion = jnp.dot(resid, sensing_operator, preferred_element_type=jnp.float32)
        grad_share = lax.psum_scatter(gradient_portion, "base", scatter_dimension=1, tiled=True)
        moved = current + descent_stride * grad_share
        tiles = moved.reshape(chans, tiles_share, TILE)
        local_sum = jnp.sum(tiles * tiles, axis=(0, 2))
        total = lax.psum(local_sum, "freq")
        ranks = lax.dynamic_slice_in_dim(
            patch_order_record[step], base_index * tiles_share, tiles_share, 0
        )
        rms_tile = jnp.sqrt(total / (CH * TILE) + eps_norm)
        keeping = (ranks < keep_count).astype(jnp.float32)
        factor = keeping * rms_tile / (rms_tile + lam_shrink)
        current = (tiles * factor[None, :, None]).reshape(chans, share_width)
    return current.reshape(chans, 1, 1, share_width)


def swap(value, axis, offset):
    size = lax.axis_size(axis)
    return lax.ppermute(value, axis, [(i, i ^ offset) for i in range(size)])


def routes(size):
    if size == 4:
        return [(1, 3, 0, 2), (3, 2, 1, 0), (2, 0, 3, 1)]
    return [tuple(i ^ d for i in range(size)) for d in range(1, size)]


def send(pieces):
    got = []
    for piece, route in zip(pieces, routes(lax.axis_size("pix"))):
        got.append(lax.ppermute(piece, "pix", list(enumerate(route))))
    return got


def target(pix, k, size):
    if k == 0:
        return pix
    place = jnp.int32(0)
    for i, to in enumerate(routes(size)[k - 1]):
        place = jnp.where(pix == i, to, place)
    return place


def call(body, out_shape, args, scratch=(), hbm=(), scalars=()):
    specs = [pl.BlockSpec(memory_space=pltpu.HBM if i in hbm else pltpu.VMEM) for i in range(len(args))]
    place = lambda i: pltpu.SMEM if i in scalars else pltpu.VMEM
    if isinstance(out_shape, list):
        out_specs = [pl.BlockSpec(memory_space=place(i)) for i in range(len(out_shape))]
    else:
        out_specs = pl.BlockSpec(memory_space=place(0))
    return pl.pallas_call(
        body,
        out_shape=out_shape,
        in_specs=specs,
        out_specs=out_specs,
        scratch_shapes=list(scratch),
        compiler_params=pltpu.CompilerParams(vmem_limit_bytes=VMEM_LIMIT),
    )(*args)


def split(value):
    high = value.astype(jnp.bfloat16)
    return high, (value - high.astype(jnp.float32)).astype(jnp.bfloat16)


def pack_body(slots, n_pix, ranks_hbm, a_hbm, x0_hbm, out, notes_ref, round_ref, ranks_ref, a_ref, x0_ref, sems):
    pix, base = lax.axis_index("pix"), lax.axis_index("base")
    tiles = ranks_ref.shape[0]
    quarter = a_ref.shape[0]
    places = (out.shape[0] - PAD) // quarter
    at = pl.ds(pl.multiple_of(target(pix, 1, n_pix) * quarter, quarter), quarter)
    copies = [
        pltpu.make_async_copy(ranks_hbm, ranks_ref, sems.at[0]),
        pltpu.make_async_copy(a_hbm.at[at, :], a_ref, sems.at[1]),
        pltpu.make_async_copy(x0_hbm, x0_ref, sems.at[2]),
    ]
    for copy in copies:
        copy.start()
    copies[0].wait()
    rows = lax.broadcasted_iota(jnp.int32, (PAD, TILE), 0)
    count = jnp.int32(0)
    table = []
    notes = jnp.full((PAD, TILE), -1, jnp.int32)
    for j in range(tiles):
        rank = ranks_ref[j, 0]
        slot = jnp.where(rank < slots, rank, -1)
        table.append((slot, count))
        notes = jnp.where(rows == j, slot, notes)
        notes = jnp.where(jnp.logical_and(rows == PAD - 2, base == j), slot, notes)
        count = count + jnp.where(rank < slots, 1, 0)
    notes = jnp.where(rows == PAD - 1, count, notes)
    notes_ref[...] = notes.astype(jnp.float32).astype(jnp.bfloat16)
    sent = jnp.where(rows == PAD - 1, count, -1)
    lanes = []
    for i in range(places):
        tile = jnp.int32(0)
        for j, (slot, before) in enumerate(table):
            hit = jnp.logical_and(slot >= 0, before == i)
            tile = jnp.where(hit, j, tile)
            sent = jnp.where(jnp.logical_and(rows == i, hit), slot, sent)
        lanes.append(pl.ds(pl.multiple_of(tile * TILE, TILE), TILE))
    out[places * quarter :, :] = sent.astype(jnp.float32).astype(jnp.bfloat16)
    copies[1].wait()
    for i in range(places):
        out[i * quarter : (i + 1) * quarter, :] = a_ref[:, lanes[i]]
    copies[2].wait()
    round_ref[...] = x0_ref[...].astype(jnp.bfloat16)


def rest_body(first, route, n_pix, notes_ref, a_ref, *outs):
    pix = lax.axis_index("pix")
    quarter = a_ref.shape[0] // n_pix
    places = (outs[0].shape[0] - PAD) // quarter
    notes = notes_ref[...].astype(jnp.float32)
    tiles = a_ref.shape[1] // TILE
    rows = lax.broadcasted_iota(jnp.int32, (PAD, TILE), 0)
    before = jnp.zeros((1, TILE), jnp.float32)
    sent = jnp.where(rows == PAD - 1, notes, -1.0)
    hits = []
    for j in range(tiles):
        slot = notes[j : j + 1]
        hits.append([jnp.logical_and(slot >= 0, before == first + i) for i in range(places)])
        for i in range(places):
            sent = jnp.where(jnp.logical_and(rows == i, hits[j][i]), slot, sent)
        before = before + jnp.where(slot >= 0, 1.0, 0.0)
    for d, out in enumerate(outs):
        at = pl.ds(pl.multiple_of(target(pix, d + route, n_pix) * quarter, quarter), quarter)
        for i in range(places):
            block = a_ref[at, :TILE]
            for j in range(1, tiles):
                tile = a_ref[at, j * TILE : (j + 1) * TILE]
                block = jnp.where(jnp.broadcast_to(hits[j][i], block.shape), tile, block)
            out[i * quarter : (i + 1) * quarter, :] = block
        out[places * quarter :, :] = sent.astype(jnp.bfloat16)


def crowd_body(places, *refs):
    *parts, out_ref = refs
    most = parts[0][-PAD:, :].astype(jnp.float32)
    for part in parts[1:]:
        most = jnp.maximum(most, part[-PAD:, :].astype(jnp.float32))
    rows = lax.broadcasted_iota(jnp.int32, (PAD, TILE), 0)
    most = jnp.max(jnp.where(rows == PAD - 1, most, -1.0))
    out_ref[0] = jnp.where(most > places, 1, 0)


def first_body(a_ref, *refs):
    pix, base = lax.axis_index("pix"), lax.axis_index("base")
    n_base = a_ref.shape[1] // TILE
    shares, rest = refs[:n_base], refs[n_base:]
    outs, x_ref = rest[:-1], rest[-1]
    quarter = outs[0].shape[1]
    for d, share in enumerate(shares):
        x_ref[:, pl.ds(pl.multiple_of((base ^ d) * TILE, TILE), TILE)] = share[...]
    for d, out in enumerate(outs):
        rows = pl.ds(pl.multiple_of(target(pix, d, len(outs)) * quarter, quarter), quarter)
        piece = lax.dot_general(
            x_ref[...], a_ref[rows, :], (((1,), (1,)), ((), ())), preferred_element_type=jnp.float32
        )
        out[...] = piece.astype(out.dtype)


def in_order(values, index):
    bit = 1
    while bit < len(values):
        odd = (index & bit) != 0
        values = [jnp.where(odd, values[d ^ bit], values[d]) for d in range(len(values))]
        bit *= 2
    return values


def pairs(slots):
    return [(r, s) for r in range(slots) for s in range(r + 1, slots)] + [(r, r + 1) for r in range(0, slots, 2)]


def pack_rows(slots, n_base):
    return len(pairs(slots)) * TILE // n_base


def corner():
    rows = lax.broadcasted_iota(jnp.int32, (TILE, TILE), 0)
    cols = lax.broadcasted_iota(jnp.int32, (TILE, TILE), 1)
    return rows, cols


def gram_body(slots, n_parts, y_ref, a_ref, notes_ref, *refs):
    pix, base = lax.axis_index("pix"), lax.axis_index("base")
    parts = refs[:n_parts]
    cols_ref, own_ref, sent_ref, all_ref = refs[n_parts:]
    n_base = all_ref.shape[0]
    chans, quarter = y_ref.shape[0], cols_ref.shape[0]
    own_rows = pl.ds(pl.multiple_of(pix * quarter, quarter), quarter)
    tiles = a_ref.shape[1] // TILE
    blocks = [a_ref[own_rows, j * TILE : (j + 1) * TILE] for j in range(tiles)]
    notes = notes_ref[...].astype(jnp.float32)
    marks = [notes[j : j + 1] for j in range(tiles)]
    for part in parts:
        places = (part.shape[0] - PAD) // quarter
        notes = part[places * quarter :, :].astype(jnp.float32)
        blocks += [part[i * quarter : (i + 1) * quarter, :] for i in range(places)]
        marks += [notes[i : i + 1] for i in range(places)]
    columns = []
    for r in range(slots):
        column = jnp.zeros((quarter, TILE), jnp.bfloat16)
        for block, mark in zip(blocks, marks):
            column = jnp.where(jnp.broadcast_to(mark == r, column.shape), block, column)
        columns.append(column)
    a = jnp.concatenate(columns, axis=1)
    cols_ref[...] = a
    y = y_ref[:, pl.ds(pl.multiple_of(pix * quarter, quarter), quarter)]
    both = jnp.dot(jnp.concatenate(split(y), axis=0), a, preferred_element_type=jnp.float32)
    data = both[:chans] + both[chans:]
    bands = [
        lax.dot_general(
            columns[r], a[:, r * TILE :], (((0,), (0,)), ((), ())), preferred_element_type=jnp.float32
        )
        for r in range(slots)
    ]
    rows, cols = corner()
    g_rows = pack_rows(slots, n_base)
    per = slots // n_base
    half = min(TILE, g_rows & -g_rows)

    def block_of(r, s):
        return bands[r][:, (s - r) * TILE : (s - r + 1) * TILE]

    n_off = slots * (slots - 1) // 2
    for i, (r, s) in enumerate(pairs(slots)):
        block = block_of(r, s) if i < n_off else jnp.where(rows < cols, block_of(r, r), block_of(s, s))
        block = block.astype(jnp.bfloat16)
        for q in range(TILE // half):
            at = i * TILE + q * half
            all_ref[at // g_rows, at % g_rows : at % g_rows + half, :] = block[q * half : (q + 1) * half]
    for r in range(slots):
        diag = jnp.sum(jnp.where(rows == cols, block_of(r, r), 0.0), axis=0, keepdims=True)
        at = g_rows + (r % per) * (2 * chans + PAD)
        wide = jnp.concatenate(split(data[:, r * TILE : (r + 1) * TILE]), axis=0)
        all_ref[r // per, at : at + 2 * chans, :] = wide
        all_ref[r // per, at + 2 * chans : at + 2 * chans + PAD, :] = tail_of(diag)
    by_core(base, all_ref, own_ref, sent_ref)


def by_core(base, all_ref, own_ref, sent_ref):
    size = all_ref.shape[1]
    for k in range(all_ref.shape[0] // 2):
        own_ref[k * size : (k + 1) * size, :] = all_ref[base ^ (2 * k)]
        sent_ref[k * size : (k + 1) * size, :] = all_ref[base ^ (2 * k + 1)]


def tail_of(row):
    return jnp.concatenate([*split(row), jnp.zeros((PAD - 2, TILE), jnp.bfloat16)], axis=0)


def start_body(slots, n_pix, y_ref, x0_ref, notes_ref, cols_ref, *refs):
    pix, base = lax.axis_index("pix"), lax.axis_index("base")
    preds = refs[:n_pix]
    own_ref, sent_ref, all_ref = refs[n_pix:]
    per = slots // all_ref.shape[0]
    chans, quarter = preds[0].shape
    pred = preds[0][...].astype(jnp.float32)
    for piece in preds[1:]:
        pred = pred + piece[...].astype(jnp.float32)
    y = y_ref[:, pl.ds(pl.multiple_of(pix * quarter, quarter), quarter)]
    resid = (y - pred).astype(jnp.bfloat16)
    moved = descent_stride * jnp.dot(resid, cols_ref[...], preferred_element_type=jnp.float32)
    mark = notes_ref[PAD - 2 : PAD - 1, :].astype(jnp.float32)
    for r in range(slots):
        start = moved[:, r * TILE : (r + 1) * TILE] + jnp.where(mark == r, x0_ref[...], 0.0)
        at = (r % per) * 2 * chans
        all_ref[r // per, at : at + 2 * chans, :] = jnp.concatenate(split(start), axis=0)
    by_core(base, all_ref, own_ref, sent_ref)


def summed(parts, at, size, pair):
    value = parts[0][at : at + size].astype(jnp.float32)
    for part in parts[1:]:
        value = value + part[at : at + size].astype(jnp.float32)
    if pair == 0:
        return value.astype(jnp.bfloat16)
    if pair == 1:
        return tail_of(value[0:1] + value[1:2])
    return jnp.concatenate(split(value[:pair] + value[pair:]), axis=0)


def core_body(layout, own_ref, got_ref, *outs):
    at = 0
    for out in outs:
        to = 0
        for size, pair in layout:
            out[to : to + size] = summed([own_ref, got_ref], at, size, pair)
            at += size
            to += size


def join_body(layouts, *refs):
    *parts, out = refs
    to = 0
    for i, layout in enumerate(layouts):
        at = 0
        for size, pair in layout:
            place = out.shape[0] - size if pair == 1 else to
            out[place : place + size] = summed(parts[i :: len(layouts)], at, size, pair)
            at += size
            to += 0 if pair == 1 else size


def total_body(layout, *refs):
    *parts, out, short = refs
    at = to = 0
    for size, pair in layout:
        value = summed(parts, at, size, pair)
        out[at : at + size] = value
        kept = pair if pair > 1 else size
        short[to : to + kept] = value[:kept]
        at += size
        to += kept


def iterate_body(slots, n_base, notes_ref, *refs):
    base = lax.axis_index("base")
    *chunks, out_ref, gram_ref = refs
    chans = out_ref.shape[0]
    rows, cols = corner()
    n_off = slots * (slots - 1) // 2
    g_rows = pack_rows(slots, n_base)
    half = min(TILE, g_rows & -g_rows)
    states, datas, diags = [], [], []

    def put(g, r, s, block):
        gram_ref[g, r * TILE : (r + 1) * TILE, s * TILE : (s + 1) * TILE] = block

    for g in range(2):
        full = in_order([ref[...] for ref in chunks[g * n_base : (g + 1) * n_base]], base)
        for i, (r, s) in enumerate(pairs(slots)):
            pieces = []
            for q in range(TILE // half):
                at = i * TILE + q * half
                pieces.append(full[at // g_rows][at % g_rows : at % g_rows + half])
            block = jnp.concatenate(pieces, axis=0)
            if i < n_off:
                put(g, r, s, block)
                put(g, s, r, block.T)
            else:
                upper = jnp.where(rows < cols, block, jnp.zeros_like(block))
                lower = jnp.where(rows > cols, block, jnp.zeros_like(block))
                put(g, r, r, upper + upper.T)
                put(g, s, s, lower + lower.T)
        wide = (full[0].shape[0] - g_rows - PAD) // 2

        def gather(at):
            values = [v[at : at + wide].astype(jnp.float32) for v in full]
            return jnp.concatenate([v[:chans] + v[chans:] if wide > chans else v for v in values], axis=1)

        datas.append(gather(g_rows))
        states.append(gather(g_rows + wide))
        tails = [v[g_rows + 2 * wide :].astype(jnp.float32) for v in full]
        diags.append(jnp.concatenate([t[0:1] + t[1:2] for t in tails], axis=1))
    tile = lambda v, r: v[:, r * TILE : (r + 1) * TILE]
    for step in range(ITERS):
        parts = [[], []]
        if step < ITERS - 1:
            for g in range(2):
                high, low = split(states[g])
                left = jnp.concatenate([high, low], axis=0) if g == 0 else high
                for r in range(slots):
                    rows_r = gram_ref[g, r * TILE : (r + 1) * TILE, :]
                    part = jnp.dot(tile(left, r), rows_r, preferred_element_type=jnp.float32)
                    parts[g].append(part[:chans] + part[chans:] if g == 0 else part)
        squares = states[0] * states[0] + states[1] * states[1]
        column = jnp.sum(squares, axis=0, keepdims=True)
        factors = []
        for r in range(slots):
            norm = jnp.sum(tile(column, r), axis=1, keepdims=True)
            rms = jnp.sqrt(norm / (CH * TILE) + eps_norm)
            factors.append(rms / (rms + lam_shrink))
        factor = jnp.concatenate([jnp.broadcast_to(f, (1, TILE)) for f in factors], axis=1)
        states = [state * factor for state in states]
        if step == ITERS - 1:
            break
        for g in range(2):
            product = states[g] * diags[g]
            for f, part in zip(factors, parts[g]):
                product = product + f * part
            states[g] = states[g] + descent_stride * (datas[g] - product)
    mark = notes_ref[PAD - 2 : PAD - 1, :].astype(jnp.float32)
    image = jnp.zeros(out_ref.shape, jnp.float32)
    for r in range(slots):
        image = jnp.where(mark == r, states[0][:, r * TILE : (r + 1) * TILE], image)
    out_ref[...] = image


def gram_plan(sensing_operator_parts, sampled_correlations, first_sky_estimate, patch_order_record):
    a = sensing_operator_parts[0]
    chans, m_dev = sampled_correlations.shape
    n_base, n_pix = lax.axis_size("base"), lax.axis_size("pix")
    slots = n_base * n_pix // 4
    quarter = m_dev // n_pix
    x0 = first_sky_estimate[:, 0, 0, :]
    ranks = pltpu.with_memory_space_constraint(patch_order_record.T, pltpu.HBM)
    shape = jax.ShapeDtypeStruct
    bf16, f32 = jnp.bfloat16, jnp.float32

    def pieces_of(places):
        return [shape((places * quarter + PAD, TILE), bf16)] * (n_pix - 1)

    tiles = ranks.shape[0]
    places = min(CAPACITY, tiles)
    piece, notes, x0_round = call(
        functools.partial(pack_body, slots, n_pix),
        [pieces_of(places)[0], shape((PAD, TILE), bf16), shape(x0.shape, bf16)],
        (ranks, a, x0),
        scratch=[
            pltpu.SMEM(ranks.shape, jnp.int32),
            pltpu.VMEM((quarter, a.shape[1]), bf16),
            pltpu.VMEM(x0.shape, f32),
            pltpu.SemaphoreType.DMA((3,)),
        ],
        hbm=(0, 1, 2),
    )

    def pack(first, places, route):
        return call(functools.partial(rest_body, first, route, n_pix), pieces_of(places)[route - 1 :], (notes, a))

    parts = send([piece, *pack(0, places, 2)])

    def rest():
        return send(pack(places, tiles - places, 1))

    shares = [x0_round] + [swap(x0_round, "base", d) for d in range(1, n_base)]
    firsts = call(
        first_body,
        [shape((chans, quarter), bf16)] * n_pix,
        (a, *shares),
        scratch=[pltpu.VMEM((chans, n_base * TILE), bf16)],
    )
    preds = [firsts[0]] + send(firsts[1:])

    per = slots // n_base
    gram_layout = [(pack_rows(slots, n_base), 0), (2 * chans, chans), (PAD, 1)]
    side_layout = [(2 * chans, chans)]
    total_layout = [gram_layout[0], gram_layout[1], *side_layout, gram_layout[2]]
    layouts = [gram_layout, side_layout]
    heights = [sum(size for size, _ in layout) for layout in layouts]
    chunk = shape((sum(heights), TILE), bf16)
    short = shape((chunk.shape[0] - 2 * chans * per, TILE), bf16)

    def halves(height):
        return [shape((n_base // 2 * height, TILE), bf16)] * 2

    def base_sum(parts):
        columns, *gram = call(
            functools.partial(gram_body, slots, len(parts)),
            [shape((quarter, slots * TILE), bf16)] + halves(heights[0]),
            (sampled_correlations, a, notes, *parts),
            scratch=[pltpu.VMEM((n_base, heights[0], TILE), bf16)],
        )
        side = call(
            functools.partial(start_body, slots, n_pix),
            halves(heights[1]),
            (sampled_correlations, x0, notes, columns, *preds),
            scratch=[pltpu.VMEM((n_base, heights[1], TILE), bf16)],
        )
        pieces = []
        for (own, sent), layout in zip((gram, side), layouts):
            height = sum(size for size, _ in layout)
            sums = call(
                functools.partial(core_body, layout),
                [shape((height, TILE), bf16)] * (n_base // 2),
                (own, swap(sent, "base", 1)),
            )
            far = [swap(sums[k], "base", 2 * k) for k in range(1, n_base // 2)]
            pieces.append([sums[0], *far])
        return [piece for pair in zip(*pieces) for piece in pair]

    def join(pieces):
        return call(functools.partial(join_body, layouts), chunk, pieces)

    crowded = call(functools.partial(crowd_body, places), shape((1,), jnp.int32), (notes, *parts), scalars=(0,))[0]
    pieces = base_sum(parts)
    part = lax.cond(crowded != 0, lambda: join(base_sum(parts + rest())), lambda: join(pieces))
    total, brief = call(
        functools.partial(total_body, total_layout), [chunk, short], [part] + send([part] * (n_pix - 1))
    )

    axes = ("freq", "base")
    got = {0: total, n_base: swap(brief, axes, n_base)}
    for offset in range(2, n_base, 2):
        got[n_base + offset] = swap(brief, axes, n_base + offset)
        got[offset] = swap(total, axes, offset)
    got[1] = swap(total, axes, 1)
    for offset in range(2, 2 * n_base, 2):
        got[offset + 1] = swap(got[offset], axes, 1)
    image = call(
        functools.partial(iterate_body, slots, n_base),
        shape((chans, TILE), f32),
        (notes, *[got[i] for i in range(2 * n_base)]),
        scratch=[
            pltpu.VMEM((2, slots * TILE, slots * TILE), bf16),
        ],
    )
    return image.reshape(chans, 1, 1, TILE)


def on_device(sensing_operator_parts, sampled_correlations, first_sky_estimate, patch_order_record):
    n_base, n_pix = lax.axis_size("base"), lax.axis_size("pix")
    slots = n_base * n_pix // 4
    chans, m_dev = sampled_correlations.shape
    fits = (
        first_sky_estimate.shape[3] == TILE
        and (slots * TILE) ** 2 <= GRAM_LIMIT
        and n_base & (n_base - 1) == 0
        and n_pix & (n_pix - 1) == 0
        and slots == n_base
        and n_base <= PAD - 2
        and slots % 2 == 0
        and len(pairs(slots)) * TILE % (n_base * 16) == 0
        and m_dev % (n_pix * TILE) == 0
        and lax.axis_size("freq") == 2
        and chans % 16 == 0
    )
    plan = gram_plan if fits else streaming
    return plan(sensing_operator_parts, sampled_correlations, first_sky_estimate, patch_order_record)


def solution(mesh):
    in_specs = (
        P("freq", "base", "pix"),
        P("freq", "base"),
        P("freq", "pix", "base", None),
        P(None, "pix"),
    )
    out_specs = P("freq", "pix", "base", None)
    return jax.shard_map(
        on_device, mesh=mesh, in_specs=in_specs, out_specs=out_specs, check_vma=False
    )
```
